32 devices in a mesh: seq: 8 (over z, core), fsdp: 4 (over y, x).
Axes of the slice: x: 2, y: 2, z: 4, core: 2. Of those that a mesh axis runs over, the one named last changes fastest.
Arguments:
- tokens: bfloat16 [4, 1024, 2048], P('fsdp', 'seq'), may hold values from -6 to 6
- ln_gain: bfloat16 [2048], P('fsdp'), may hold values from 0.5 to 1.5
- ln_bias: bfloat16 [2048], P('fsdp'), may hold values from -3 to 3
- qkv_weight: bfloat16 [2048, 6144], P('fsdp')
- qkv_bias: bfloat16 [6144], P('fsdp'), may hold values from -3 to 3
- dense_weight: bfloat16 [2048, 2048], P('fsdp'), may hold values from -0.5 to 0.5
- dense_bias: bfloat16 [2048], P('fsdp'), may hold values from -3 to 3
- fc1_weight: bfloat16 [2048, 8192], P('fsdp'), may hold values from -0.125 to 0.125
- fc1_bias: bfloat16 [8192], P('fsdp'), may hold values from -3 to 3
- fc2_weight: bfloat16 [8192, 2048], P('fsdp'), may hold values from -0.0625 to 0.0625
- fc2_bias: bfloat16 [2048], P('fsdp'), may hold values from -3 to 3
- segments: int32 [4, 1024], P('fsdp'), may hold values from 0 to 1, as said below
- positions: int32 [4, 1024], P('fsdp', 'seq'), may hold values from 0 to 2046, as said below
- cotangent: bfloat16 [4, 1024, 2048], P('fsdp', 'seq'), may hold values from -6 to 6
Outputs:
- out: bfloat16 [4, 1024, 2048], P('fsdp', 'seq')
- grad_tokens: float32 [4, 1024, 2048], P('fsdp', 'seq')
- grad_ln_gain: float32 [2048], P('fsdp')
- grad_ln_bias: float32 [2048], P('fsdp')
- grad_qkv_weight: float32 [2048, 6144], P('fsdp')
- grad_qkv_bias: float32 [6144], P('fsdp')
- grad_dense_weight: float32 [2048, 2048], P('fsdp')
- grad_dense_bias: float32 [2048], P('fsdp')
- grad_fc1_weight: float32 [2048, 8192], P('fsdp')
- grad_fc1_bias: float32 [8192], P('fsdp')
- grad_fc2_weight: float32 [8192, 2048], P('fsdp')
- grad_fc2_bias: float32 [2048], P('fsdp')
The draws below stay inside these ranges and needn't reach their ends.
Inputs may be any that keep to these rules, and one draw needn't show every extreme that they name: `segments`: document numbers never fall along a sequence and each of 0 to 1 occurs in every sequence. The first document of each sequence starts at position 0; positions rise by one from token to token within a document; in every sequence the last token of the last document has position 2046.
All inputs are finite; a program needn't handle non-finite values.
Results may differ from the reference program's by a relative error of at most 0.0095.
Values may be sent and summed in bfloat16 or wider, within the bound.
A program may use at most 448 MiB of HBM per device.

```python
import jax
import jax.numpy as jnp
from jax import lax

D = 2048
HEADS = 32
HEAD = 64
ROT = 32
FF = 8192
LEN = 1024
SEQS = 4
DOCS = 2


def layout(key):

    def one_row(row_key):
        cut_key, off_key = jax.random.split(row_key)
        cut_points = jnp.sort(jax.random.permutation(cut_key, LEN - 1)[:DOCS - 1].astype(jnp.int32) + 1)
        places = jnp.arange(LEN, dtype=jnp.int32)
        after_cut = places[:, None] >= cut_points[None, :]
        segment = jnp.sum(after_cut.astype(jnp.int32), axis=1)
        doc_start = jnp.max(jnp.where(after_cut, cut_points[None, :], 0), axis=1)
        doc_index = jnp.arange(DOCS, dtype=jnp.int32)
        offsets = jax.random.randint(off_key, (DOCS,), 0, 1024, dtype=jnp.int32)
        offsets = jnp.where(doc_index == DOCS - 1, cut_points[DOCS - 2] + 1023 - LEN + LEN, offsets)
        offsets = jnp.where(doc_index == 0, 0, offsets)
        doc_offset = jnp.sum(jnp.where(segment[:, None] == doc_index[None, :], offsets[None, :], 0), axis=1)
        return (segment, places - doc_start + doc_offset)
    return jax.vmap(one_row)(jax.random.split(key, SEQS))


def draw_segments(key, part):
    return layout(jax.random.fold_in(key, 11))[0].astype(jnp.int32)


def draw_positions(key, part):
    return layout(jax.random.fold_in(key, 11))[1].astype(jnp.int32)


def draw_qkv_weight(key, part):
    key_query, key_keys, key_value = jax.random.split(key, 3)
    spread = D ** (-0.5)
    query_part = jax.random.normal(key_query, (D, D), jnp.float32) * spread
    key_part = jax.random.normal(key_keys, (D, D), jnp.float32) * spread
    value_part = jax.random.normal(key_value, (D, D), jnp.float32) * spread
    return jnp.concatenate([query_part, key_part, value_part], axis=1).astype(jnp.bfloat16)


def levels(key, dims, cuts, low, top_value):
    factor_of, own = 1.0, jax.random.fold_in(key, 6)
    for position, blocks in cuts:
        heights = jnp.exp(jax.random.uniform(jax.random.fold_in(own, position), (blocks,), jnp.float32, low / len(cuts), top_value / len(cuts)))
        factor_of = factor_of * jnp.repeat(heights, dims[position] // blocks).reshape([-1 if axis == position else 1 for axis in range(len(dims))])
    return factor_of


def centred(rng, dims, scale, reach, pieces=(), kind=jnp.bfloat16):
    drawn = scale * jax.random.normal(rng, dims, jnp.float32)
    if pieces:
        drawn = drawn * levels(rng, dims, pieces, -0.22, 0.18)
    return jnp.clip(drawn, -reach, reach).astype(kind)


def setup_inputs(seed: int = 0) -> dict:
    splits = jax.random.split(jax.random.key(seed), 15)
    tokens = centred(splits[0], (SEQS, LEN, D), 1.0, 6.0, ((0, 4), (1, 8)))
    ln_gain = jnp.clip(1.0 + 0.1 * jax.random.normal(splits[1], (D,), jnp.float32), 0.5, 1.5).astype(jnp.bfloat16)
    ln_bias = centred(splits[2], (D,), 0.5, 3.0, ((0, 4),))
    qkv_weight = draw_qkv_weight(jax.random.fold_in(splits[14], 71), 0)
    qkv_bias = centred(splits[4], (3 * D,), 0.5, 3.0, ((0, 4),))
    dense_weight = centred(splits[5], (D, D), (D // 16) ** -0.5, 0.5, ((0, 4),))
    dense_bias = centred(splits[6], (D,), 0.5, 3.0, ((0, 4),))
    fc1_weight = centred(splits[7], (D, FF), D ** -0.5, 0.125, ((0, 4),))
    fc1_bias = centred(splits[8], (FF,), 0.5, 3.0, ((0, 4),))
    fc2_weight = centred(splits[9], (FF, D), FF ** -0.5, 0.0625, ((0, 4),))
    fc2_bias = centred(splits[10], (D,), 0.5, 3.0, ((0, 4),))
    segments = draw_segments(jax.random.fold_in(splits[14], 71), 0)
    positions = draw_positions(jax.random.fold_in(splits[14], 71), 0)
    cotangent = centred(splits[13], (SEQS, LEN, D), 1.0, 6.0, ((0, 4), (1, 8)))
    return dict(tokens=tokens, ln_gain=ln_gain, ln_bias=ln_bias, qkv_weight=qkv_weight, qkv_bias=qkv_bias, dense_weight=dense_weight, dense_bias=dense_bias, fc1_weight=fc1_weight, fc1_bias=fc1_bias, fc2_weight=fc2_weight, fc2_bias=fc2_bias, segments=segments, positions=positions, cotangent=cotangent)


@jax.custom_vjp
def low(v):
    return lax.optimization_barrier(v.astype(jnp.bfloat16)).astype(jnp.float32)

@jax.custom_vjp
def low_back(v):
    return v

def low_keep(v):
    return (low(v), None)

def low_pass(kept, grad):
    return (grad,)

def back_keep(v):
    return (v, None)

def back_low(kept, grad):
    return (low(grad),)
low.defvjp(low_keep, low_pass)
low_back.defvjp(back_keep, back_low)
norm_epsilon = 1e-05

def matmul(left_side, right_side):
    return jnp.dot(left_side, right_side, precision=lax.Precision.HIGHEST, preferred_element_type=jnp.float32)

def rotary_angles(pos_row, rot_width):
    inverse = 1.0 / 10000.0 ** (jnp.arange(0, rot_width, 2, dtype=jnp.float32) / rot_width)
    return pos_row.astype(jnp.float32)[:, None] * inverse[None, :]

def rotate_pair(values_in, angles):
    half_width = angles.shape[-1]
    cosine = jnp.cos(angles)[:, None, None, :]
    sine_part = jnp.sin(angles)[:, None, None, :]
    low_half = values_in[..., :half_width]
    high_half = values_in[..., half_width:2 * half_width]
    rest_part = values_in[..., 2 * half_width:]
    return jnp.concatenate([low_half * cosine - high_half * sine_part, high_half * cosine + low_half * sine_part, rest_part], axis=-1)

def attention(queries, keys_all, values, seg_row):
    seq_len = queries.shape[0]
    block_len = min(512, seq_len)
    count_blocks = seq_len // block_len
    score_scale = HEAD ** (-0.5)
    key_place = jnp.arange(seq_len)

    def one_block(per_item):
        query_block, query_seg, query_place = per_item
        scores = jnp.einsum('qhd,khd->hqk', query_block, keys_all, precision=lax.Precision.HIGHEST) * score_scale
        allowed = (key_place[None, :] <= query_place[:, None]) & (query_seg[:, None] == seg_row[None, :])
        scores = low_back(jnp.where(allowed[None], scores, -1e+30))
        row_top = lax.optimization_barrier(jnp.max(scores, axis=-1, keepdims=True))
        raised = jnp.exp(scores - row_top)
        row_total = lax.optimization_barrier(jnp.sum(raised, axis=-1, keepdims=True))
        probabilities = raised / row_total
        return jnp.einsum('hqk,khd->qhd', low(probabilities), values, precision=lax.Precision.HIGHEST)
    blocks = lax.map(jax.checkpoint(one_block), (queries.reshape(count_blocks, block_len, HEADS, HEAD), seg_row.reshape(count_blocks, block_len), key_place.reshape(count_blocks, block_len)))
    return blocks.reshape(seq_len, HEADS * HEAD)

def residual_block(inputs, weights, seg_row, pos_row):
    ln_gain, ln_bias, qkv_weight, qkv_bias, dense_weight, dense_bias, fc1_weight, fc1_bias, fc2_weight, fc2_bias = weights
    seq_len = inputs.shape[0]
    centre = lax.optimization_barrier(jnp.mean(inputs, axis=-1, keepdims=True))
    variance = lax.optimization_barrier(jnp.mean((inputs - centre) ** 2, axis=-1, keepdims=True))
    standard = (inputs - centre) * lax.rsqrt(variance + norm_epsilon)
    normed = low(standard * ln_gain + ln_bias)
    projected = low_back(matmul(normed, qkv_weight) + qkv_bias).reshape(seq_len, 3, HEADS, HEAD)
    angles = rotary_angles(pos_row, ROT)
    turned = low_back(low(rotate_pair(projected[:, :2], angles)))
    value_rows = low_back(low(projected[:, 2]))
    attended = low_back(low(attention(turned[:, 0], turned[:, 1], value_rows, seg_row)))
    branch_att = matmul(attended, dense_weight) + dense_bias
    pre_act = low_back(matmul(normed, fc1_weight) + fc1_bias)
    activated = low(jax.nn.gelu(pre_act, approximate=True))
    branch_mlp = matmul(activated, fc2_weight) + fc2_bias
    return inputs + branch_att + branch_mlp

def reference(tokens, ln_gain, ln_bias, qkv_weight, qkv_bias, dense_weight, dense_bias, fc1_weight, fc1_bias, fc2_weight, fc2_bias, segments, positions, cotangent):
    params = tuple((param.astype(jnp.float32) for param in (ln_gain, ln_bias, qkv_weight, qkv_bias, dense_weight, dense_bias, fc1_weight, fc1_bias, fc2_weight, fc2_bias)))

    def per_sequence(totals, per_item):
        inputs, seg_row, pos_row, upstream = per_item

        def forward(inputs_f, *weights):
            return residual_block(inputs_f, weights, seg_row, pos_row)
        output, pullback = jax.vjp(forward, inputs, *params)
        gradients = pullback(upstream)
        summed = tuple((running + part_grad for running, part_grad in zip(totals, gradients[1:])))
        return (summed, (output.astype(jnp.bfloat16), gradients[0]))
    start_totals = tuple((jnp.zeros_like(param) for param in params))
    totals, (outputs, grad_inputs) = lax.scan(per_sequence, start_totals, (tokens.astype(jnp.float32), segments, positions, cotangent.astype(jnp.float32)))
    return (outputs, grad_inputs, totals[0], totals[1], totals[2], totals[3], totals[4], totals[5], totals[6], totals[7], totals[8], totals[9])
```

```python
import functools

import jax
import jax.numpy as jnp
from jax import lax
from jax.experimental import pallas as pl
from jax.experimental.pallas import tpu as pltpu
from jax.sharding import PartitionSpec as P

HEADS = 32
HEAD = 64
ROT = 32
EPS = 1e-05
DOC_SHIFT = 1023
LANES = 2 * HEAD
BF = jnp.bfloat16
F32 = jnp.float32


def dot(left, right):
    return lax.dot_general(left, right, (((1,), (0,)), ((), ())), preferred_element_type=F32)


def dot_nt(left, right):
    return lax.dot_general(left, right, (((1,), (1,)), ((), ())), preferred_element_type=F32)


def dot_tn(left, right):
    return lax.dot_general(left, right, (((0,), (0,)), ((), ())), preferred_element_type=F32)


def gelu_tanh(values_in):
    return jax.nn.gelu(values_in, approximate=True)


def turn(values, cos, sin_low, sin_high):
    half = ROT // 2
    return (
        values * cos
        - pltpu.roll(values, LANES - half, 1) * sin_low
        + pltpu.roll(values, half, 1) * sin_high
    )


def attention_kernel(
    rows, proj, grad_out, cos, sin_low, sin_high, seg_col, seg_row,
    out, grad_proj, qs, ks, vs, dk, dv,
):
    length = proj.shape[0]
    blocks = length // rows
    scale = HEAD**-0.5
    for i in range(blocks):
        r = slice(i * rows, (i + 1) * rows)
        c, lo, hi = cos[r, :], sin_low[r, :], sin_high[r, :]
        qs[r, :] = turn(proj[r, 0:LANES], c, lo, hi).astype(BF) * jnp.asarray(scale, BF)
        ks[r, :] = turn(proj[r, LANES : 2 * LANES], c, lo, hi).astype(BF)
        vs[r, :] = proj[r, 2 * LANES : 3 * LANES].astype(BF)
    lane = lax.broadcasted_iota(jnp.int32, (rows, LANES), 1)
    first = lane < HEAD
    zero = jnp.zeros((rows, LANES), BF)
    for i in reversed(range(blocks)):
        r = slice(i * rows, (i + 1) * rows)
        n = (i + 1) * rows
        place_q = i * rows + lax.broadcasted_iota(jnp.int32, (rows, n), 0)
        place_k = lax.broadcasted_iota(jnp.int32, (rows, n), 1)
        allowed = (place_k <= place_q) & (seg_col[r, :] == seg_row[:, 0:n])
        q2, g2 = qs[r, :], grad_out[r, :]
        k, v = ks[0:n, :], vs[0:n, :]
        o_parts, dq_parts = [], []
        for h in range(2):
            mine = first if h == 0 else ~first
            q = jnp.where(mine, q2, zero)
            g = jnp.where(mine, g2, zero)
            s = jnp.where(allowed, dot_nt(q, k), -1e30)
            e = jnp.exp(s - jnp.max(s, axis=-1, keepdims=True))
            p = e * (1.0 / jnp.sum(e, axis=-1, keepdims=True))
            pb = p.astype(BF)
            o_parts.append(dot(pb, v))
            dp = dot_nt(g, v)
            inner = jnp.sum(p * dp, axis=-1, keepdims=True)
            ds = (p * (dp - inner)).astype(BF)
            dq_parts.append(dot(ds, k))
            dk_new, dv_new = dot_tn(ds, q), dot_tn(pb, g)
            if i == blocks - 1 and h == 0:
                dk[...] = dk_new
                dv[...] = dv_new
            else:
                dk[0:n, :] += dk_new
                dv[0:n, :] += dv_new
        out[r, :] = jnp.where(first, o_parts[0], o_parts[1]).astype(BF)
        dq = (jnp.where(first, dq_parts[0], dq_parts[1]) * scale).astype(BF).astype(F32)
        c, lo, hi = cos[r, :], sin_low[r, :], sin_high[r, :]
        grad_proj[r, 0:LANES] = turn(dq, c, -lo, -hi).astype(BF)
    for i in range(blocks):
        r = slice(i * rows, (i + 1) * rows)
        c, lo, hi = cos[r, :], sin_low[r, :], sin_high[r, :]
        grad_k = dk[r, :].astype(BF).astype(F32)
        grad_proj[r, LANES : 2 * LANES] = turn(grad_k, c, -lo, -hi).astype(BF)
        grad_proj[r, 2 * LANES : 3 * LANES] = dv[r, :].astype(BF)


def attention(proj, grad_att, tables, segments):
    length = proj.shape[0]
    pairs = grad_att.shape[1] // LANES
    rows = 256
    whole = lambda shape: pl.BlockSpec(shape, lambda p: (0, 0))
    return pl.pallas_call(
        functools.partial(attention_kernel, rows),
        grid=(pairs,),
        out_shape=(
            jax.ShapeDtypeStruct((length, pairs * LANES), BF),
            jax.ShapeDtypeStruct((length, 3 * pairs * LANES), BF),
        ),
        in_specs=[
            pl.BlockSpec((length, 3 * LANES), lambda p: (0, p)),
            pl.BlockSpec((length, LANES), lambda p: (0, p)),
            whole((length, LANES)),
            whole((length, LANES)),
            whole((length, LANES)),
            whole((length, 1)),
            whole((1, length)),
        ],
        out_specs=(
            pl.BlockSpec((length, LANES), lambda p: (0, p)),
            pl.BlockSpec((length, 3 * LANES), lambda p: (0, p)),
        ),
        scratch_shapes=[pltpu.VMEM((length, LANES), BF)] * 3
        + [pltpu.VMEM((length, LANES), F32)] * 2,
        cost_estimate=pl.CostEstimate(
            flops=14 * pairs * length * length * LANES,
            bytes_accessed=pairs * length * LANES * 24,
            transcendentals=pairs * length * length,
        ),
    )(proj, grad_att, *tables, segments[:, None], segments[None, :])


def angle_tables(seg_row):
    length = seg_row.shape[0]
    position = jnp.arange(length, dtype=jnp.int32) + jnp.where(seg_row > 0, DOC_SHIFT, 0)
    half = ROT // 2
    inverse = 1.0 / 10000.0 ** (jnp.arange(0, ROT, 2, dtype=F32) / ROT)
    angles = position.astype(F32)[:, None] * inverse[None, :]
    cosine, sine = jnp.cos(angles), jnp.sin(angles)
    ones = jnp.ones((length, HEAD - ROT), F32)
    zeros = jnp.zeros((length, HEAD - ROT), F32)
    none = jnp.zeros((length, half), F32)
    cos = jnp.concatenate([cosine, cosine, ones] * 2, axis=1)
    low = jnp.concatenate([sine, none, zeros] * 2, axis=1)
    high = jnp.concatenate([none, sine, zeros] * 2, axis=1)
    return cos, low, high


def body(
    tokens,
    ln_gain,
    ln_bias,
    qkv_weight,
    qkv_bias,
    dense_weight,
    dense_bias,
    fc1_weight,
    fc1_bias,
    fc2_weight,
    fc2_bias,
    segments,
    positions,
    cotangent,
):
    S, F = lax.axis_size("seq"), lax.axis_size("fsdp")
    j, f = lax.axis_index("seq"), lax.axis_index("fsdp")
    tok, D = tokens.shape[1], tokens.shape[2]
    length = tok * S
    rows_d = D // F
    ff = fc1_weight.shape[1]
    cols_up = ff // S
    block_up = cols_up // F
    hp = HEADS // S
    pairs = hp // 2
    per_shard = HEADS // F
    spread = per_shard % S == 0
    slots = per_shard // S if spread else 0

    def heads_of(array, lead):
        shape = array.shape
        if spread:
            split = array.reshape(shape[:lead] + (F, S, slots) + shape[lead + 1 :])
            mine = lax.dynamic_index_in_dim(split, j, lead + 1, keepdims=False)
            return mine.reshape(shape[:lead] + (hp,) + shape[lead + 1 :])
        return lax.dynamic_slice_in_dim(array, j * hp, hp, lead)

    def qkv_cols(array):
        n = array.shape[0]
        mine = heads_of(array.reshape(n, 3, HEADS, HEAD), 2)
        return mine.reshape(n, 3, pairs, 2, HEAD).transpose(0, 2, 1, 3, 4).reshape(n, -1)

    small = jnp.concatenate([ln_gain, ln_bias, qkv_bias, dense_bias, fc1_bias, fc2_bias])
    small = lax.all_gather(small, "fsdp", axis=0)
    cuts, at = [], 0
    for piece in (ln_gain, ln_bias, qkv_bias, dense_bias, fc1_bias, fc2_bias):
        cuts.append(small[:, at : at + piece.shape[0]].reshape(-1).astype(F32))
        at += piece.shape[0]
    gain, shift, b_qkv, b_dense, b_up, b_down = cuts

    inputs = tokens[0].astype(F32)
    centre = jnp.mean(inputs, axis=-1, keepdims=True)
    variance = jnp.mean((inputs - centre) ** 2, axis=-1, keepdims=True)
    inv_std = lax.rsqrt(variance + EPS)
    standard = (inputs - centre) * inv_std
    normed_own = (standard * gain + shift).astype(BF)
    upstream_own = cotangent[0]
    normed = lax.all_gather(normed_own, "seq", axis=0, tiled=True)
    upstream = lax.all_gather(upstream_own, "seq", axis=0, tiled=True)

    up_own = lax.dynamic_index_in_dim(
        fc1_weight.reshape(rows_d, F, S, block_up), j, 2, keepdims=False
    ).reshape(rows_d, cols_up)
    w_up = lax.all_gather(up_own, "fsdp", axis=0, tiled=True)
    down_own = lax.dynamic_slice_in_dim(fc2_weight, j * block_up, block_up, 0)
    w_down = lax.all_gather(down_own, "fsdp", axis=0, tiled=True)
    w_qkv = lax.all_gather(qkv_cols(qkv_weight), "fsdp", axis=0, tiled=True)
    if spread:
        block_dense = slots * HEAD
        dense_own = lax.dynamic_slice_in_dim(dense_weight, j * block_dense, block_dense, 0)
        w_dense = lax.all_gather(dense_own, "fsdp", axis=0, tiled=True)
    else:
        w_dense = lax.dynamic_slice_in_dim(
            lax.all_gather(dense_weight, "fsdp", axis=0, tiled=True), j * hp * HEAD, hp * HEAD, 0
        )

    bias_up = lax.dynamic_index_in_dim(b_up.reshape(F, S, block_up), j, 1, keepdims=False)
    bias_up = bias_up.reshape(-1)
    bias_qkv = qkv_cols(b_qkv[None])[0]
    seg_row = segments[0]

    pre_act = dot(normed, w_up) + bias_up
    activated = gelu_tanh(pre_act).astype(BF)
    grad_act = dot_nt(upstream, w_down)
    grad_pre = jax.vjp(gelu_tanh, pre_act)[1](grad_act)[0].astype(BF)
    projected = dot(normed, w_qkv) + bias_qkv
    grad_att = dot_nt(upstream, w_dense).astype(BF)
    attended, grad_mixed = attention(projected, grad_att, angle_tables(seg_row), seg_row)

    partial_out = dot(attended, w_dense) + dot(activated, w_down)
    branches = lax.psum_scatter(partial_out.astype(BF), "seq", scatter_dimension=0, tiled=True)
    result = (inputs + branches.astype(F32) + (b_dense + b_down)).astype(BF)

    partial_normed = dot_nt(grad_mixed, w_qkv) + dot_nt(grad_pre, w_up)
    grad_normed = lax.psum_scatter(
        partial_normed.astype(BF), "seq", scatter_dimension=0, tiled=True
    ).astype(F32)
    scaled = grad_normed * gain
    grad_inputs = upstream_own.astype(F32) + inv_std * (
        scaled
        - jnp.mean(scaled, axis=-1, keepdims=True)
        - standard * jnp.mean(scaled * standard, axis=-1, keepdims=True)
    )

    def summed(left, right):
        return lax.psum_scatter(
            dot_tn(left, right).astype(BF), "fsdp", scatter_dimension=0, tiled=True
        )

    piece_down = summed(activated, upstream)
    piece_up = summed(normed, grad_pre)
    piece_qkv = summed(normed, grad_mixed)
    grad_down = lax.all_gather(piece_down, "seq", axis=0, tiled=True).astype(F32)
    grad_up = (
        lax.all_gather(piece_up, "seq", axis=0)
        .reshape(S, rows_d, F, block_up)
        .transpose(1, 2, 0, 3)
        .reshape(rows_d, ff)
        .astype(F32)
    )

    def to_heads(array, lead):
        shape = array.shape
        if spread:
            split = array.reshape(shape[: 1 + lead] + (F, slots) + shape[2 + lead :])
            moved = jnp.moveaxis(split, 0, lead + 1)
        else:
            moved = jnp.moveaxis(array, 0, lead)
        return moved.reshape(shape[1 : 1 + lead] + (HEADS,) + shape[2 + lead :])

    def from_qkv_cols(gathered):
        n = gathered.shape[1]
        split = gathered.reshape(S, n, pairs, 3, 2, HEAD).transpose(0, 1, 3, 2, 4, 5)
        return to_heads(split.reshape(S, n, 3, hp, HEAD), 2).reshape(n, -1)

    grad_qkv = from_qkv_cols(lax.all_gather(piece_qkv, "seq", axis=0)).astype(F32)
    if spread:
        piece_dense = summed(attended, upstream)
        grad_dense = lax.all_gather(piece_dense, "seq", axis=0, tiled=True).astype(F32)
    else:
        part = lax.all_gather(dot_tn(attended, upstream).astype(BF), "seq", axis=0, tiled=True)
        grad_dense = lax.psum_scatter(part, "fsdp", scatter_dimension=0, tiled=True).astype(F32)

    ln_terms = jnp.concatenate(
        [jnp.sum(grad_normed * standard, axis=0), jnp.sum(grad_normed, axis=0)]
    )
    ln_terms = lax.psum_scatter(ln_terms, "seq", scatter_dimension=0, tiled=True)
    out_term = jnp.sum(upstream.astype(F32), axis=0)
    out_term = lax.dynamic_slice_in_dim(out_term, j * (D // S), D // S, 0)
    up_term = jnp.sum(grad_pre.astype(F32), axis=0)
    qkv_term = jnp.sum(grad_mixed.astype(F32), axis=0)
    terms = lax.psum(jnp.concatenate([ln_terms, out_term, up_term, qkv_term]), "fsdp")
    terms = lax.all_gather(terms, "seq", axis=0)
    n_ln = 2 * D // S
    n_out = n_ln + D // S
    n_up = n_out + cols_up
    ln_full = terms[:, :n_ln].reshape(2, F, rows_d)
    ln_mine = lax.dynamic_index_in_dim(ln_full, f, 1, keepdims=False)
    out_full = terms[:, n_ln:n_out].reshape(F, rows_d)
    out_mine = lax.dynamic_index_in_dim(out_full, f, 0, keepdims=False)
    up_full = terms[:, n_out:n_up].reshape(S, F, block_up)
    up_mine = lax.dynamic_index_in_dim(up_full, f, 1, keepdims=False).reshape(-1)
    qkv_full = from_qkv_cols(terms[:, n_up:][:, None]).reshape(F, -1)
    qkv_mine = lax.dynamic_index_in_dim(qkv_full, f, 0, keepdims=False)
    return (
        result[None],
        grad_inputs[None],
        ln_mine[0],
        ln_mine[1],
        grad_qkv,
        qkv_mine,
        grad_dense,
        out_mine,
        grad_up,
        up_mine,
        grad_down,
        out_mine,
    )


def solution(mesh):
    row, mat = P("fsdp"), P("fsdp", None)
    act = P("fsdp", "seq", None)
    return jax.shard_map(
        body,
        mesh=mesh,
        in_specs=(
            act, row, row, mat, row, mat, row, mat, row, mat, row, mat, P("fsdp", "seq"), act,
        ),
        out_specs=(act, act, row, row, mat, row, mat, row, mat, row, mat, row),
        check_vma=False,
    )
```

```python
import functools

import jax
import jax.numpy as jnp
from jax import lax
from jax.experimental import pallas as pl
from jax.experimental.pallas import tpu as pltpu
from jax.sharding import PartitionSpec as P


HEADS = 32
HEAD = 64
ROT = 32
EPS = 1e-05
DOC_SHIFT = 1023
LANES = 2 * HEAD
BF = jnp.bfloat16
F32 = jnp.float32


def dot(left, right):
    return lax.dot_general(left, right, (((1,), (0,)), ((), ())), preferred_element_type=F32)


def dot_nt(left, right):
    return lax.dot_general(left, right, (((1,), (1,)), ((), ())), preferred_element_type=F32)


def dot_tn(left, right):
    return lax.dot_general(left, right, (((0,), (0,)), ((), ())), preferred_element_type=F32)


def gelu_tanh(values_in):
    return jax.nn.gelu(values_in, approximate=True)


def turn(values, cos, sin_low, sin_high):
    half = ROT // 2
    return (
        values * cos
        - pltpu.roll(values, LANES - half, 1) * sin_low
        + pltpu.roll(values, half, 1) * sin_high
    )


def attention_kernel(
    rows, proj, grad_out, cos, sin_low, sin_high, seg_col, seg_row,
    out, grad_proj, qs, ks, vs, dk, dv,
):
    length = proj.shape[0]
    blocks = length // rows
    scale = HEAD**-0.5
    for i in range(blocks):
        r = slice(i * rows, (i + 1) * rows)
        c, lo, hi = cos[r, :], sin_low[r, :], sin_high[r, :]
        qs[r, :] = turn(proj[r, 0:LANES], c, lo, hi).astype(BF) * jnp.asarray(scale, BF)
        ks[r, :] = turn(proj[r, LANES : 2 * LANES], c, lo, hi).astype(BF)
        vs[r, :] = proj[r, 2 * LANES : 3 * LANES].astype(BF)
    lane = lax.broadcasted_iota(jnp.int32, (rows, LANES), 1)
    first = lane < HEAD
    zero = jnp.zeros((rows, LANES), BF)
    for i in reversed(range(blocks)):
        r = slice(i * rows, (i + 1) * rows)
        n = (i + 1) * rows
        place_q = i * rows + lax.broadcasted_iota(jnp.int32, (rows, n), 0)
        place_k = lax.broadcasted_iota(jnp.int32, (rows, n), 1)
        allowed = (place_k <= place_q) & (seg_col[r, :] == seg_row[:, 0:n])
        q2, g2 = qs[r, :], grad_out[r, :]
        k, v = ks[0:n, :], vs[0:n, :]
        o_parts, dq_parts = [], []
        for h in range(2):
            mine = first if h == 0 else ~first
            q = jnp.where(mine, q2, zero)
            g = jnp.where(mine, g2, zero)
            s = jnp.where(allowed, dot_nt(q, k), -1e30)
            e = jnp.exp(s - jnp.max(s, axis=-1, keepdims=True))
            p = e * (1.0 / jnp.sum(e, axis=-1, keepdims=True))
            pb = p.astype(BF)
            o_parts.append(dot(pb, v))
            dp = dot_nt(g, v)
            inner = jnp.sum(p * dp, axis=-1, keepdims=True)
            ds = (p * (dp - inner)).astype(BF)
            dq_parts.append(dot(ds, k))
            dk_new, dv_new = dot_tn(ds, q), dot_tn(pb, g)
            if i == blocks - 1 and h == 0:
                dk[...] = dk_new
                dv[...] = dv_new
            else:
                dk[0:n, :] += dk_new
                dv[0:n, :] += dv_new
        out[r, :] = jnp.where(first, o_parts[0], o_parts[1]).astype(BF)
        dq = (jnp.where(first, dq_parts[0], dq_parts[1]) * scale).astype(BF).astype(F32)
        c, lo, hi = cos[r, :], sin_low[r, :], sin_high[r, :]
        grad_proj[r, 0:LANES] = turn(dq, c, -lo, -hi).astype(BF)
    for i in range(blocks):
        r = slice(i * rows, (i + 1) * rows)
        c, lo, hi = cos[r, :], sin_low[r, :], sin_high[r, :]
        grad_k = dk[r, :].astype(BF).astype(F32)
        grad_proj[r, LANES : 2 * LANES] = turn(grad_k, c, -lo, -hi).astype(BF)
        grad_proj[r, 2 * LANES : 3 * LANES] = dv[r, :].astype(BF)


def attention(proj, grad_att, tables, segments):
    length = proj.shape[0]
    pairs = grad_att.shape[1] // LANES
    rows = 256
    whole = lambda shape: pl.BlockSpec(shape, lambda p: (0, 0))
    return pl.pallas_call(
        functools.partial(attention_kernel, rows),
        grid=(pairs,),
        out_shape=(
            jax.ShapeDtypeStruct((length, pairs * LANES), BF),
            jax.ShapeDtypeStruct((length, 3 * pairs * LANES), BF),
        ),
        in_specs=[
            pl.BlockSpec((length, 3 * LANES), lambda p: (0, p)),
            pl.BlockSpec((length, LANES), lambda p: (0, p)),
            whole((length, LANES)),
            whole((length, LANES)),
            whole((length, LANES)),
            whole((length, 1)),
            whole((1, length)),
        ],
        out_specs=(
            pl.BlockSpec((length, LANES), lambda p: (0, p)),
            pl.BlockSpec((length, 3 * LANES), lambda p: (0, p)),
        ),
        scratch_shapes=[pltpu.VMEM((length, LANES), BF)] * 3
        + [pltpu.VMEM((length, LANES), F32)] * 2,
        cost_estimate=pl.CostEstimate(
            flops=14 * pairs * length * length * LANES,
            bytes_accessed=pairs * length * LANES * 24,
            transcendentals=pairs * length * length,
        ),
    )(proj, grad_att, *tables, segments[:, None], segments[None, :])


def angle_tables(seg_row):
    length = seg_row.shape[0]
    position = jnp.arange(length, dtype=jnp.int32) + jnp.where(seg_row > 0, DOC_SHIFT, 0)
    half = ROT // 2
    inverse = 1.0 / 10000.0 ** (jnp.arange(0, ROT, 2, dtype=F32) / ROT)
    angles = position.astype(F32)[:, None] * inverse[None, :]
    cosine, sine = jnp.cos(angles), jnp.sin(angles)
    ones = jnp.ones((length, HEAD - ROT), F32)
    zeros = jnp.zeros((length, HEAD - ROT), F32)
    none = jnp.zeros((length, half), F32)
    cos = jnp.concatenate([cosine, cosine, ones] * 2, axis=1)
    low = jnp.concatenate([sine, none, zeros] * 2, axis=1)
    high = jnp.concatenate([none, sine, zeros] * 2, axis=1)
    return cos, low, high


MESH = pl.DeviceIdType.MESH


def remote(src, dst, send, recv, device):
    return pltpu.make_async_remote_copy(
        src_ref=src, dst_ref=dst, send_sem=send, recv_sem=recv, device_id=device,
        device_id_type=MESH,
    )


class Place:
    def __init__(self, S, F):
        self.S, self.F, self.Q = S, F, S // 2
        self.j, self.f = lax.axis_index("seq"), lax.axis_index("fsdp")
        self.q, self.c = self.j // 2, lax.rem(self.j, 2)
        self.partner = 2 * self.q + 1 - self.c

    def greet(self, over_fsdp, over_seq):
        barrier = pltpu.get_barrier_semaphore()
        count = 0
        if over_fsdp:
            for k in range(1, self.F):
                pl.semaphore_signal(
                    barrier, inc=1, device_id=(self.j, lax.rem(self.f + k, self.F)),
                    device_id_type=MESH,
                )
            count = self.F - 1
        if over_seq:
            pl.semaphore_signal(
                barrier, inc=1, device_id=(self.partner, self.f), device_id_type=MESH
            )

            @pl.when(self.q > 0)
            def _():
                pl.semaphore_signal(
                    barrier, inc=1, device_id=(self.j - 2, self.f), device_id_type=MESH
                )

            @pl.when(self.q < self.Q - 1)
            def _():
                pl.semaphore_signal(
                    barrier, inc=1, device_id=(self.j + 2, self.f), device_id_type=MESH
                )

            count += 1 + (self.q + self.Q - 1) // self.Q + (2 * self.Q - 2 - self.q) // self.Q
        pl.semaphore_wait(barrier, count)


class ShardGather:
    @staticmethod
    def scratch(F):
        n = 6 if F == 4 else F - 1
        return [pltpu.SemaphoreType.DMA((n,)), pltpu.SemaphoreType.DMA((n,)),
                pltpu.SemaphoreType.DMA]

    def __init__(self, at, src, dst, send, recv, local):
        self.at, self.src, self.dst = at, src, dst
        f, j = at.f, at.j
        self.own = pltpu.make_async_copy(src, dst.at[f], local)
        self.first, self.later, self.arrivals = [], [], []
        if at.F == 4:
            nx = f + 1 - 2 * lax.rem(f, 2)
            ny = lax.rem(f + 2, 4)
            nd = lax.rem(nx + 2, 4)
            half = src.shape[0] // 2
            a, b = pl.ds(0, half), pl.ds(half, half)
            table = ((nx, a), (nx, b), (ny, a), (ny, b))
            for i, (to, rows) in enumerate(table):
                self.first.append(
                    remote(src.at[rows], dst.at[f, rows], send.at[i], recv.at[i], (j, to))
                )
                self.arrivals.append(
                    remote(src.at[rows], dst.at[to, rows], send.at[i], recv.at[i], (j, to))
                )
            for i, (of, rows, to) in ((4, (nx, a, ny)), (5, (ny, b, nx))):
                self.later.append(
                    remote(dst.at[of, rows], dst.at[of, rows], send.at[i], recv.at[i], (j, to))
                )
                self.arrivals.append(
                    remote(dst.at[nd, rows], dst.at[nd, rows], send.at[i], recv.at[i], (j, to))
                )
        else:
            for k in range(1, at.F):
                to, of = lax.rem(f + k, at.F), lax.rem(f + at.F - k, at.F)
                self.first.append(
                    remote(src, dst.at[f], send.at[k - 1], recv.at[k - 1], (j, to))
                )
                self.arrivals.append(
                    remote(src, dst.at[of], send.at[k - 1], recv.at[k - 1], (j, to))
                )

    def start(self):
        self.own.start()
        for copy in self.first:
            copy.start()

    def relay(self):
        if self.later:
            self.arrivals[0].wait_recv()
            self.later[0].start()
            self.arrivals[3].wait_recv()
            self.later[1].start()

    def finish(self):
        for i, copy in enumerate(self.arrivals):
            if not (self.later and i in (0, 3)):
                copy.wait_recv()
        for copy in self.first + self.later:
            copy.wait_send()
        self.own.wait()


class TokenGather:
    @staticmethod
    def scratch(S):
        Q = S // 2
        return [pltpu.SemaphoreType.DMA((2 * Q,)), pltpu.SemaphoreType.DMA((2 * Q,)),
                pltpu.SemaphoreType.DMA((S,)), pltpu.SemaphoreType.DMA]

    def __init__(self, at, src, dst, send, share, recv, local):
        self.at, self.src, self.dst = at, src, dst
        self.send, self.share, self.recv = send, share, recv
        self.own = pltpu.make_async_copy(src, dst.at[at.j], local)

    def onward(self, slot, source, i, by):
        to = self.dst.at[slot]
        return remote(
            source, to, self.send.at[i], self.recv.at[slot], (self.at.j + by, self.at.f)
        )

    def given(self, slot, source, i):
        to = self.dst.at[slot]
        return remote(
            source, to, self.share.at[i], self.recv.at[slot], (self.at.partner, self.at.f)
        )

    def plan(self, d):
        at, Q = self.at, self.at.Q
        below, above = at.j - 2 * d, at.j + 2 * d
        dst = self.dst
        return (
            (at.q >= d, self.onward(below, dst.at[below], d, 2), at.q < Q - 1,
             self.given(below, dst.at[below], d)),
            (at.q + d <= Q - 1, self.onward(above, dst.at[above], Q + d, -2), at.q > 0,
             self.given(above, dst.at[above], Q + d)),
        )

    def ends(self):
        j, Q = self.at.j, self.at.Q
        return (
            self.onward(j, self.src, 0, 2), self.onward(j, self.src, Q, -2),
            self.given(j, self.src, 0),
        )

    def start(self):
        at, Q = self.at, self.at.Q
        self.own.start()
        up, down, part = self.ends()

        @pl.when(at.q < Q - 1)
        def _():
            up.start()

        @pl.when(at.q > 0)
        def _():
            down.start()

        part.start()

    def step(self, d):
        for valid, onward, go, part in self.plan(d):

            @pl.when(valid)
            def _():
                onward.wait_recv()

                @pl.when(go)
                def _():
                    onward.start()

                part.start()

    def finish(self):
        at, Q = self.at, self.at.Q
        for q in range(Q):
            slot = 2 * q + 1 - at.c
            self.given(slot, self.dst.at[slot], 0).wait_recv()
        up, down, part = self.ends()

        @pl.when(at.q < Q - 1)
        def _():
            up.wait_send()

        @pl.when(at.q > 0)
        def _():
            down.wait_send()

        part.wait_send()
        for d in range(1, Q):
            for valid, onward, go, part in self.plan(d):

                @pl.when(valid & go)
                def _():
                    onward.wait_send()

                @pl.when(valid)
                def _():
                    part.wait_send()

        self.own.wait()


class GradReduce:
    @staticmethod
    def scratch(F, rows, n):
        return [pltpu.VMEM((F, rows, n), BF), pltpu.VMEM((F - 1, rows, n), BF),
                pltpu.SemaphoreType.DMA((F - 1,)), pltpu.SemaphoreType.DMA((F - 1,))]

    def __init__(self, at, left, right, extra, made, got, send, recv):
        self.at, self.left, self.right, self.extra = at, left, right, extra
        self.made, self.got, self.send, self.recv = made, got, send, recv
        self.n = right.shape[1]
        self.rows = left.shape[1] // at.F
        self.tile = 512 if self.n % 512 == 0 else 256 if self.n % 256 == 0 else 128

    def copy(self, k):
        at = self.at
        to = lax.rem(at.f + k, at.F)
        return remote(
            self.made.at[to], self.got.at[k - 1], self.send.at[k - 1], self.recv.at[k - 1],
            (at.j, to),
        )

    def start(self):
        at, rows = self.at, self.rows
        aligned = rows % 128 == 0
        for t in range(0, self.n, self.tile) if not aligned else ():
            cols = slice(t, t + self.tile)
            full = dot_tn(self.left[...], self.right[:, cols]).astype(BF)
            for p in range(at.F):
                self.made[p, 0:rows, cols] = full[p * rows : (p + 1) * rows, :]
        for k in list(range(1, at.F)) + [0]:
            p = lax.rem(at.f + k, at.F)
            if aligned:
                block = self.left[:, pl.ds(pl.multiple_of(p * rows, 128), rows)]
                for t in range(0, self.n, self.tile):
                    cols = slice(t, t + self.tile)
                    self.made[p, 0:rows, cols] = dot_tn(block, self.right[:, cols]).astype(BF)
            if self.extra is not None:
                self.made[p, rows : rows + self.extra.shape[1], :] = self.extra[p].astype(BF)
            if k:
                self.copy(k).start()

    def finish(self, store):
        at = self.at
        for k in range(1, at.F):
            self.copy(k).wait_recv()
        for t in range(0, self.n, self.tile):
            cols = slice(t, t + self.tile)
            total = self.made[at.f, :, cols].astype(F32)
            for k in range(1, at.F):
                total += self.got[k - 1, :, cols].astype(F32)
            store(t, self.tile, total.astype(BF))
        for k in range(1, at.F):
            self.copy(k).wait_send()


EXTRA = 16


def exchange(S, F, collective_id, grads=(), shards=(), tokens=(), merge=None):
    operands, in_specs = [], []
    vmem = pl.BlockSpec(memory_space=pltpu.VMEM)
    outs, out_specs, scratch = [], [], []
    shapes, row = [], 0
    for left, right, extra in grads:
        rows, n = left.shape[1] // F + (0 if extra is None else EXTRA), right.shape[1]
        operands += [left, right] + ([] if extra is None else [extra])
        scratch += GradReduce.scratch(F, rows, n)
        shapes.append((rows, n, row))
        row += rows * pl.cdiv(n, merge or n)
        if not merge:
            outs.append(jax.ShapeDtypeStruct((rows, n), BF))
    if merge:
        outs.append(jax.ShapeDtypeStruct((row, merge), BF))
    out_specs += [vmem] * len(outs)
    for array in shards:
        operands.append(array)
        outs.append(jax.ShapeDtypeStruct((F,) + array.shape, BF))
        out_specs.append(pl.BlockSpec(memory_space=pl.ANY))
        scratch += ShardGather.scratch(F)
    for array in tokens:
        operands.append(array)
        outs.append(jax.ShapeDtypeStruct((S,) + array.shape, BF))
        out_specs.append(pl.BlockSpec(memory_space=pl.ANY))
        scratch += TokenGather.scratch(S)
    in_specs = [vmem] * len(operands)
    n_in, n_out = len(operands), len(outs)

    def kernel(*refs):
        ins, results, rest = list(refs[:n_in]), list(refs[n_in : n_in + n_out]), list(
            refs[n_in + n_out :]
        )
        take = lambda items, n: [items.pop(0) for _ in range(n)]
        at = Place(S, F)
        jobs, stores = [], []
        packed = take(results, 1)[0] if merge else None
        for (_, _, extra), (rows, n, row0) in zip(grads, shapes):
            left, right = take(ins, 2)
            extra_ref = None if extra is None else take(ins, 1)[0]
            jobs.append(GradReduce(at, left, right, extra_ref, *take(rest, 4)))
            target = packed if merge else take(results, 1)[0]

            def store(t, width, value, target=target, rows=rows, row0=row0):
                if not merge:
                    target[:, t : t + width] = value
                    return
                while width:
                    chunk, col = divmod(t, merge)
                    part = min(width, merge - col)
                    target[row0 + chunk * rows : row0 + (chunk + 1) * rows, col : col + part] = (
                        value[:, :part]
                    )
                    value, t, width = value[:, part:], t + part, width - part

            stores.append(store)
        spreads = [
            ShardGather(at, take(ins, 1)[0], take(results, 1)[0], *take(rest, 3)) for _ in shards
        ]
        lines = [
            TokenGather(at, take(ins, 1)[0], take(results, 1)[0], *take(rest, 4)) for _ in tokens
        ]
        at.greet(bool(jobs or spreads), bool(lines))
        for item in lines + spreads:
            item.start()
        for job in jobs:
            job.start()
        waiting = list(spreads)
        for d in range(1, at.Q) if lines else ():
            for item in lines:
                item.step(d)
            if waiting:
                waiting.pop(0).relay()
        for item in waiting:
            item.relay()
        for job, store in zip(jobs, stores):
            job.finish(store)
        for item in spreads + lines:
            item.finish()

    flops = sum(2 * l.shape[0] * l.shape[1] * r.shape[1] for l, r, _ in grads)
    moved = sum(o.size * 2 for o in outs)
    return pl.pallas_call(
        kernel,
        out_shape=tuple(outs),
        in_specs=in_specs,
        out_specs=tuple(out_specs),
        scratch_shapes=scratch,
        compiler_params=pltpu.CompilerParams(
            collective_id=collective_id, has_side_effects=True
        ),
        cost_estimate=pl.CostEstimate(
            flops=flops, bytes_accessed=20 * moved, transcendentals=0
        ),
    )(*operands)


def seq_sum(S, F, collective_id, arrays):
    Q = S // 2
    t, d = arrays[0].shape[1:]
    n = len(arrays)

    def kernel(*refs):
        at = Place(S, F)
        jobs = []
        for i in range(n):
            scratch = refs[2 * n + 7 * i : 2 * n + 7 * (i + 1)]
            jobs.append((refs[i], refs[n + i]) + tuple(scratch))
        at.greet(False, True)

        def share(job, q):
            part, _, pair, _, _, _, _, s_pair, r_pair = job[:9]
            return remote(
                part.at[2 * q + 1 - at.c], pair.at[q], s_pair.at[q], r_pair.at[q],
                (at.partner, at.f),
            )

        def hop(job, q, up):
            _, _, _, buf, got, s_line, r_line, _, _ = job[:9]
            i = q if up else Q + q
            return remote(
                buf.at[i], got.at[i], s_line.at[i], r_line.at[i],
                (at.j + 2 if up else at.j - 2, at.f),
            )

        order = []
        for i in range(Q):
            for q in (Q - 1 - i, i):
                if q not in order:
                    order.append(q)
        for q in order:
            for job in jobs:
                share(job, q).start()

        def base(job, q):
            share(job, q).wait_recv()
            return job[0][2 * q + at.c].astype(F32) + job[2][q].astype(F32)

        for i in range(Q - 1):
            for job in jobs:
                for q, up in ((Q - 1 - i, True), (i, False)):
                    sends = at.q < q if up else at.q > q
                    inner = at.q > 0 if up else at.q < Q - 1
                    copy = hop(job, q, up)
                    slot = q if up else Q + q

                    @pl.when(sends)
                    def _():
                        value = base(job, q)
                        job[3][slot] = value.astype(BF)

                        @pl.when(inner)
                        def _():
                            copy.wait_recv()
                            job[3][slot] = (value + job[4][slot].astype(F32)).astype(BF)

                        copy.start()

        for job in jobs:
            for q in range(Q):

                @pl.when(at.q == q)
                def _():
                    job[1][...] = base(job, q)
                    if q > 0:
                        hop(job, q, True).wait_recv()
                        job[1][...] += job[4][q].astype(F32)
                    if q < Q - 1:
                        hop(job, q, False).wait_recv()
                        job[1][...] += job[4][Q + q].astype(F32)

        for job in jobs:
            for q in range(Q):
                share(job, q).wait_send()

                @pl.when(at.q < q)
                def _():
                    hop(job, q, True).wait_send()

                @pl.when(at.q > q)
                def _():
                    hop(job, q, False).wait_send()

    vmem = pl.BlockSpec(memory_space=pltpu.VMEM)
    scratch = [
        pltpu.VMEM((Q, t, d), BF),
        pltpu.VMEM((2 * Q, t, d), BF),
        pltpu.VMEM((2 * Q, t, d), BF),
        pltpu.SemaphoreType.DMA((2 * Q,)),
        pltpu.SemaphoreType.DMA((2 * Q,)),
        pltpu.SemaphoreType.DMA((Q,)),
        pltpu.SemaphoreType.DMA((Q,)),
    ]
    return pl.pallas_call(
        kernel,
        out_shape=tuple(jax.ShapeDtypeStruct((t, d), F32) for _ in arrays),
        in_specs=[vmem] * n,
        out_specs=tuple([vmem] * n),
        scratch_shapes=scratch * n,
        compiler_params=pltpu.CompilerParams(
            collective_id=collective_id, has_side_effects=True
        ),
        cost_estimate=pl.CostEstimate(
            flops=n * S * t * d, bytes_accessed=40 * n * S * t * d, transcendentals=0
        ),
    )(*arrays)


def half_lanes(first, second, odd):
    lane = lax.broadcasted_iota(jnp.int32, first.shape, 1)
    if odd:
        first = pltpu.roll(first, HEAD, 1)
    else:
        second = pltpu.roll(second, HEAD, 1)
    return jnp.where(lane < HEAD, first, second)


def pick_qkv(weight, j, F, S, pairs):
    rows = weight.shape[0]
    per_shard = S // 2

    def kernel(j_ref, first, second, out):
        a, b = first[...].astype(F32), second[...].astype(F32)

        @pl.when(j_ref[0] % 2 == 0)
        def _():
            out[...] = half_lanes(a, b, 0).astype(BF)

        @pl.when(j_ref[0] % 2 == 1)
        def _():
            out[...] = half_lanes(a, b, 1).astype(BF)

    def column(which):
        return lambda i, j_ref: (
            0, (i % 3) * F * per_shard + (2 * (i // 3) + which) * per_shard + j_ref[0] // 2
        )

    return pl.pallas_call(
        kernel,
        grid_spec=pltpu.PrefetchScalarGridSpec(
            num_scalar_prefetch=1,
            grid=(3 * pairs,),
            in_specs=[pl.BlockSpec((rows, LANES), column(0)), pl.BlockSpec((rows, LANES), column(1))],
            out_specs=pl.BlockSpec((rows, LANES), lambda i, j_ref: (0, i)),
        ),
        out_shape=jax.ShapeDtypeStruct((rows, 3 * pairs * LANES), BF),
    )(j[None].astype(jnp.int32), weight, weight)


def unpack_qkv(gathered, rows, S, pairs):
    width = S * HEAD

    def kernel(src, out):
        for half in range(2):
            for z in range(S // 2):
                a, b = src[2 * z].astype(F32), src[2 * z + 1].astype(F32)
                out[:, half * width + z * LANES : half * width + (z + 1) * LANES] = half_lanes(
                    a, b, half
                )

    return pl.pallas_call(
        kernel,
        grid=(3 * pairs,),
        in_specs=[pl.BlockSpec((S, rows, LANES), lambda i: (0, 0, i))],
        out_specs=pl.BlockSpec((rows, 2 * width), lambda i: (0, (i % 3) * pairs + i // 3)),
        out_shape=jax.ShapeDtypeStruct((rows, HEADS * HEAD * 3), F32),
    )(gathered)


def unpack_cols(gathered, rows, F):
    S, _, cols = gathered.shape
    w = cols // F
    if w % LANES:
        split = gathered[:, :rows].reshape(S, rows, F, w)
        return split.transpose(1, 2, 0, 3).reshape(rows, F * S * w).astype(F32)

    def kernel(src, out):
        for s in range(S):
            out[:, s * w : (s + 1) * w] = src[s].astype(F32)

    return pl.pallas_call(
        kernel,
        grid=(F,),
        in_specs=[pl.BlockSpec((S, rows, w), lambda i: (0, 0, i))],
        out_specs=pl.BlockSpec((rows, S * w), lambda i: (0, i)),
        out_shape=jax.ShapeDtypeStruct((rows, F * S * w), F32),
    )(gathered)


def unpack_rows(gathered, rows):
    S, _, n = gathered.shape

    def kernel(src, out):
        out[...] = src[0].astype(F32)

    return pl.pallas_call(
        kernel,
        grid=(S,),
        in_specs=[pl.BlockSpec((1, rows, n), lambda i: (i, 0, 0))],
        out_specs=pl.BlockSpec((rows, n), lambda i: (i, 0)),
        out_shape=jax.ShapeDtypeStruct((S * rows, n), F32),
    )(gathered)


def body(
    tokens,
    ln_gain,
    ln_bias,
    qkv_weight,
    qkv_bias,
    dense_weight,
    dense_bias,
    fc1_weight,
    fc1_bias,
    fc2_weight,
    fc2_bias,
    segments,
    positions,
    cotangent,
):
    S, F = lax.axis_size("seq"), lax.axis_size("fsdp")
    j, f = lax.axis_index("seq"), lax.axis_index("fsdp")
    tok, D = tokens.shape[1], tokens.shape[2]
    length = tok * S
    rows_d = D // F
    ff = fc1_weight.shape[1]
    cols_up = ff // S
    block_up = cols_up // F
    hp = HEADS // S
    pairs = hp // 2
    per_shard = HEADS // F
    spread = per_shard % S == 0
    slots = per_shard // S if spread else 0

    qkv_width = pairs * 3 * LANES

    def heads_of(array, lead):
        shape = array.shape
        if spread:
            split = array.reshape(shape[:lead] + (F, S, slots) + shape[lead + 1 :])
            mine = lax.dynamic_index_in_dim(split, j, lead + 1, keepdims=False)
            return mine.reshape(shape[:lead] + (hp,) + shape[lead + 1 :])
        return lax.dynamic_slice_in_dim(array, j * hp, hp, lead)

    def qkv_cols(array):
        n = array.shape[0]
        mine = heads_of(array.reshape(n, 3, HEADS, HEAD), 2)
        return mine.reshape(n, 3, pairs, 2, HEAD).transpose(0, 2, 1, 3, 4).reshape(n, -1)

    def from_qkv_cols(gathered):
        n = gathered.shape[1]
        split = gathered.reshape(S, n, pairs, 3, 2, HEAD).transpose(0, 1, 3, 2, 4, 5)
        split = split.reshape(S, n, 3, hp, HEAD)
        if spread:
            moved = jnp.moveaxis(split.reshape(S, n, 3, F, slots, HEAD), 0, 3)
        else:
            moved = jnp.moveaxis(split, 0, 2)
        return moved.reshape(n, -1)

    small = jnp.concatenate([ln_gain, ln_bias, qkv_bias, dense_bias, fc1_bias, fc2_bias])
    small = lax.all_gather(small, "fsdp", axis=0)
    cuts, at = [], 0
    for piece in (ln_gain, ln_bias, qkv_bias, dense_bias, fc1_bias, fc2_bias):
        cuts.append(small[:, at : at + piece.shape[0]].reshape(-1).astype(F32))
        at += piece.shape[0]
    gain, shift, b_qkv, b_dense, b_up, b_down = cuts

    inputs = tokens[0].astype(F32)
    centre = jnp.mean(inputs, axis=-1, keepdims=True)
    variance = jnp.mean((inputs - centre) ** 2, axis=-1, keepdims=True)
    inv_std = lax.rsqrt(variance + EPS)
    standard = (inputs - centre) * inv_std
    normed_own = (standard * gain + shift).astype(BF)
    upstream_own = cotangent[0]

    up_own = lax.dynamic_index_in_dim(
        fc1_weight.reshape(rows_d, F, S, block_up), j, 2, keepdims=False
    ).reshape(rows_d, cols_up)
    down_own = lax.dynamic_slice_in_dim(fc2_weight, j * block_up, block_up, 0)
    if spread and slots == 1:
        qkv_own = pick_qkv(qkv_weight, j, F, S, pairs)
    else:
        qkv_own = qkv_cols(qkv_weight)
    w_up, w_down, normed, upstream = exchange(
        S, F, 1, shards=(up_own, down_own), tokens=(normed_own, upstream_own)
    )
    w_up, w_down = w_up.reshape(D, cols_up), w_down.reshape(cols_up, D)
    normed, upstream = normed.reshape(length, D), upstream.reshape(length, D)

    bias_up = lax.dynamic_index_in_dim(b_up.reshape(F, S, block_up), j, 1, keepdims=False)
    bias_up = bias_up.reshape(-1)
    bias_qkv = qkv_cols(b_qkv[None])[0]
    seg_row = segments[0]

    def rider(values, width):
        return jnp.pad(values[:, None], ((0, 0), (0, EXTRA - 1), (0, width - values.shape[1])))

    pre_act = dot(normed, w_up) + bias_up
    activated = gelu_tanh(pre_act).astype(BF)
    out_term = jnp.sum(upstream.astype(F32), axis=0).reshape(F, rows_d)
    (piece_down,) = exchange(S, F, 2, grads=((activated, upstream, rider(out_term, D)),))
    piece_down, qkv_own = lax.optimization_barrier((piece_down, qkv_own))
    out_mine = piece_down[block_up, :rows_d].astype(F32)
    all_down = lax.all_gather(piece_down, "seq", axis=0)

    grad_act = dot_nt(upstream, w_down)
    grad_pre = jax.vjp(gelu_tanh, pre_act)[1](grad_act)[0].astype(BF)
    up_term = jnp.sum(grad_pre.astype(F32), axis=0).reshape(F, block_up)
    block_dense = slots * HEAD
    shards = (qkv_own,)
    if spread:
        shards += (lax.dynamic_slice_in_dim(dense_weight, j * block_dense, block_dense, 0),)
    piece_up, w_qkv, *w_dense = exchange(
        S, F, 3, grads=((normed, grad_pre, rider(up_term, cols_up)),), shards=shards
    )
    all_up = lax.all_gather(piece_up, "seq", axis=0)
    w_qkv = w_qkv.reshape(D, qkv_width)
    if spread:
        w_dense = w_dense[0].reshape(hp * HEAD, D)
    else:
        w_dense = lax.dynamic_slice_in_dim(
            lax.all_gather(dense_weight, "fsdp", axis=0, tiled=True), j * hp * HEAD, hp * HEAD, 0
        )

    projected = dot(normed, w_qkv) + bias_qkv
    grad_att = dot_nt(upstream, w_dense).astype(BF)
    attended, grad_mixed = attention(projected, grad_att, angle_tables(seg_row), seg_row)
    qkv_term = jnp.sum(grad_mixed.astype(F32), axis=0)
    qkv_term = jnp.broadcast_to(qkv_term[None], (F, qkv_width))
    grads = ((normed, grad_mixed, rider(qkv_term, qkv_width)),)
    if spread:
        grads += ((attended, upstream, None),)
    (piece_qkv,) = exchange(S, F, 4, grads=grads, merge=qkv_width)
    all_qkv = lax.all_gather(piece_qkv, "seq", axis=0)

    partial_out = (dot(attended, w_dense) + dot(activated, w_down)).astype(BF)
    partial_normed = (dot_nt(grad_mixed, w_qkv) + dot_nt(grad_pre, w_up)).astype(BF)
    branches, grad_normed = seq_sum(
        S, F, 5, (partial_out.reshape(S, tok, D), partial_normed.reshape(S, tok, D))
    )
    result = (inputs + branches + (b_dense + b_down)).astype(BF)
    scaled = grad_normed * gain
    grad_inputs = upstream_own.astype(F32) + inv_std * (
        scaled
        - jnp.mean(scaled, axis=-1, keepdims=True)
        - standard * jnp.mean(scaled * standard, axis=-1, keepdims=True)
    )
    ln_terms = jnp.stack([jnp.sum(grad_normed * standard, axis=0), jnp.sum(grad_normed, axis=0)])
    ln_terms = lax.psum(ln_terms, ("seq", "fsdp"))
    ln_mine = lax.dynamic_slice_in_dim(ln_terms, f * rows_d, rows_d, 1)

    grad_down = unpack_rows(all_down, block_up)
    grad_up = unpack_cols(all_up, rows_d, F)
    up_mine = all_up[:, rows_d, :block_up].astype(F32).reshape(-1)
    qkv_sums = from_qkv_cols(all_qkv[:, rows_d][:, None]).reshape(F, -1)
    qkv_mine = lax.dynamic_index_in_dim(qkv_sums, f, 0, keepdims=False).astype(F32)
    if spread and slots == 1:
        grad_qkv = unpack_qkv(all_qkv, rows_d, S, pairs)
    else:
        grad_qkv = from_qkv_cols(all_qkv[:, :rows_d]).astype(F32)
    if spread:
        chunks, at = [], rows_d + EXTRA
        for col in range(0, D, qkv_width):
            n = min(qkv_width, D - col)
            chunks.append(all_qkv[:, at : at + block_dense, :n])
            at += block_dense
        grad_dense = jnp.concatenate(chunks, axis=2).astype(F32).reshape(rows_d, D)
    else:
        part = lax.all_gather(dot_tn(attended, upstream).astype(BF), "seq", axis=0, tiled=True)
        grad_dense = lax.psum_scatter(part, "fsdp", scatter_dimension=0, tiled=True).astype(F32)
    return (
        result[None],
        grad_inputs[None],
        ln_mine[0],
        ln_mine[1],
        grad_qkv,
        qkv_mine,
        grad_dense,
        out_mine,
        grad_up,
        up_mine,
        grad_down,
        out_mine,
    )


def solution(mesh):
    row, mat = P("fsdp"), P("fsdp", None)
    act = P("fsdp", "seq", None)
    return jax.shard_map(
        body,
        mesh=mesh,
        in_specs=(
            act, row, row, mat, row, mat, row, mat, row, mat, row, mat, P("fsdp", "seq"), act,
        ),
        out_specs=(act, act, row, row, mat, row, mat, row, mat, row, mat, row),
        check_vma=False,
    )
```

```python
import functools

import jax
import jax.numpy as jnp
from jax import lax
from jax.experimental import pallas as pl
from jax.experimental.pallas import tpu as pltpu
from jax.sharding import PartitionSpec as P


HEADS = 32
HEAD = 64
ROT = 32
EPS = 1e-05
DOC_SHIFT = 1023
LANES = 2 * HEAD
BF = jnp.bfloat16
F32 = jnp.float32


def dot(left, right):
    return lax.dot_general(left, right, (((1,), (0,)), ((), ())), preferred_element_type=F32)


def dot_nt(left, right):
    return lax.dot_general(left, right, (((1,), (1,)), ((), ())), preferred_element_type=F32)


def dot_tn(left, right):
    return lax.dot_general(left, right, (((0,), (0,)), ((), ())), preferred_element_type=F32)


def gelu_tanh(values_in):
    return jax.nn.gelu(values_in, approximate=True)


def turn(values, cos, sin_low, sin_high):
    half = ROT // 2
    return (
        values * cos
        - pltpu.roll(values, LANES - half, 1) * sin_low
        + pltpu.roll(values, half, 1) * sin_high
    )


def attention_kernel(
    rows, proj, grad_out, cos, sin_low, sin_high, seg_col, seg_row,
    out, grad_proj, qs, ks, vs, dk, dv,
):
    length = proj.shape[0]
    blocks = length // rows
    scale = HEAD**-0.5
    for i in range(blocks):
        r = slice(i * rows, (i + 1) * rows)
        c, lo, hi = cos[r, :], sin_low[r, :], sin_high[r, :]
        qs[r, :] = turn(proj[r, 0:LANES], c, lo, hi).astype(BF) * jnp.asarray(scale, BF)
        ks[r, :] = turn(proj[r, LANES : 2 * LANES], c, lo, hi).astype(BF)
        vs[r, :] = proj[r, 2 * LANES : 3 * LANES].astype(BF)
    lane = lax.broadcasted_iota(jnp.int32, (rows, LANES), 1)
    first = lane < HEAD
    zero = jnp.zeros((rows, LANES), BF)
    for i in reversed(range(blocks)):
        r = slice(i * rows, (i + 1) * rows)
        n = (i + 1) * rows
        place_q = i * rows + lax.broadcasted_iota(jnp.int32, (rows, n), 0)
        place_k = lax.broadcasted_iota(jnp.int32, (rows, n), 1)
        allowed = (place_k <= place_q) & (seg_col[r, :] == seg_row[:, 0:n])
        q2, g2 = qs[r, :], grad_out[r, :]
        k, v = ks[0:n, :], vs[0:n, :]
        o_parts, dq_parts = [], []
        for h in range(2):
            mine = first if h == 0 else ~first
            q = jnp.where(mine, q2, zero)
            g = jnp.where(mine, g2, zero)
            s = jnp.where(allowed, dot_nt(q, k), -1e30)
            e = jnp.exp(s - jnp.max(s, axis=-1, keepdims=True))
            p = e * (1.0 / jnp.sum(e, axis=-1, keepdims=True))
            pb = p.astype(BF)
            o_parts.append(dot(pb, v))
            dp = dot_nt(g, v)
            inner = jnp.sum(p * dp, axis=-1, keepdims=True)
            ds = (p * (dp - inner)).astype(BF)
            dq_parts.append(dot(ds, k))
            dk_new, dv_new = dot_tn(ds, q), dot_tn(pb, g)
            if i == blocks - 1 and h == 0:
                dk[...] = dk_new
                dv[...] = dv_new
            else:
                dk[0:n, :] += dk_new
                dv[0:n, :] += dv_new
        out[r, :] = jnp.where(first, o_parts[0], o_parts[1]).astype(BF)
        dq = (jnp.where(first, dq_parts[0], dq_parts[1]) * scale).astype(BF).astype(F32)
        c, lo, hi = cos[r, :], sin_low[r, :], sin_high[r, :]
        grad_proj[r, 0:LANES] = turn(dq, c, -lo, -hi).astype(BF)
    for i in range(blocks):
        r = slice(i * rows, (i + 1) * rows)
        c, lo, hi = cos[r, :], sin_low[r, :], sin_high[r, :]
        grad_k = dk[r, :].astype(BF).astype(F32)
        grad_proj[r, LANES : 2 * LANES] = turn(grad_k, c, -lo, -hi).astype(BF)
        grad_proj[r, 2 * LANES : 3 * LANES] = dv[r, :].astype(BF)


def attention(proj, grad_att, tables, segments):
    length = proj.shape[0]
    pairs = grad_att.shape[1] // LANES
    rows = 256
    whole = lambda shape: pl.BlockSpec(shape, lambda p: (0, 0))
    return pl.pallas_call(
        functools.partial(attention_kernel, rows),
        grid=(pairs,),
        out_shape=(
            jax.ShapeDtypeStruct((length, pairs * LANES), BF),
            jax.ShapeDtypeStruct((length, 3 * pairs * LANES), BF),
        ),
        in_specs=[
            pl.BlockSpec((length, 3 * LANES), lambda p: (0, p)),
            pl.BlockSpec((length, LANES), lambda p: (0, p)),
            whole((length, LANES)),
            whole((length, LANES)),
            whole((length, LANES)),
            whole((length, 1)),
            whole((1, length)),
        ],
        out_specs=(
            pl.BlockSpec((length, LANES), lambda p: (0, p)),
            pl.BlockSpec((length, 3 * LANES), lambda p: (0, p)),
        ),
        scratch_shapes=[pltpu.VMEM((length, LANES), BF)] * 3
        + [pltpu.VMEM((length, LANES), F32)] * 2,
        cost_estimate=pl.CostEstimate(
            flops=14 * pairs * length * length * LANES,
            bytes_accessed=pairs * length * LANES * 24,
            transcendentals=pairs * length * length,
        ),
    )(proj, grad_att, *tables, segments[:, None], segments[None, :])


def angle_tables(seg_row):
    length = seg_row.shape[0]
    position = jnp.arange(length, dtype=jnp.int32) + jnp.where(seg_row > 0, DOC_SHIFT, 0)
    half = ROT // 2
    inverse = 1.0 / 10000.0 ** (jnp.arange(0, ROT, 2, dtype=F32) / ROT)
    angles = position.astype(F32)[:, None] * inverse[None, :]
    cosine, sine = jnp.cos(angles), jnp.sin(angles)
    ones = jnp.ones((length, HEAD - ROT), F32)
    zeros = jnp.zeros((length, HEAD - ROT), F32)
    none = jnp.zeros((length, half), F32)
    cos = jnp.concatenate([cosine, cosine, ones] * 2, axis=1)
    low = jnp.concatenate([sine, none, zeros] * 2, axis=1)
    high = jnp.concatenate([none, sine, zeros] * 2, axis=1)
    return cos, low, high


MESH = pl.DeviceIdType.MESH


def remote(src, dst, send, recv, device):
    return pltpu.make_async_remote_copy(
        src_ref=src, dst_ref=dst, send_sem=send, recv_sem=recv, device_id=device,
        device_id_type=MESH,
    )


class Place:
    def __init__(self, S, F):
        self.S, self.F, self.Q = S, F, S // 2
        self.j, self.f = lax.axis_index("seq"), lax.axis_index("fsdp")
        self.q, self.c = self.j // 2, lax.rem(self.j, 2)
        self.partner = 2 * self.q + 1 - self.c

    def greet(self, over_fsdp, over_seq):
        barrier = pltpu.get_barrier_semaphore()

        def signal(j, f):
            pl.semaphore_signal(barrier, inc=1, device_id=(j, f), device_id_type=MESH)

        count = 0
        if over_fsdp:
            for k in range(1, self.F):
                signal(self.j, lax.rem(self.f + k, self.F))
            count += self.F - 1
        if over_seq == "all":
            for k in range(1, self.S):
                signal(lax.rem(self.j + k, self.S), self.f)
            count += self.S - 1
        elif over_seq == "line":
            signal(self.partner, self.f)

            @pl.when(self.q > 0)
            def _():
                signal(self.j - 2, self.f)

            @pl.when(self.q < self.Q - 1)
            def _():
                signal(self.j + 2, self.f)

            count += 1 + (self.q + self.Q - 1) // self.Q + (2 * self.Q - 2 - self.q) // self.Q
        pl.semaphore_wait(barrier, count)


class ShardGather:
    @staticmethod
    def scratch(F):
        n = 6 if F == 4 else F - 1
        return [pltpu.SemaphoreType.DMA((n,)), pltpu.SemaphoreType.DMA((n,)),
                pltpu.SemaphoreType.DMA]

    def __init__(self, at, src, dst, send, recv, local):
        self.at, self.src, self.dst = at, src, dst
        f, j = at.f, at.j
        self.own = pltpu.make_async_copy(src, dst.at[f], local)
        self.first, self.later, self.arrivals = [], [], []
        if at.F == 4:
            nx = f + 1 - 2 * lax.rem(f, 2)
            ny = lax.rem(f + 2, 4)
            nd = lax.rem(nx + 2, 4)
            half = src.shape[0] // 2
            a, b = pl.ds(0, half), pl.ds(half, half)
            table = ((nx, a), (nx, b), (ny, a), (ny, b))
            for i, (to, rows) in enumerate(table):
                self.first.append(
                    remote(src.at[rows], dst.at[f, rows], send.at[i], recv.at[i], (j, to))
                )
                self.arrivals.append(
                    remote(src.at[rows], dst.at[to, rows], send.at[i], recv.at[i], (j, to))
                )
            for i, (of, rows, to) in ((4, (nx, a, ny)), (5, (ny, b, nx))):
                self.later.append(
                    remote(dst.at[of, rows], dst.at[of, rows], send.at[i], recv.at[i], (j, to))
                )
                self.arrivals.append(
                    remote(dst.at[nd, rows], dst.at[nd, rows], send.at[i], recv.at[i], (j, to))
                )
        else:
            for k in range(1, at.F):
                to, of = lax.rem(f + k, at.F), lax.rem(f + at.F - k, at.F)
                self.first.append(
                    remote(src, dst.at[f], send.at[k - 1], recv.at[k - 1], (j, to))
                )
                self.arrivals.append(
                    remote(src, dst.at[of], send.at[k - 1], recv.at[k - 1], (j, to))
                )

    def start(self):
        self.own.start()
        for copy in self.first:
            copy.start()

    def relay(self):
        if self.later:
            self.arrivals[0].wait_recv()
            self.later[0].start()
            self.arrivals[3].wait_recv()
            self.later[1].start()

    def finish(self):
        for i, copy in enumerate(self.arrivals):
            if not (self.later and i in (0, 3)):
                copy.wait_recv()
        for copy in self.first + self.later:
            copy.wait_send()
        self.own.wait()


class TokenGather:
    @staticmethod
    def scratch(S):
        Q = S // 2
        return [pltpu.SemaphoreType.DMA((2 * Q,)), pltpu.SemaphoreType.DMA((2 * Q,)),
                pltpu.SemaphoreType.DMA((S,)), pltpu.SemaphoreType.DMA]

    def __init__(self, at, src, dst, send, share, recv, local):
        self.at, self.src, self.dst = at, src, dst
        self.send, self.share, self.recv = send, share, recv
        self.own = pltpu.make_async_copy(src, dst.at[at.j], local)

    def onward(self, slot, source, i, by):
        to = self.dst.at[slot]
        return remote(
            source, to, self.send.at[i], self.recv.at[slot], (self.at.j + by, self.at.f)
        )

    def given(self, slot, source, i):
        to = self.dst.at[slot]
        return remote(
            source, to, self.share.at[i], self.recv.at[slot], (self.at.partner, self.at.f)
        )

    def plan(self, d):
        at, Q = self.at, self.at.Q
        below, above = at.j - 2 * d, at.j + 2 * d
        dst = self.dst
        return (
            (at.q >= d, self.onward(below, dst.at[below], d, 2), at.q < Q - 1,
             self.given(below, dst.at[below], d)),
            (at.q + d <= Q - 1, self.onward(above, dst.at[above], Q + d, -2), at.q > 0,
             self.given(above, dst.at[above], Q + d)),
        )

    def ends(self):
        j, Q = self.at.j, self.at.Q
        return (
            self.onward(j, self.src, 0, 2), self.onward(j, self.src, Q, -2),
            self.given(j, self.src, 0),
        )

    def start(self):
        at, Q = self.at, self.at.Q
        self.own.start()
        up, down, part = self.ends()

        @pl.when(at.q < Q - 1)
        def _():
            up.start()

        @pl.when(at.q > 0)
        def _():
            down.start()

        part.start()

    def step(self, d):
        for valid, onward, go, part in self.plan(d):

            @pl.when(valid)
            def _():
                onward.wait_recv()

                @pl.when(go)
                def _():
                    onward.start()

                part.start()

    def finish(self):
        at, Q = self.at, self.at.Q
        for q in range(Q):
            slot = 2 * q + 1 - at.c
            self.given(slot, self.dst.at[slot], 0).wait_recv()
        up, down, part = self.ends()

        @pl.when(at.q < Q - 1)
        def _():
            up.wait_send()

        @pl.when(at.q > 0)
        def _():
            down.wait_send()

        part.wait_send()
        for d in range(1, Q):
            for valid, onward, go, part in self.plan(d):

                @pl.when(valid & go)
                def _():
                    onward.wait_send()

                @pl.when(valid)
                def _():
                    part.wait_send()

        self.own.wait()


class GradReduce:
    @staticmethod
    def scratch(F, rows, n):
        return [pltpu.VMEM((F, rows, n), BF), pltpu.VMEM((F - 1, rows, n), BF),
                pltpu.SemaphoreType.DMA((F - 1,)), pltpu.SemaphoreType.DMA((F - 1,))]

    def __init__(self, at, left, right, extra, made, got, send, recv):
        self.at, self.left, self.right, self.extra = at, left, right, extra
        self.made, self.got, self.send, self.recv = made, got, send, recv
        self.n = right.shape[1]
        self.rows = left.shape[1] // at.F
        self.tile = 512 if self.n % 512 == 0 else 256 if self.n % 256 == 0 else 128

    def copy(self, k):
        at = self.at
        to = lax.rem(at.f + k, at.F)
        return remote(
            self.made.at[to], self.got.at[k - 1], self.send.at[k - 1], self.recv.at[k - 1],
            (at.j, to),
        )

    def start(self):
        at, rows = self.at, self.rows
        aligned = rows % 128 == 0
        for t in range(0, self.n, self.tile) if not aligned else ():
            cols = slice(t, t + self.tile)
            full = dot_tn(self.left[...], self.right[:, cols]).astype(BF)
            for p in range(at.F):
                self.made[p, 0:rows, cols] = full[p * rows : (p + 1) * rows, :]
        for k in list(range(1, at.F)) + [0]:
            p = lax.rem(at.f + k, at.F)
            if aligned:
                block = self.left[:, pl.ds(pl.multiple_of(p * rows, 128), rows)]
                for t in range(0, self.n, self.tile):
                    cols = slice(t, t + self.tile)
                    self.made[p, 0:rows, cols] = dot_tn(block, self.right[:, cols]).astype(BF)
            if self.extra is not None:
                self.made[p, rows : rows + self.extra.shape[1], :] = self.extra[p].astype(BF)
            if k:
                self.copy(k).start()

    def finish(self, store):
        at = self.at
        for k in range(1, at.F):
            self.copy(k).wait_recv()
        for t in range(0, self.n, self.tile):
            cols = slice(t, t + self.tile)
            total = self.made[at.f, :, cols].astype(F32)
            for k in range(1, at.F):
                total += self.got[k - 1, :, cols].astype(F32)
            store(t, self.tile, total.astype(BF))
        for k in range(1, at.F):
            self.copy(k).wait_send()


EXTRA = 16


def exchange(S, F, collective_id, grads=(), shards=(), tokens=(), merge=None, split=False):
    operands, in_specs = [], []
    vmem = pl.BlockSpec(memory_space=pltpu.VMEM)
    outs, out_specs, scratch = [], [], []
    shapes, row = [], 0
    for left, right, extra in grads:
        rows, n = left.shape[1] // F + (0 if extra is None else EXTRA), right.shape[1]
        operands += [left, right] + ([] if extra is None else [extra])
        scratch += GradReduce.scratch(F, rows, n)
        shapes.append((rows, n, row))
        row += rows * pl.cdiv(n, merge or n)
        if split:
            outs.append(jax.ShapeDtypeStruct((rows - EXTRA, n), BF))
            outs.append(jax.ShapeDtypeStruct((EXTRA, n), BF))
        elif not merge:
            outs.append(jax.ShapeDtypeStruct((rows, n), BF))
    if merge:
        outs.append(jax.ShapeDtypeStruct((row, merge), BF))
    out_specs += [vmem] * len(outs)
    for array in shards:
        operands.append(array)
        outs.append(jax.ShapeDtypeStruct((F,) + array.shape, BF))
        out_specs.append(pl.BlockSpec(memory_space=pl.ANY))
        scratch += ShardGather.scratch(F)
    for array in tokens:
        operands.append(array)
        outs.append(jax.ShapeDtypeStruct((S,) + array.shape, BF))
        out_specs.append(pl.BlockSpec(memory_space=pl.ANY))
        scratch += TokenGather.scratch(S)
    in_specs = [vmem] * len(operands)
    n_in, n_out = len(operands), len(outs)

    def kernel(*refs):
        ins, results, rest = list(refs[:n_in]), list(refs[n_in : n_in + n_out]), list(
            refs[n_in + n_out :]
        )
        take = lambda items, n: [items.pop(0) for _ in range(n)]
        at = Place(S, F)
        jobs, stores = [], []
        packed = take(results, 1)[0] if merge else None
        for (_, _, extra), (rows, n, row0) in zip(grads, shapes):
            left, right = take(ins, 2)
            extra_ref = None if extra is None else take(ins, 1)[0]
            jobs.append(GradReduce(at, left, right, extra_ref, *take(rest, 4)))
            target = packed if merge else take(results, 1)[0]
            rider_ref = take(results, 1)[0] if split else None

            def store(t, width, value, target=target, rows=rows, row0=row0, rider_ref=rider_ref):
                if split:
                    target[:, t : t + width] = value[: rows - EXTRA]
                    rider_ref[:, t : t + width] = value[rows - EXTRA :]
                    return
                if not merge:
                    target[:, t : t + width] = value
                    return
                while width:
                    chunk, col = divmod(t, merge)
                    part = min(width, merge - col)
                    target[row0 + chunk * rows : row0 + (chunk + 1) * rows, col : col + part] = (
                        value[:, :part]
                    )
                    value, t, width = value[:, part:], t + part, width - part

            stores.append(store)
        spreads = [
            ShardGather(at, take(ins, 1)[0], take(results, 1)[0], *take(rest, 3)) for _ in shards
        ]
        lines = [
            TokenGather(at, take(ins, 1)[0], take(results, 1)[0], *take(rest, 4)) for _ in tokens
        ]
        at.greet(bool(jobs or spreads), "line" if lines else "")
        for item in lines + spreads:
            item.start()
        for job in jobs:
            job.start()
        waiting = list(spreads)
        for d in range(1, at.Q) if lines else ():
            for item in lines:
                item.step(d)
            if waiting:
                waiting.pop(0).relay()
        for item in waiting:
            item.relay()
        for job, store in zip(jobs, stores):
            job.finish(store)
        for item in spreads + lines:
            item.finish()

    flops = sum(2 * l.shape[0] * l.shape[1] * r.shape[1] for l, r, _ in grads)
    moved = sum(o.size * 2 for o in outs)
    return pl.pallas_call(
        kernel,
        out_shape=tuple(outs),
        in_specs=in_specs,
        out_specs=tuple(out_specs),
        scratch_shapes=scratch,
        compiler_params=pltpu.CompilerParams(
            collective_id=collective_id, has_side_effects=True
        ),
        cost_estimate=pl.CostEstimate(
            flops=flops, bytes_accessed=20 * moved, transcendentals=0
        ),
    )(*operands)


LN_ROWS = 8


def token_sums(S, F, collective_id, out_part, normed_part, standard, pieces):
    Q = S // 2
    t, d = out_part.shape[1:]
    w = d // F
    m = len(pieces)
    n_in = 3 + m

    def kernel(*refs):
        at = Place(S, F)
        ins, results, rest = refs[:n_in], refs[n_in : n_in + 3 + m], list(refs[n_in + 3 + m :])
        take = lambda n: [rest.pop(0) for _ in range(n)]
        jobs = [(ins[i], results[i]) + tuple(take(7)) for i in range(2)]
        lines = [TokenGather(at, ins[3 + i], results[3 + i], *take(4)) for i in range(m)]
        made, by_shard, by_seq, s_f, r_f, s_s, r_s = take(7)
        j, f, q = at.j, at.f, at.q
        low = 1 - q // (Q // 2)
        at.greet(True, "all")

        def share(job, slot):
            part, _, pair, _, _, _, _, s_pair, r_pair = job
            return remote(
                part.at[2 * slot + 1 - at.c], pair.at[slot], s_pair.at[slot], r_pair.at[slot],
                (at.partner, f),
            )

        def hop(job, slot, up):
            _, _, _, buf, got, s_line, r_line, _, _ = job
            i = slot + (1 - up) * Q
            return remote(
                buf.at[slot], got.at[i], s_line.at[i], r_line.at[i], (j + 4 * up - 2, f)
            )

        order = []
        for i in range(Q):
            for slot in (Q - 1 - i, i):
                if slot not in order:
                    order.append(slot)
        for slot in order:
            for job in jobs:
                share(job, slot).start()
        for line in lines:
            line.start()

        def base(job, slot):
            share(job, slot).wait_recv()
            return job[0][2 * slot + at.c].astype(F32) + job[2][slot].astype(F32)

        def pass_on(job, slot, up, inner):
            copy = hop(job, slot, up)
            i = slot + (1 - up) * Q

            @pl.when((2 * up - 1) * (slot - q) > 0)
            def _():
                value = base(job, slot)
                if inner is None:
                    copy.wait_recv()
                    job[3][slot] = (value + job[4][i].astype(F32)).astype(BF)
                else:
                    job[3][slot] = value.astype(BF)

                    @pl.when(inner)
                    def _():
                        copy.wait_recv()
                        job[3][slot] = (value + job[4][i].astype(F32)).astype(BF)

                copy.start()

        near = low * q + (1 - low) * (Q - 1 - q)
        for i in range(Q - 1):
            for job in jobs:
                pass_on(job, low * (Q - 1 - i) + (1 - low) * i, low, near > 0)
            for job in jobs:
                pass_on(job, (1 - low) * (Q - 1 - i) + low * i, 1 - low, None)
            for line in lines:
                line.step(i + 1)

        for job in jobs:
            job[1][...] = base(job, q)

            @pl.when(q > 0)
            def _():
                hop(job, q, 1).wait_recv()
                job[1][...] += job[4][q].astype(F32)

            @pl.when(q < Q - 1)
            def _():
                hop(job, q, 0).wait_recv()
                job[1][...] += job[4][Q + q].astype(F32)

        grad_normed = jobs[1][1][...]
        gain_row = jnp.sum(grad_normed * ins[2][...], axis=0, keepdims=True)
        bias_row = jnp.sum(grad_normed, axis=0, keepdims=True)
        both = jnp.concatenate(
            [gain_row, bias_row, jnp.zeros((LN_ROWS - 2, d), F32)], axis=0
        )
        for p in range(F):
            made[p] = both[:, p * w : (p + 1) * w]
        over_f = []
        for k in range(1, F):
            to, of = lax.rem(f + k, F), lax.rem(f + F - k, F)
            over_f.append(
                (remote(made.at[to], by_shard.at[f], s_f.at[k - 1], r_f.at[f], (j, to)),
                 remote(made.at[to], by_shard.at[of], s_f.at[k - 1], r_f.at[of], (j, to)))
            )
        for copy, _ in over_f:
            copy.start()
        by_shard[f] = made[f]
        for _, arrival in over_f:
            arrival.wait_recv()
        total = by_shard[0]
        for p in range(1, F):
            total += by_shard[p]
        by_seq[j] = total
        over_s = []
        for k in range(1, S):
            to, of = lax.rem(j + k, S), lax.rem(j + S - k, S)
            over_s.append(
                (remote(by_seq.at[j], by_seq.at[j], s_s.at[k - 1], r_s.at[j], (to, f)),
                 remote(by_seq.at[j], by_seq.at[of], s_s.at[k - 1], r_s.at[of], (to, f)))
            )
        for copy, _ in over_s:
            copy.start()
        for _, arrival in over_s:
            arrival.wait_recv()
        total = by_seq[0]
        for p in range(1, S):
            total += by_seq[p]
        results[2][...] = total
        for copy, _ in over_f + over_s:
            copy.wait_send()
        for job in jobs:
            for slot in range(Q):
                share(job, slot).wait_send()

                @pl.when(q < slot)
                def _():
                    hop(job, slot, 1).wait_send()

                @pl.when(q > slot)
                def _():
                    hop(job, slot, 0).wait_send()

        for line in lines:
            line.finish()

    vmem = pl.BlockSpec(memory_space=pltpu.VMEM)
    scratch = [
        pltpu.VMEM((Q, t, d), BF),
        pltpu.VMEM((Q, t, d), BF),
        pltpu.VMEM((2 * Q, t, d), BF),
        pltpu.SemaphoreType.DMA((2 * Q,)),
        pltpu.SemaphoreType.DMA((2 * Q,)),
        pltpu.SemaphoreType.DMA((Q,)),
        pltpu.SemaphoreType.DMA((Q,)),
    ] * 2
    for _ in pieces:
        scratch += TokenGather.scratch(S)
    scratch += [
        pltpu.VMEM((F, LN_ROWS, w), F32),
        pltpu.VMEM((F, LN_ROWS, w), F32),
        pltpu.VMEM((S, LN_ROWS, w), F32),
        pltpu.SemaphoreType.DMA((F - 1,)),
        pltpu.SemaphoreType.DMA((F,)),
        pltpu.SemaphoreType.DMA((S - 1,)),
        pltpu.SemaphoreType.DMA((S,)),
    ]
    full = jax.ShapeDtypeStruct((t, d), F32)
    return pl.pallas_call(
        kernel,
        out_shape=(full, full, jax.ShapeDtypeStruct((LN_ROWS, w), F32))
        + tuple(jax.ShapeDtypeStruct((S,) + p.shape, BF) for p in pieces),
        in_specs=[vmem] * n_in,
        out_specs=(vmem,) * 3 + (pl.BlockSpec(memory_space=pl.ANY),) * m,
        scratch_shapes=scratch,
        compiler_params=pltpu.CompilerParams(
            collective_id=collective_id, has_side_effects=True
        ),
        cost_estimate=pl.CostEstimate(
            flops=2 * S * t * d, bytes_accessed=80 * S * t * d, transcendentals=0
        ),
    )(out_part, normed_part, standard, *pieces)


def half_lanes(first, second, odd):
    lane = lax.broadcasted_iota(jnp.int32, first.shape, 1)
    if odd:
        first = pltpu.roll(first, HEAD, 1)
    else:
        second = pltpu.roll(second, HEAD, 1)
    return jnp.where(lane < HEAD, first, second)


def pick_qkv(weight, j, F, S, pairs):
    rows = weight.shape[0]
    per_shard = S // 2

    def kernel(j_ref, first, second, out):
        a, b = first[...].astype(F32), second[...].astype(F32)

        @pl.when(j_ref[0] % 2 == 0)
        def _():
            out[...] = half_lanes(a, b, 0).astype(BF)

        @pl.when(j_ref[0] % 2 == 1)
        def _():
            out[...] = half_lanes(a, b, 1).astype(BF)

    def column(which):
        return lambda i, j_ref: (
            0, (i % 3) * F * per_shard + (2 * (i // 3) + which) * per_shard + j_ref[0] // 2
        )

    return pl.pallas_call(
        kernel,
        grid_spec=pltpu.PrefetchScalarGridSpec(
            num_scalar_prefetch=1,
            grid=(3 * pairs,),
            in_specs=[pl.BlockSpec((rows, LANES), column(0)), pl.BlockSpec((rows, LANES), column(1))],
            out_specs=pl.BlockSpec((rows, LANES), lambda i, j_ref: (0, i)),
        ),
        out_shape=jax.ShapeDtypeStruct((rows, 3 * pairs * LANES), BF),
    )(j[None].astype(jnp.int32), weight, weight)


def pick_up(weight, j, F, S):
    rows, ff = weight.shape
    w = ff // (F * S)
    if w % LANES:
        split = weight.reshape(rows, F, S, w)
        return lax.dynamic_index_in_dim(split, j, 2, keepdims=False).reshape(rows, F * w)

    def kernel(j_ref, src, out):
        out[...] = src[...]

    return pl.pallas_call(
        kernel,
        grid_spec=pltpu.PrefetchScalarGridSpec(
            num_scalar_prefetch=1,
            grid=(F,),
            in_specs=[pl.BlockSpec((rows, w), lambda i, j_ref: (0, i * S + j_ref[0]))],
            out_specs=pl.BlockSpec((rows, w), lambda i, j_ref: (0, i)),
        ),
        out_shape=jax.ShapeDtypeStruct((rows, F * w), BF),
    )(j[None].astype(jnp.int32), weight)


def unpack_qkv(gathered, rows, S, pairs):
    width = S * HEAD

    def kernel(src, out):
        for half in range(2):
            for z in range(S // 2):
                a, b = src[2 * z].astype(F32), src[2 * z + 1].astype(F32)
                out[:, half * width + z * LANES : half * width + (z + 1) * LANES] = half_lanes(
                    a, b, half
                )

    return pl.pallas_call(
        kernel,
        grid=(3 * pairs,),
        in_specs=[pl.BlockSpec((S, rows, LANES), lambda i: (0, 0, i))],
        out_specs=pl.BlockSpec((rows, 2 * width), lambda i: (0, (i % 3) * pairs + i // 3)),
        out_shape=jax.ShapeDtypeStruct((rows, HEADS * HEAD * 3), F32),
    )(gathered)


def unpack_cols(gathered, rows, F):
    S, _, cols = gathered.shape
    w = cols // F
    if w % LANES:
        split = gathered[:, :rows].reshape(S, rows, F, w)
        return split.transpose(1, 2, 0, 3).reshape(rows, F * S * w).astype(F32)

    def kernel(src, out):
        for s in range(S):
            out[:, s * w : (s + 1) * w] = src[s].astype(F32)

    return pl.pallas_call(
        kernel,
        grid=(F,),
        in_specs=[pl.BlockSpec((S, rows, w), lambda i: (0, 0, i))],
        out_specs=pl.BlockSpec((rows, S * w), lambda i: (0, i)),
        out_shape=jax.ShapeDtypeStruct((rows, F * S * w), F32),
    )(gathered)


def unpack_rows(gathered, rows):
    S, _, n = gathered.shape

    def kernel(src, out):
        out[...] = src[0].astype(F32)

    return pl.pallas_call(
        kernel,
        grid=(S,),
        in_specs=[pl.BlockSpec((1, rows, n), lambda i: (i, 0, 0))],
        out_specs=pl.BlockSpec((rows, n), lambda i: (i, 0)),
        out_shape=jax.ShapeDtypeStruct((S * rows, n), F32),
    )(gathered)


def body(
    tokens,
    ln_gain,
    ln_bias,
    qkv_weight,
    qkv_bias,
    dense_weight,
    dense_bias,
    fc1_weight,
    fc1_bias,
    fc2_weight,
    fc2_bias,
    segments,
    positions,
    cotangent,
):
    S, F = lax.axis_size("seq"), lax.axis_size("fsdp")
    j, f = lax.axis_index("seq"), lax.axis_index("fsdp")
    tok, D = tokens.shape[1], tokens.shape[2]
    length = tok * S
    rows_d = D // F
    ff = fc1_weight.shape[1]
    cols_up = ff // S
    block_up = cols_up // F
    hp = HEADS // S
    pairs = hp // 2
    per_shard = HEADS // F
    spread = per_shard % S == 0
    slots = per_shard // S if spread else 0

    qkv_width = pairs * 3 * LANES

    def heads_of(array, lead):
        shape = array.shape
        if spread:
            split = array.reshape(shape[:lead] + (F, S, slots) + shape[lead + 1 :])
            mine = lax.dynamic_index_in_dim(split, j, lead + 1, keepdims=False)
            return mine.reshape(shape[:lead] + (hp,) + shape[lead + 1 :])
        return lax.dynamic_slice_in_dim(array, j * hp, hp, lead)

    def qkv_cols(array):
        n = array.shape[0]
        mine = heads_of(array.reshape(n, 3, HEADS, HEAD), 2)
        return mine.reshape(n, 3, pairs, 2, HEAD).transpose(0, 2, 1, 3, 4).reshape(n, -1)

    def from_qkv_cols(gathered):
        n = gathered.shape[1]
        split = gathered.reshape(S, n, pairs, 3, 2, HEAD).transpose(0, 1, 3, 2, 4, 5)
        split = split.reshape(S, n, 3, hp, HEAD)
        if spread:
            moved = jnp.moveaxis(split.reshape(S, n, 3, F, slots, HEAD), 0, 3)
        else:
            moved = jnp.moveaxis(split, 0, 2)
        return moved.reshape(n, -1)

    small = jnp.concatenate([ln_gain, ln_bias, qkv_bias, dense_bias, fc1_bias, fc2_bias])
    small = lax.all_gather(small, "fsdp", axis=0)
    cuts, at = [], 0
    for piece in (ln_gain, ln_bias, qkv_bias, dense_bias, fc1_bias, fc2_bias):
        cuts.append(small[:, at : at + piece.shape[0]].reshape(-1).astype(F32))
        at += piece.shape[0]
    gain, shift, b_qkv, b_dense, b_up, b_down = cuts

    inputs = tokens[0].astype(F32)
    centre = jnp.mean(inputs, axis=-1, keepdims=True)
    variance = jnp.mean((inputs - centre) ** 2, axis=-1, keepdims=True)
    inv_std = lax.rsqrt(variance + EPS)
    standard = (inputs - centre) * inv_std
    normed_own = (standard * gain + shift).astype(BF)
    upstream_own = cotangent[0]

    up_own = pick_up(fc1_weight, j, F, S)
    down_own = lax.dynamic_slice_in_dim(fc2_weight, j * block_up, block_up, 0)
    if spread and slots == 1:
        qkv_own = pick_qkv(qkv_weight, j, F, S, pairs)
    else:
        qkv_own = qkv_cols(qkv_weight)
    w_up, w_down, normed, upstream = exchange(
        S, F, 1, shards=(up_own, down_own), tokens=(normed_own, upstream_own)
    )
    w_up, w_down = w_up.reshape(D, cols_up), w_down.reshape(cols_up, D)
    normed, upstream = normed.reshape(length, D), upstream.reshape(length, D)

    bias_up = lax.dynamic_index_in_dim(b_up.reshape(F, S, block_up), j, 1, keepdims=False)
    bias_up = bias_up.reshape(-1)
    bias_qkv = qkv_cols(b_qkv[None])[0]
    seg_row = segments[0]

    def rider(values, width):
        return jnp.pad(values[:, None], ((0, 0), (0, EXTRA - 1), (0, width - values.shape[1])))

    pre_act = dot(normed, w_up) + bias_up
    activated = gelu_tanh(pre_act).astype(BF)
    out_term = jnp.sum(upstream.astype(F32), axis=0).reshape(F, rows_d)
    piece_down, out_mine = exchange(
        S, F, 2, grads=((activated, upstream, rider(out_term, D)),), split=True
    )
    out_mine = out_mine[0, :rows_d].astype(F32)

    grad_act = dot_nt(upstream, w_down)
    grad_pre = jax.vjp(gelu_tanh, pre_act)[1](grad_act)[0].astype(BF)
    up_term = jnp.sum(grad_pre.astype(F32), axis=0).reshape(F, block_up)
    block_dense = slots * HEAD
    shards = (qkv_own,)
    if spread:
        shards += (lax.dynamic_slice_in_dim(dense_weight, j * block_dense, block_dense, 0),)
    piece_up, w_qkv, *w_dense, all_down = exchange(
        S, F, 3, grads=((normed, grad_pre, rider(up_term, cols_up)),), shards=shards,
        tokens=(piece_down,),
    )
    all_up = lax.all_gather(piece_up, "seq", axis=0)
    w_qkv = w_qkv.reshape(D, qkv_width)
    if spread:
        w_dense = w_dense[0].reshape(hp * HEAD, D)
    else:
        w_dense = lax.dynamic_slice_in_dim(
            lax.all_gather(dense_weight, "fsdp", axis=0, tiled=True), j * hp * HEAD, hp * HEAD, 0
        )

    projected = dot(normed, w_qkv) + bias_qkv
    grad_att = dot_nt(upstream, w_dense).astype(BF)
    attended, grad_mixed = attention(projected, grad_att, angle_tables(seg_row), seg_row)
    qkv_term = jnp.sum(grad_mixed.astype(F32), axis=0)
    qkv_term = jnp.broadcast_to(qkv_term[None], (F, qkv_width))
    grads = ((normed, grad_mixed, rider(qkv_term, qkv_width)),)
    if spread:
        grads += ((attended, upstream, None),)
    (piece_qkv,) = exchange(S, F, 4, grads=grads, merge=qkv_width)
    partial_out = (dot(attended, w_dense) + dot(activated, w_down)).astype(BF)
    partial_normed = (dot_nt(grad_mixed, w_qkv) + dot_nt(grad_pre, w_up)).astype(BF)
    branches, grad_normed, ln_mine, all_qkv = token_sums(
        S, F, 5, partial_out.reshape(S, tok, D), partial_normed.reshape(S, tok, D),
        standard, (piece_qkv,),
    )
    result = (inputs + branches + (b_dense + b_down)).astype(BF)
    scaled = grad_normed * gain
    grad_inputs = upstream_own.astype(F32) + inv_std * (
        scaled
        - jnp.mean(scaled, axis=-1, keepdims=True)
        - standard * jnp.mean(scaled * standard, axis=-1, keepdims=True)
    )

    grad_down = unpack_rows(all_down, block_up)
    grad_up = unpack_cols(all_up, rows_d, F)
    up_mine = all_up[:, rows_d, :block_up].astype(F32).reshape(-1)
    qkv_sums = from_qkv_cols(all_qkv[:, rows_d][:, None]).reshape(F, -1)
    qkv_mine = lax.dynamic_index_in_dim(qkv_sums, f, 0, keepdims=False).astype(F32)
    if spread and slots == 1:
        grad_qkv = unpack_qkv(all_qkv, rows_d, S, pairs)
    else:
        grad_qkv = from_qkv_cols(all_qkv[:, :rows_d]).astype(F32)
    if spread:
        chunks, at = [], rows_d + EXTRA
        for col in range(0, D, qkv_width):
            n = min(qkv_width, D - col)
            chunks.append(all_qkv[:, at : at + block_dense, :n])
            at += block_dense
        grad_dense = jnp.concatenate(chunks, axis=2).astype(F32).reshape(rows_d, D)
    else:
        part = lax.all_gather(dot_tn(attended, upstream).astype(BF), "seq", axis=0, tiled=True)
        grad_dense = lax.psum_scatter(part, "fsdp", scatter_dimension=0, tiled=True).astype(F32)
    return (
        result[None],
        grad_inputs[None],
        ln_mine[0],
        ln_mine[1],
        grad_qkv,
        qkv_mine,
        grad_dense,
        out_mine,
        grad_up,
        up_mine,
        grad_down,
        out_mine,
    )


def solution(mesh):
    row, mat = P("fsdp"), P("fsdp", None)
    act = P("fsdp", "seq", None)
    return jax.shard_map(
        body,
        mesh=mesh,
        in_specs=(
            act, row, row, mat, row, mat, row, mat, row, mat, row, mat, P("fsdp", "seq"), act,
        ),
        out_specs=(act, act, row, row, mat, row, mat, row, mat, row, mat, row),
        check_vma=False,
    )
```

```python
import functools

import jax
import jax.numpy as jnp
from jax import lax
from jax.experimental import pallas as pl
from jax.experimental.pallas import tpu as pltpu
from jax.sharding import PartitionSpec as P


HEADS = 32
HEAD = 64
ROT = 32
EPS = 1e-05
DOC_SHIFT = 1023
LANES = 2 * HEAD
BF = jnp.bfloat16
F32 = jnp.float32


def dot(left, right):
    return lax.dot_general(left, right, (((1,), (0,)), ((), ())), preferred_element_type=F32)


def dot_nt(left, right):
    return lax.dot_general(left, right, (((1,), (1,)), ((), ())), preferred_element_type=F32)


def dot_tn(left, right):
    return lax.dot_general(left, right, (((0,), (0,)), ((), ())), preferred_element_type=F32)


def columns(ref, cols):
    if len(ref.shape) == 2:
        return ref[:, cols]
    block = ref[:, :, cols]
    return block.reshape(-1, block.shape[-1])


def gelu_tanh(values_in):
    return jax.nn.gelu(values_in, approximate=True)


def turn(values, cos, sin_low, sin_high):
    half = ROT // 2
    return (
        values * cos
        - pltpu.roll(values, LANES - half, 1) * sin_low
        + pltpu.roll(values, half, 1) * sin_high
    )


def attention_kernel(
    rows, proj, grad_out, cos, sin_low, sin_high, seg_col, seg_row,
    out, grad_proj, qs, ks, vs, dk, dv, pause=None,
):
    length = proj.shape[0]
    blocks = length // rows
    scale = HEAD**-0.5
    for i in range(blocks):
        r = slice(i * rows, (i + 1) * rows)
        c, lo, hi = cos[r, :], sin_low[r, :], sin_high[r, :]
        qs[r, :] = turn(proj[r, 0:LANES], c, lo, hi).astype(BF) * jnp.asarray(scale, BF)
        ks[r, :] = turn(proj[r, LANES : 2 * LANES], c, lo, hi).astype(BF)
        vs[r, :] = proj[r, 2 * LANES : 3 * LANES].astype(BF)
    lane = lax.broadcasted_iota(jnp.int32, (rows, LANES), 1)
    first = lane < HEAD
    zero = jnp.zeros((rows, LANES), BF)
    for i in reversed(range(blocks)):
        r = slice(i * rows, (i + 1) * rows)
        n = (i + 1) * rows
        place_q = i * rows + lax.broadcasted_iota(jnp.int32, (rows, n), 0)
        place_k = lax.broadcasted_iota(jnp.int32, (rows, n), 1)
        allowed = (place_k <= place_q) & (seg_col[r, :] == seg_row[:, 0:n])
        q2, g2 = qs[r, :], grad_out[r, :]
        k, v = ks[0:n, :], vs[0:n, :]
        o_parts, dq_parts = [], []
        for h in range(2):
            mine = first if h == 0 else ~first
            q = jnp.where(mine, q2, zero)
            g = jnp.where(mine, g2, zero)
            s = jnp.where(allowed, dot_nt(q, k), -1e30)
            e = jnp.exp(s - jnp.max(s, axis=-1, keepdims=True))
            p = e * (1.0 / jnp.sum(e, axis=-1, keepdims=True))
            pb = p.astype(BF)
            o_parts.append(dot(pb, v))
            dp = dot_nt(g, v)
            inner = jnp.sum(p * dp, axis=-1, keepdims=True)
            ds = (p * (dp - inner)).astype(BF)
            dq_parts.append(dot(ds, k))
            dk_new, dv_new = dot_tn(ds, q), dot_tn(pb, g)
            if i == blocks - 1 and h == 0:
                dk[...] = dk_new
                dv[...] = dv_new
            else:
                dk[0:n, :] += dk_new
                dv[0:n, :] += dv_new
        out[r, :] = jnp.where(first, o_parts[0], o_parts[1]).astype(BF)
        dq = (jnp.where(first, dq_parts[0], dq_parts[1]) * scale).astype(BF).astype(F32)
        c, lo, hi = cos[r, :], sin_low[r, :], sin_high[r, :]
        grad_proj[r, 0:LANES] = turn(dq, c, -lo, -hi).astype(BF)
        if pause is not None:
            pause(i)
    for i in range(blocks):
        r = slice(i * rows, (i + 1) * rows)
        c, lo, hi = cos[r, :], sin_low[r, :], sin_high[r, :]
        grad_k = dk[r, :].astype(BF).astype(F32)
        grad_proj[r, LANES : 2 * LANES] = turn(grad_k, c, -lo, -hi).astype(BF)
        grad_proj[r, 2 * LANES : 3 * LANES] = dv[r, :].astype(BF)


def attention(proj, grad_att, tables, segments):
    length = proj.shape[0]
    pairs = grad_att.shape[1] // LANES
    rows = 256
    whole = lambda shape: pl.BlockSpec(shape, lambda p: (0, 0))
    return pl.pallas_call(
        functools.partial(attention_kernel, rows),
        grid=(pairs,),
        out_shape=(
            jax.ShapeDtypeStruct((length, pairs * LANES), BF),
            jax.ShapeDtypeStruct((length, 3 * pairs * LANES), BF),
        ),
        in_specs=[
            pl.BlockSpec((length, 3 * LANES), lambda p: (0, p)),
            pl.BlockSpec((length, LANES), lambda p: (0, p)),
            whole((length, LANES)),
            whole((length, LANES)),
            whole((length, LANES)),
            whole((length, 1)),
            whole((1, length)),
        ],
        out_specs=(
            pl.BlockSpec((length, LANES), lambda p: (0, p)),
            pl.BlockSpec((length, 3 * LANES), lambda p: (0, p)),
        ),
        scratch_shapes=[pltpu.VMEM((length, LANES), BF)] * 3
        + [pltpu.VMEM((length, LANES), F32)] * 2,
        cost_estimate=pl.CostEstimate(
            flops=14 * pairs * length * length * LANES,
            bytes_accessed=pairs * length * LANES * 24,
            transcendentals=pairs * length * length,
        ),
    )(proj, grad_att, *tables, segments[:, None], segments[None, :])


def angle_tables(seg_row):
    length = seg_row.shape[0]
    position = jnp.arange(length, dtype=jnp.int32) + jnp.where(seg_row > 0, DOC_SHIFT, 0)
    inverse = 1.0 / 10000.0 ** (jnp.arange(0, ROT, 2, dtype=F32) / ROT)
    inverse = jnp.tile(inverse, LANES // (ROT // 2))
    angles = position.astype(F32)[:, None] * inverse[None, :]
    cosine, sine = jnp.cos(angles), jnp.sin(angles)
    lane = jnp.arange(LANES)[None, :] % HEAD
    low = lane < ROT // 2
    return (
        jnp.where(lane < ROT, cosine, 1.0),
        jnp.where(low, sine, 0.0),
        jnp.where((lane < ROT) & ~low, sine, 0.0),
    )


MESH = pl.DeviceIdType.MESH


def remote(src, dst, send, recv, device):
    return pltpu.make_async_remote_copy(
        src_ref=src, dst_ref=dst, send_sem=send, recv_sem=recv, device_id=device,
        device_id_type=MESH,
    )


class Place:
    def __init__(self, S, F):
        self.S, self.F, self.Q = S, F, S // 2
        self.j, self.f = lax.axis_index("seq"), lax.axis_index("fsdp")
        self.q, self.c = self.j // 2, lax.rem(self.j, 2)
        self.partner = 2 * self.q + 1 - self.c
        self.low = 1 - self.q // (self.Q // 2)
        self.side = 2 * (2 * self.low - 1)
        self.end = self.low * self.q + (1 - self.low) * (self.Q - 1 - self.q)

    def greet(self, over_fsdp, over_seq):
        barrier = pltpu.get_barrier_semaphore()

        def signal(j, f):
            pl.semaphore_signal(barrier, inc=1, device_id=(j, f), device_id_type=MESH)

        count = 0
        if over_fsdp:
            for k in range(1, self.F):
                signal(self.j, lax.rem(self.f + k, self.F))
            count += self.F - 1
        if over_seq == "all":
            for k in range(1, self.S):
                signal(lax.rem(self.j + k, self.S), self.f)
            count += self.S - 1
        elif over_seq == "line":
            signal(self.partner, self.f)

            @pl.when(self.q > 0)
            def _():
                signal(self.j - 2, self.f)

            @pl.when(self.q < self.Q - 1)
            def _():
                signal(self.j + 2, self.f)

            count += 1 + (self.q + self.Q - 1) // self.Q + (2 * self.Q - 2 - self.q) // self.Q
        pl.semaphore_wait(barrier, count)


class ShardGather:
    @staticmethod
    def scratch(F):
        n = 6 if F == 4 else F - 1
        return [pltpu.SemaphoreType.DMA((n,)), pltpu.SemaphoreType.DMA((n,)),
                pltpu.SemaphoreType.DMA]

    def __init__(self, at, src, dst, send, recv, local):
        self.at, self.src, self.dst = at, src, dst
        f, j = at.f, at.j
        self.own = pltpu.make_async_copy(src, dst.at[f], local)
        self.first, self.later, self.arrivals = [], [], []
        if at.F == 4:
            nx = f + 1 - 2 * lax.rem(f, 2)
            ny = lax.rem(f + 2, 4)
            nd = lax.rem(nx + 2, 4)
            half = src.shape[0] // 2
            a, b = pl.ds(0, half), pl.ds(half, half)
            table = ((nx, a), (nx, b), (ny, a), (ny, b))
            for i, (to, rows) in enumerate(table):
                self.first.append(
                    remote(src.at[rows], dst.at[f, rows], send.at[i], recv.at[i], (j, to))
                )
                self.arrivals.append(
                    remote(src.at[rows], dst.at[to, rows], send.at[i], recv.at[i], (j, to))
                )
            for i, (of, rows, to) in ((4, (nx, a, ny)), (5, (ny, b, nx))):
                self.later.append(
                    remote(dst.at[of, rows], dst.at[of, rows], send.at[i], recv.at[i], (j, to))
                )
                self.arrivals.append(
                    remote(dst.at[nd, rows], dst.at[nd, rows], send.at[i], recv.at[i], (j, to))
                )
        else:
            for k in range(1, at.F):
                to, of = lax.rem(f + k, at.F), lax.rem(f + at.F - k, at.F)
                self.first.append(
                    remote(src, dst.at[f], send.at[k - 1], recv.at[k - 1], (j, to))
                )
                self.arrivals.append(
                    remote(src, dst.at[of], send.at[k - 1], recv.at[k - 1], (j, to))
                )

    def start(self):
        self.own.start()
        for copy in self.first:
            copy.start()

    def relay(self):
        if self.later:
            self.arrivals[0].wait_recv()
            self.later[0].start()
            self.arrivals[3].wait_recv()
            self.later[1].start()

    def arrived(self):
        for i, copy in enumerate(self.arrivals):
            if not (self.later and i in (0, 3)):
                copy.wait_recv()
        self.own.wait()

    def finish(self):
        for copy in self.first + self.later:
            copy.wait_send()


class TokenGather:
    @staticmethod
    def scratch(S):
        Q = S // 2
        return [pltpu.SemaphoreType.DMA((2 * Q,)), pltpu.SemaphoreType.DMA((2 * Q,)),
                pltpu.SemaphoreType.DMA((S,)), pltpu.SemaphoreType.DMA]

    def __init__(self, at, src, dst, send, share, recv, local, rows=None):
        self.at, self.src, self.dst, self.rows = at, src, dst, rows
        self.send, self.share, self.recv = send, share, recv
        self.own = pltpu.make_async_copy(src, self.place(at.j), local)

    def place(self, slot):
        return self.dst.at[slot] if self.rows is None else self.dst.at[slot, self.rows]

    def onward(self, slot, source, i, by):
        to = self.place(slot)
        return remote(
            source, to, self.send.at[i], self.recv.at[slot], (self.at.j + by, self.at.f)
        )

    def given(self, slot, source, i):
        to = self.place(slot)
        return remote(
            source, to, self.share.at[i], self.recv.at[slot], (self.at.partner, self.at.f)
        )

    def own_copies(self):
        at, j = self.at, self.at.j
        return (
            self.onward(j, self.src, 0, at.side), self.onward(j, self.src, at.Q, -at.side),
            self.given(j, self.src, 0),
        )

    def start(self):
        self.own.start()
        far, near, part = self.own_copies()
        far.start()

        @pl.when(self.at.end > 0)
        def _():
            near.start()

        part.start()

    def from_near(self, d):
        at = self.at
        slot = at.j - at.side * d
        here = self.place(slot)
        return self.onward(slot, here, d, at.side), self.given(slot, here, d)

    def from_far(self, d):
        at = self.at
        slot = at.j + at.side * d
        here = self.place(slot)
        return self.onward(slot, here, at.Q + d, -at.side), self.given(slot, here, at.Q + d)

    def near(self, d):
        if d > self.at.Q // 2 - 1:
            return

        @pl.when(self.at.end >= d)
        def _():
            onward, part = self.from_near(d)
            onward.wait_recv()
            onward.start()
            part.start()

    def far(self, d):
        @pl.when(self.at.end + d <= self.at.Q - 1)
        def _():
            onward, part = self.from_far(d)
            part.wait_recv()

            @pl.when(self.at.end > 0)
            def _():
                onward.start()

            part.start()

    def arrived(self):
        for q in range(self.at.Q):
            slot = 2 * q + 1 - self.at.c
            self.given(slot, self.place(slot), 0).wait_recv()
        self.own.wait()

    def finish(self):
        at, Q = self.at, self.at.Q
        far, near, part = self.own_copies()
        far.wait_send()

        @pl.when(at.end > 0)
        def _():
            near.wait_send()

        part.wait_send()
        for d in range(1, Q):
            if d <= Q // 2 - 1:

                @pl.when(at.end >= d)
                def _():
                    onward, part = self.from_near(d)
                    onward.wait_send()
                    part.wait_send()

            @pl.when(at.end + d <= Q - 1)
            def _():
                onward, part = self.from_far(d)

                @pl.when(at.end > 0)
                def _():
                    onward.wait_send()

                part.wait_send()


class GradReduce:
    @staticmethod
    def scratch(F, rows, n):
        return [pltpu.VMEM((F, rows, n), BF), pltpu.VMEM((F - 1, rows, n), BF),
                pltpu.SemaphoreType.DMA((F - 1,)), pltpu.SemaphoreType.DMA((F - 1,))]

    def __init__(self, at, left, right, extra, made, got, send, recv):
        self.at, self.left, self.right, self.extra = at, left, right, extra
        self.made, self.got, self.send, self.recv = made, got, send, recv
        self.n = right.shape[-1]
        self.rows = left.shape[-1] // at.F
        self.tile = next(t for t in (512, 384, 256, 128) if self.n % t == 0)

    def copy(self, k):
        at = self.at
        to = lax.rem(at.f + k, at.F)
        return remote(
            self.made.at[to], self.got.at[k - 1], self.send.at[k - 1], self.recv.at[k - 1],
            (at.j, to),
        )

    def start(self):
        at, rows = self.at, self.rows
        aligned = rows % 128 == 0
        for t in range(0, self.n, self.tile) if not aligned else ():
            cols = slice(t, t + self.tile)
            full = dot_tn(self.left[...], columns(self.right, cols)).astype(BF)
            for p in range(at.F):
                self.made[p, 0:rows, cols] = full[p * rows : (p + 1) * rows, :]
        for k in list(range(1, at.F)) + [0]:
            p = lax.rem(at.f + k, at.F)
            if aligned:
                block = columns(self.left, pl.ds(pl.multiple_of(p * rows, 128), rows))
                for t in range(0, self.n, self.tile):
                    cols = slice(t, t + self.tile)
                    made = dot_tn(block, columns(self.right, cols))
                    self.made[p, 0:rows, cols] = made.astype(BF)
            if callable(self.extra):
                self.made[p, rows:, :] = self.extra()
            elif self.extra is not None:
                self.made[p, rows : rows + self.extra.shape[1], :] = self.extra[p].astype(BF)
            if k:
                self.copy(k).start()

    def finish(self, store):
        at = self.at
        for k in range(1, at.F):
            self.copy(k).wait_recv()
        for t in range(0, self.n, self.tile):
            cols = slice(t, t + self.tile)
            total = self.made[at.f, :, cols].astype(F32)
            for k in range(1, at.F):
                total += self.got[k - 1, :, cols].astype(F32)
            store(t, self.tile, total.astype(BF))
        for k in range(1, at.F):
            self.copy(k).wait_send()


EXTRA = 16


def exchange(S, F, collective_id, grads=(), shards=(), tokens=(), split=False):
    operands, in_specs = [], []
    vmem = pl.BlockSpec(memory_space=pltpu.VMEM)
    outs, out_specs, scratch = [], [], []
    shapes = []
    for left, right, extra in grads:
        rows, n = left.shape[1] // F + (0 if extra is None else EXTRA), right.shape[1]
        operands += [left, right] + ([] if extra is None else [extra])
        scratch += GradReduce.scratch(F, rows, n)
        shapes.append((rows, n))
        if split:
            outs.append(jax.ShapeDtypeStruct((rows - EXTRA, n), BF))
            outs.append(jax.ShapeDtypeStruct((EXTRA, n), BF))
        else:
            outs.append(jax.ShapeDtypeStruct((rows, n), BF))
    out_specs += [vmem] * len(outs)
    for array in shards:
        operands.append(array)
        outs.append(jax.ShapeDtypeStruct((F,) + array.shape, BF))
        out_specs.append(pl.BlockSpec(memory_space=pl.ANY))
        scratch += ShardGather.scratch(F)
    for array in tokens:
        operands.append(array)
        outs.append(jax.ShapeDtypeStruct((S,) + array.shape, BF))
        out_specs.append(pl.BlockSpec(memory_space=pl.ANY))
        scratch += TokenGather.scratch(S)
    in_specs = [vmem] * len(operands)
    n_in, n_out = len(operands), len(outs)

    def kernel(*refs):
        ins, results, rest = list(refs[:n_in]), list(refs[n_in : n_in + n_out]), list(
            refs[n_in + n_out :]
        )
        take = lambda items, n: [items.pop(0) for _ in range(n)]
        at = Place(S, F)
        jobs, stores = [], []
        for (_, _, extra), (rows, n) in zip(grads, shapes):
            left, right = take(ins, 2)
            extra_ref = None if extra is None else take(ins, 1)[0]
            jobs.append(GradReduce(at, left, right, extra_ref, *take(rest, 4)))
            target = take(results, 1)[0]
            rider_ref = take(results, 1)[0] if split else None

            def store(t, width, value, target=target, rows=rows, rider_ref=rider_ref):
                if split:
                    target[:, t : t + width] = value[: rows - EXTRA]
                    rider_ref[:, t : t + width] = value[rows - EXTRA :]
                else:
                    target[:, t : t + width] = value

            stores.append(store)
        spreads = [
            ShardGather(at, take(ins, 1)[0], take(results, 1)[0], *take(rest, 3)) for _ in shards
        ]
        lines = [
            TokenGather(at, take(ins, 1)[0], take(results, 1)[0], *take(rest, 4)) for _ in tokens
        ]
        at.greet(bool(jobs or spreads), "line" if lines else "")
        for item in lines + spreads:
            item.start()
        for job in jobs:
            job.start()
        waiting = list(spreads)
        for d in range(1, at.Q) if lines else ():
            for item in lines:
                item.near(d)
                item.far(d)
            if waiting:
                waiting.pop(0).relay()
        for item in waiting:
            item.relay()
        for job, store in zip(jobs, stores):
            job.finish(store)
        for item in spreads + lines:
            item.arrived()
            item.finish()

    flops = sum(2 * l.shape[0] * l.shape[1] * r.shape[1] for l, r, _ in grads)
    moved = sum(o.size * 2 for o in outs)
    return pl.pallas_call(
        kernel,
        out_shape=tuple(outs),
        in_specs=in_specs,
        out_specs=tuple(out_specs),
        scratch_shapes=scratch,
        compiler_params=pltpu.CompilerParams(
            collective_id=collective_id, has_side_effects=True
        ),
        cost_estimate=pl.CostEstimate(
            flops=flops, bytes_accessed=20 * moved, transcendentals=0
        ),
    )(*operands)


LN_ROWS = 8


class Loads:
    def __init__(self, sources, buffers, sems):
        self.copies = [
            pltpu.make_async_copy(src, buf, sems.at[i])
            for i, (src, buf) in enumerate(zip(sources, buffers))
        ]
        self.buffers = buffers

    def start(self):
        for copy in self.copies:
            copy.start()

    def ready(self, *which):
        for i in which:
            self.copies[i].wait()


class LineSum:
    @staticmethod
    def scratch(S, t, d):
        Q = S // 2
        return [pltpu.VMEM((Q, t, d), BF), pltpu.VMEM((Q + 1, t, d), BF),
                pltpu.SemaphoreType.DMA((2 * Q,)), pltpu.SemaphoreType.DMA((2 * Q,)),
                pltpu.SemaphoreType.DMA((Q,)), pltpu.SemaphoreType.DMA((Q,))]

    def __init__(self, at, part, result, pair, got, s_line, r_line, s_pair, r_pair):
        self.at, self.part, self.result, self.pair, self.got = at, part, result, pair, got
        self.s_line, self.r_line, self.s_pair, self.r_pair = s_line, r_line, s_pair, r_pair

    def share(self, slot):
        at = self.at
        return remote(
            self.part.at[2 * slot + 1 - at.c], self.pair.at[slot], self.s_pair.at[slot],
            self.r_pair.at[slot], (at.partner, at.f),
        )

    def hop(self, slot, up, last):
        at = self.at
        i = slot + (1 - up) * at.Q
        into = slot + last * (at.Q - slot)
        return remote(
            self.pair.at[slot], self.got.at[into], self.s_line.at[i], self.r_line.at[i],
            (at.j + 4 * up - 2, at.f),
        )

    def last(self, slot, up):
        at = self.at
        return (1 - up) * (1 - (at.q - 1 - slot + at.Q - 1) // at.Q)

    def start(self):
        order = []
        for i in range(self.at.Q):
            for slot in (self.at.Q - 1 - i, i):
                if slot not in order:
                    order.append(slot)
        for slot in order:
            self.share(slot).start()

    def base(self, slot):
        self.share(slot).wait_recv()
        return self.part[2 * slot + self.at.c].astype(F32) + self.pair[slot].astype(F32)

    def pass_on(self, slot, up):
        at = self.at

        @pl.when((2 * up - 1) * (slot - at.q) > 0)
        def _():
            value = self.base(slot)
            self.hop(slot, up, 0).wait_recv()
            self.pair[slot] = (value + self.got[slot].astype(F32)).astype(BF)
            self.hop(slot, up, self.last(slot, up)).start()

    def ends(self, steps):
        at = self.at

        @pl.when(at.end == 0)
        def _():
            for i in steps:
                slot = at.low * (at.Q - 1 - i) + (1 - at.low) * i
                self.pair[slot] = self.base(slot).astype(BF)
                self.hop(slot, at.low, self.last(slot, at.low)).start()

    def near(self, i):
        at = self.at

        @pl.when(at.end > 0)
        def _():
            self.pass_on(at.low * (at.Q - 1 - i) + (1 - at.low) * i, at.low)

    def far(self, i):
        at = self.at
        self.pass_on((1 - at.low) * (at.Q - 1 - i) + at.low * i, 1 - at.low)

    def total(self):
        at = self.at
        self.result[...] = self.base(at.q)

        @pl.when(at.q > 0)
        def _():
            self.hop(at.q, 1, 0).wait_recv()
            self.result[...] += self.got[at.q].astype(F32)

        @pl.when(at.q < at.Q - 1)
        def _():
            self.hop(at.q, 0, 1).wait_recv()
            self.result[...] += self.got[at.Q].astype(F32)

    def finish(self):
        q = self.at.q
        for slot in range(self.at.Q):
            self.share(slot).wait_send()

            @pl.when(q < slot)
            def _():
                self.hop(slot, 1, 0).wait_send()

            @pl.when(q > slot)
            def _():
                self.hop(slot, 0, 0).wait_send()


class VectorSum:
    @staticmethod
    def scratch(S, F, w):
        return [
            pltpu.VMEM((F, LN_ROWS, w), F32),
            pltpu.VMEM((F, LN_ROWS, w), F32),
            pltpu.VMEM((S, LN_ROWS, w), F32),
            pltpu.SemaphoreType.DMA((F - 1,)),
            pltpu.SemaphoreType.DMA((F,)),
            pltpu.SemaphoreType.DMA((S - 1,)),
            pltpu.SemaphoreType.DMA((S,)),
        ]

    def __init__(self, at, made, by_shard, by_seq, s_f, r_f, s_s, r_s):
        self.at, self.made, self.by_shard, self.by_seq = at, made, by_shard, by_seq
        j, f, S, F = at.j, at.f, at.S, at.F
        self.over_f, self.over_s = [], []
        for k in range(1, F):
            to, of = lax.rem(f + k, F), lax.rem(f + F - k, F)
            self.over_f.append(
                (remote(made.at[to], by_shard.at[f], s_f.at[k - 1], r_f.at[f], (j, to)),
                 remote(made.at[to], by_shard.at[of], s_f.at[k - 1], r_f.at[of], (j, to)))
            )
        for k in range(1, S):
            to, of = lax.rem(j + k, S), lax.rem(j + S - k, S)
            self.over_s.append(
                (remote(by_seq.at[j], by_seq.at[j], s_s.at[k - 1], r_s.at[j], (to, f)),
                 remote(by_seq.at[j], by_seq.at[of], s_s.at[k - 1], r_s.at[of], (to, f)))
            )

    def start(self):
        for copy, _ in self.over_f:
            copy.start()
        self.by_shard[self.at.f] = self.made[self.at.f]

    def turn_to_seq(self):
        for _, arrival in self.over_f:
            arrival.wait_recv()
        total = self.by_shard[0]
        for p in range(1, self.at.F):
            total += self.by_shard[p]
        self.by_seq[self.at.j] = total
        for copy, _ in self.over_s:
            copy.start()

    def finish(self, result):
        for _, arrival in self.over_s:
            arrival.wait_recv()
        total = self.by_seq[0]
        for p in range(1, self.at.S):
            total += self.by_seq[p]
        result[...] = total
        for copy, _ in self.over_f + self.over_s:
            copy.wait_send()


def closing(
    S, F, collective_id, tok, normed, upstream, grad_mixed, attended, activated, grad_pre,
    w_dense, w_down, w_qkv, w_up, extra, standard, with_dense,
):
    L, D = normed.shape
    w = D // F
    chunk = 3 * LANES
    pairs = grad_mixed.shape[1] // chunk
    grads = [(D // F + EXTRA, chunk)] * pairs
    if with_dense:
        grads.append((attended.shape[1] // F, D))
    big = [normed, grad_mixed, attended, activated, w_dense, w_down, grad_pre, w_qkv, w_up]
    if with_dense:
        big.append(upstream)
    tile = 512
    m = len(grads)

    def kernel(*refs):
        refs = list(refs)
        take = lambda n: [refs.pop(0) for _ in range(n)]
        at = Place(S, F)
        sources = take(len(big))
        extra_ref, standard_ref = take(2)
        branches, normed_sum, ln_out = take(3)
        gathered = take(m)
        loads = Loads(sources, take(len(big)), take(1)[0])
        x, gm, att, act, wd, wdn, gp, wq, wu = loads.buffers[:9]
        jobs, packed, lines = [], [], []
        for i in range(pairs):
            cols = slice(i * chunk, (i + 1) * chunk)
            jobs.append(GradReduce(at, x, gm.at[:, cols], extra_ref.at[:, :, cols], *take(4)))
        if with_dense:
            jobs.append(GradReduce(at, att, loads.buffers[9], None, *take(4)))
        for i in range(m):
            packed.append(take(1)[0])
            lines.append(TokenGather(at, packed[i], gathered[i], *take(4)))
        parts = take(2)
        sums = [
            LineSum(at, part, res, *take(6)) for part, res in zip(parts, (branches, normed_sum))
        ]
        vectors = VectorSum(at, *take(7))
        loads.start()
        at.greet(True, "all")
        loads.ready(0, 1)
        for job in jobs[:pairs]:
            job.start()
        loads.ready(2)
        if with_dense:
            loads.ready(9)
            jobs[-1].start()
        loads.ready(3, 4, 5)

        @pl.loop(0, D // tile)
        def _(i):
            cols = pl.ds(pl.multiple_of(i * tile, tile), tile)
            made = dot(att[...], wd[:, cols]) + dot(act[...], wdn[:, cols])
            parts[0][:, :, cols] = made.astype(BF).reshape(S, tok, tile)

        sums[0].start()
        sums[0].ends([0])
        loads.ready(6, 7, 8)

        @pl.loop(0, D // tile)
        def _(i):
            rows = pl.ds(pl.multiple_of(i * tile, tile), tile)
            made = dot_nt(gm[...], wq[rows, :]) + dot_nt(gp[...], wu[rows, :])
            parts[1][:, :, rows] = made.astype(BF).reshape(S, tok, tile)

        sums[1].start()
        sums[1].ends([0])

        def reduced(i):
            def store(t, wide, value):
                packed[i][:, t : t + wide] = value

            jobs[i].finish(store)
            lines[i].start()

        for i in range(m):
            reduced(i)
            if i < 2:
                sums[i].near(0)
            lines[i].far(1)
        for i in range(m, 2):
            sums[i].near(0)
        for item in sums:
            item.ends(range(1, at.Q - 1))
        for i in range(max(m, 2)):
            if i < 2:
                sums[i].far(0)
            if i < m:
                lines[i].near(1)
        for step in range(1, at.Q - 1):
            for line in lines:
                line.far(step + 1)
            for item in sums:
                item.near(step)
            for item in sums:
                item.far(step)
            for line in lines:
                line.near(step + 1)
        for item in sums:
            item.total()
        grad_normed = normed_sum[...]
        both = jnp.concatenate(
            [
                jnp.sum(grad_normed * standard_ref[...], axis=0, keepdims=True),
                jnp.sum(grad_normed, axis=0, keepdims=True),
                jnp.zeros((LN_ROWS - 2, D), F32),
            ],
            axis=0,
        )
        for p in range(F):
            vectors.made[p] = both[:, p * w : (p + 1) * w]
        vectors.start()
        vectors.turn_to_seq()
        for line in lines:
            line.arrived()
            line.finish()
        vectors.finish(ln_out)
        for item in sums:
            item.finish()

    vmem = pl.BlockSpec(memory_space=pltpu.VMEM)
    anywhere = pl.BlockSpec(memory_space=pl.ANY)
    scratch = [pltpu.VMEM(a.shape, a.dtype) for a in big]
    scratch.append(pltpu.SemaphoreType.DMA((len(big),)))
    for rows, n in grads:
        scratch += GradReduce.scratch(F, rows, n)
    for rows, n in grads:
        scratch.append(pltpu.VMEM((rows, n), BF))
        scratch += TokenGather.scratch(S)
    scratch += [pltpu.VMEM((S, tok, D), BF)] * 2
    scratch += LineSum.scratch(S, tok, D) * 2
    scratch += VectorSum.scratch(S, F, w)
    full = jax.ShapeDtypeStruct((tok, D), F32)
    return pl.pallas_call(
        kernel,
        out_shape=(full, full, jax.ShapeDtypeStruct((LN_ROWS, w), F32))
        + tuple(jax.ShapeDtypeStruct((S, rows, n), BF) for rows, n in grads),
        in_specs=[anywhere] * len(big) + [vmem] * 2,
        out_specs=(vmem,) * 3 + (anywhere,) * m,
        scratch_shapes=scratch,
        compiler_params=pltpu.CompilerParams(
            collective_id=collective_id, has_side_effects=True,
            vmem_limit_bytes=67_000_000 if L > 1024 else None,
        ),
        cost_estimate=pl.CostEstimate(
            flops=6 * L * D * (grad_mixed.shape[1] + activated.shape[1]),
            bytes_accessed=80 * L * D,
            transcendentals=0,
        ),
    )(*big, extra, standard)


def attend_and_close(
    S, F, collective_id, tok, normed, upstream, feed_out, feed_gn, w_dense, w_qkv, rest_up, tables,
     seg_col, seg_row, bias, standard,
):
    L, D = S * tok, normed.shape[2]
    w = D // F
    chunk = 3 * LANES
    pairs = w_qkv.shape[1] // chunk
    rows_att = 256
    grads = [(D // F + EXTRA, chunk)] * pairs + [(pairs * LANES // F, D)]
    m = len(grads)
    big = [normed, upstream, w_qkv, w_dense, feed_out, feed_gn]
    small = [*tables, seg_col, seg_row, bias, standard, rest_up]
    tile = 512
    late = rest_up.shape[0]

    def kernel(*refs):
        refs = list(refs)
        take = lambda n: [refs.pop(0) for _ in range(n)]
        at = Place(S, F)
        sources = take(len(big))
        cos, low, high, seg_c, seg_r, bias_ref, standard_ref, up_ref = take(8)
        branches, normed_sum, ln_out, all_up = take(4)
        gathered = take(m)
        loads = Loads(sources, take(len(big)), take(1)[0])
        x, g, wq, wd, out_part, gn_part = loads.buffers
        gm, att, proj, gatt, qs, ks, vs, dk, dv = take(9)
        ones = jnp.ones((16, L), BF)
        jobs, lines = [], []
        for i in range(pairs):
            cols = slice(i * chunk, (i + 1) * chunk)
            total_row = lambda cols=cols: dot(ones, gm[:, cols]).astype(BF)
            jobs.append(GradReduce(at, x, gm.at[:, cols], total_row, *take(4)))
        jobs.append(GradReduce(at, att, g, None, *take(4)))
        for i in range(m):
            lines.append(TokenGather(at, jobs[i].made.at[at.f], gathered[i], *take(4)))
        ups = [
            TokenGather(at, up_ref.at[i], all_up.at[i], *take(4)) for i in range(late)
        ]
        parts = [out_part, gn_part]
        sums = [
            LineSum(at, part, res, *take(6)) for part, res in zip(parts, (branches, normed_sum))
        ]
        vectors = VectorSum(at, *take(7))
        loads.start()
        at.greet(True, "all")
        for up in ups:
            up.start()
        loads.ready(0, 1, 2, 3)

        @pl.loop(0, pairs)
        def _(p):
            cols = pl.ds(pl.multiple_of(p * chunk, LANES), chunk)
            lanes = pl.ds(pl.multiple_of(p * LANES, LANES), LANES)

            @pl.loop(0, L // rows_att)
            def _(i):
                slots = pl.ds(i * (rows_att // tok), rows_att // tok)
                rows = pl.ds(pl.multiple_of(i * rows_att, rows_att), rows_att)
                block = x[slots].reshape(rows_att, D)
                proj[rows, :] = dot(block, wq[:, cols]) + bias_ref[:, cols]
                block = g[slots].reshape(rows_att, D)
                gatt[rows, :] = dot_nt(block, wd[lanes, :]).astype(BF)

            def during(pair, *steps):
                @pl.when(p == pair)
                def _():
                    for step in steps:
                        step()

            def serve(i, d):
                return lambda: (ups[i].near(d), ups[i].far(d))

            during(0, serve(0, 1))
            during(1, serve(0, 2))

            def pause(i):
                if i == 3:
                    during(0, serve(1, 1))
                    during(1, serve(1, 2))
                if i == 2:
                    during(0, *(serve(k, 1) for k in range(2, late)))
                    during(1, *(serve(k, 2) for k in range(2, late)))

            attention_kernel(
                rows_att, proj, gatt, cos, low, high, seg_c, seg_r, att.at[:, lanes],
                gm.at[:, cols], qs, ks, vs, dk, dv, pause,
            )
            during(0, jobs[0].start)

        loads.ready(4)

        @pl.loop(0, D // tile)
        def _(i):
            cols = pl.ds(pl.multiple_of(i * tile, tile), tile)
            made = columns(out_part, cols).astype(F32) + dot(att[...], wd[:, cols])
            out_part[:, :, cols] = made.astype(BF).reshape(S, tok, tile)

        sums[0].start()
        sums[0].ends([0])
        jobs[1].start()
        loads.ready(5)

        @pl.loop(0, D // tile)
        def _(i):
            rows = pl.ds(pl.multiple_of(i * tile, tile), tile)
            made = columns(gn_part, rows).astype(F32) + dot_nt(gm[...], wq[rows, :])
            gn_part[:, :, rows] = made.astype(BF).reshape(S, tok, tile)

        sums[1].start()
        sums[1].ends([0])

        def reduced(i):
            def store(t, wide, value):
                jobs[i].made[at.f, :, t : t + wide] = value

            jobs[i].finish(store)
            lines[i].start()

        reduced(0)
        for job in jobs[2:]:
            job.start()
        for d in range(3, at.Q):
            for up in ups:
                up.near(d)
                up.far(d)
        lines[0].far(1)

        for item in sums:
            item.ends([1])
        for i in range(m):
            if i:
                reduced(i)
            if i < 2:
                sums[i].near(0)
            if i:
                lines[i].far(1)
        for item in sums:
            item.ends(range(2, at.Q - 1))
        for i in range(m):
            if i < 2:
                sums[i].far(0)
            lines[i].near(1)
        for step in range(1, at.Q - 1):
            for line in lines:
                line.far(step + 1)
            for item in sums:
                item.near(step)
            for item in sums:
                item.far(step)
            for line in lines:
                line.near(step + 1)
        for item in sums:
            item.total()
        grad_normed = normed_sum[...]
        both = jnp.concatenate(
            [
                jnp.sum(grad_normed * standard_ref[...], axis=0, keepdims=True),
                jnp.sum(grad_normed, axis=0, keepdims=True),
                jnp.zeros((LN_ROWS - 2, D), F32),
            ],
            axis=0,
        )
        for p in range(F):
            vectors.made[p] = both[:, p * w : (p + 1) * w]
        vectors.start()
        vectors.turn_to_seq()
        for line in ups + lines:
            line.arrived()
            line.finish()
        vectors.finish(ln_out)
        for item in sums:
            item.finish()

    vmem = pl.BlockSpec(memory_space=pltpu.VMEM)
    anywhere = pl.BlockSpec(memory_space=pl.ANY)
    scratch = [pltpu.VMEM(a.shape, a.dtype) for a in big]
    scratch.append(pltpu.SemaphoreType.DMA((len(big),)))
    scratch += [
        pltpu.VMEM((L, pairs * chunk), BF),
        pltpu.VMEM((L, pairs * LANES), BF),
        pltpu.VMEM((L, chunk), F32),
    ]
    scratch += [pltpu.VMEM((L, LANES), BF)] * 4 + [pltpu.VMEM((L, LANES), F32)] * 2
    for rows, n in grads:
        scratch += GradReduce.scratch(F, rows, n)
    scratch += TokenGather.scratch(S) * m
    scratch += TokenGather.scratch(S) * late
    scratch += LineSum.scratch(S, tok, D) * 2
    scratch += VectorSum.scratch(S, F, w)
    full = jax.ShapeDtypeStruct((tok, D), F32)
    return pl.pallas_call(
        kernel,
        out_shape=(
            full, full, jax.ShapeDtypeStruct((LN_ROWS, w), F32),
            jax.ShapeDtypeStruct((late, S) + rest_up.shape[1:], BF),
        )
        + tuple(jax.ShapeDtypeStruct((S, rows, n), BF) for rows, n in grads),
        in_specs=[anywhere] * len(big) + [vmem] * len(small),
        out_specs=(vmem,) * 3 + (anywhere,) * (1 + m),
        scratch_shapes=scratch,
        compiler_params=pltpu.CompilerParams(
            collective_id=collective_id, has_side_effects=True, vmem_limit_bytes=67_000_000
        ),
        cost_estimate=pl.CostEstimate(
            flops=10 * L * D * pairs * chunk,
            bytes_accessed=100 * L * D,
            transcendentals=pairs * L * L,
        ),
    )(*big, *small)


class CornerReduce:
    @staticmethod
    def scratch(rows, n):
        return [pltpu.VMEM((4, rows, n), BF), pltpu.VMEM((3, rows, n), BF),
                pltpu.SemaphoreType.DMA((3,)), pltpu.SemaphoreType.DMA((3,))]

    def __init__(self, at, axis, made, got, send, recv):
        f = at.f
        nx, ny = f + 1 - 2 * lax.rem(f, 2), lax.rem(f + 2, 4)
        self.at, self.made, self.got = at, made, got
        self.one, self.two = (nx, ny) if axis == 0 else (ny, nx)
        self.far = lax.rem(nx + 2, 4)
        self.copies = [
            remote(made.at[block], got.at[i], send.at[i], recv.at[i], (at.j, to))
            for i, (block, to) in enumerate(
                ((self.far, self.one), (self.one, self.one), (self.two, self.two))
            )
        ]

    def send(self):
        self.copies[0].start()
        self.copies[1].start()

    def make(self, make, send):
        for p in (self.far, self.one, self.two, self.at.f):
            make(p)
            if send and p is self.one:
                self.send()

    def middle(self):
        self.copies[0].wait_recv()
        block = self.made[self.two].astype(F32) + self.got[0].astype(F32)
        self.made[self.two] = block.astype(BF)
        self.copies[2].start()

    def total(self):
        self.copies[1].wait_recv()
        self.copies[2].wait_recv()
        total = self.made[self.at.f].astype(F32) + self.got[1].astype(F32)
        return (total + self.got[2].astype(F32)).astype(BF)

    def finish(self):
        for copy in self.copies:
            copy.wait_send()


SMALL = 48
CHUNKS = 4


def opening(
    S, collective_id, tok, small, tokens, cotangent, fc1_weight, fc2_weight, qkv_weight,
    dense_weight,
):
    F, Q, L = 4, S // 2, tok * S
    D, ff = tokens.shape[1], fc1_weight.shape[1]
    rows_d, cols_up = D // F, ff // S
    w_ff = cols_up // F
    pairs = HEADS // S // 2
    wide = 3 * pairs * LANES
    dense_rows = HEAD * HEADS // (F * S)
    half = S // 2
    n_down, n_up = D // CHUNKS, cols_up // CHUNKS
    lead = {}
    at_row = 0
    for name, n in (
        ("gain", rows_d), ("bias", rows_d), ("qkv", 3 * rows_d), ("dense", rows_d),
        ("up", ff // F), ("down", rows_d),
    ):
        lead[name] = (at_row, n // 128)
        at_row += n // 128

    def kernel(*refs):
        refs = list(refs)
        take = lambda n: [refs.pop(0) for _ in range(n)]
        (small_in, tok_in, cot_in, up_in, down_in, qkv_in, dense_in) = take(7)
        (o_normed, o_out, o_gn, o_g, o_qkv, o_dense, o_alldown, o_allup, o_piece,
         o_vec, o_small) = take(11)
        at = Place(S, F)
        j, f = at.j, at.f
        x_own, g_own, n_own, up_own, down_own, dense_own, qkv_raw, qkv_own = take(8)
        normed, g, w_up, w_down, act, gp, slope, part_out, part_gn = take(9)
        small_all, pieces = take(2)
        load_sem, save_sem, s_small, r_small = take(4)
        copies = []

        def load(src, dst):
            copy = pltpu.make_async_copy(src, dst, load_sem.at[len(copies)])
            copies.append(copy)
            copy.start()
            return copy

        for p in range(F):
            load(up_in.at[:, pl.ds(pl.multiple_of((p * S + j) * w_ff, w_ff), w_ff)],
                 up_own.at[:, p * w_ff : (p + 1) * w_ff])
        load(tok_in, x_own)
        load(cot_in, g_own)
        load(down_in.at[pl.ds(pl.multiple_of(j * w_ff, w_ff), w_ff)], down_own)
        load(dense_in.at[pl.ds(pl.multiple_of(j * dense_rows, dense_rows), dense_rows)],
             dense_own)
        for i in range(3 * pairs):
            for which in range(2):
                block = (i % 3) * F * half + (2 * (i // 3) + which) * half + j // 2
                load(qkv_in.at[:, pl.ds(pl.multiple_of(block * LANES, LANES), LANES)],
                     qkv_raw.at[2 * i + which])

        gathers = [
            ShardGather(at, src, dst, *take(3))
            for src, dst in (
                (up_own, w_up), (down_own, w_down), (qkv_own, o_qkv), (dense_own, o_dense),
            )
        ]
        line_n = TokenGather(at, n_own, normed, *take(4))
        line_g = TokenGather(at, g_own, g, *take(4))
        reduce_down = [CornerReduce(at, i % 2, *take(4)) for i in range(CHUNKS)]
        reduce_up = [CornerReduce(at, i % 2, *take(4)) for i in range(CHUNKS)]
        lines = [
            TokenGather(at, pieces.at[i], o_alldown.at[i], *take(4)) for i in range(CHUNKS)
        ]
        lines.append(TokenGather(at, reduce_up[0].made.at[f], o_allup.at[0], *take(4)))
        at.greet(True, "line")
        smalls = []
        for k in range(1, F):
            to, of = lax.rem(f + k, F), lax.rem(f + F - k, F)
            smalls.append(
                (remote(small_in, small_all.at[f], s_small.at[k - 1], r_small.at[k - 1], (j, to)),
                 remote(small_in, small_all.at[of], s_small.at[k - 1], r_small.at[k - 1], (j, to)))
            )
        for copy, _ in smalls:
            copy.start()
        small_all[f] = small_in[...]
        for p in range(F):
            copies[p].wait()
        gathers[0].start()
        copies[F + 2].wait()
        gathers[1].start()
        copies[F + 3].wait()
        copies[F + 1].wait()
        line_g.start()

        def row_of(name):
            first, n = lead[name]
            return jnp.concatenate(
                [small_all[p, first + r : first + r + 1, :] for p in range(F) for r in range(n)],
                axis=1,
            )

        copies[F].wait()
        values = x_own[...].astype(F32)
        centre = jnp.mean(values, axis=-1, keepdims=True)
        values = values - centre
        inv_std = lax.rsqrt(jnp.mean(values * values, axis=-1, keepdims=True) + EPS)
        values = values * inv_std
        for _, arrival in smalls:
            arrival.wait_recv()
        n_own[...] = (values * row_of("gain") + row_of("bias")).astype(BF)
        line_n.start()

        for d in range(1, Q - 1):
            line_g.near(d)
            line_g.far(d)
            if d == 1:
                gathers[0].relay()
            line_n.near(d)
            line_n.far(d)
            if d == 1:
                gathers[1].relay()
                gathers[3].start()
        odd = lax.rem(j, 2) == 1
        lane = lax.broadcasted_iota(jnp.int32, (rows_d, LANES), 1)
        for copy in copies[F + 4 :]:
            copy.wait()
        for i in range(3 * pairs):
            first, second = qkv_raw[2 * i].astype(F32), qkv_raw[2 * i + 1].astype(F32)
            first = jnp.where(odd, pltpu.roll(first, HEAD, 1), first)
            second = jnp.where(odd, second, pltpu.roll(second, HEAD, 1))
            qkv_own[:, i * LANES : (i + 1) * LANES] = jnp.where(
                lane < HEAD, first, second
            ).astype(BF)
        line_g.far(Q - 1)
        gathers[3].relay()
        line_n.far(Q - 1)
        line_n.arrived()
        gathers[0].arrived()
        saves = []

        def save(src, dst):
            copy = pltpu.make_async_copy(src, dst, save_sem.at[len(saves)])
            saves.append(copy)
            copy.start()

        save(normed, o_normed)
        up_first = lead["up"][0]

        @pl.loop(0, F)
        def _(p):
            cols = pl.ds(pl.multiple_of(p * w_ff, w_ff), w_ff)
            u = jnp.concatenate(
                [
                    small_all[p, pl.ds(up_first + j * (w_ff // 128) + r, 1), :]
                    for r in range(w_ff // 128)
                ],
                axis=1,
            )
            for s in range(F):
                part = normed[:, :, s * rows_d : (s + 1) * rows_d].reshape(L, rows_d)
                u = u + dot(part, w_up[s, :, cols])
            square = u * u
            root = 0.7978845608028654
            t = jnp.tanh(root * (u + 0.044715 * (square * u)))
            act[:, cols] = ((0.5 * u) * (1.0 + t)).astype(BF)
            slope[:, cols] = 0.5 * (1.0 + t) + (0.5 * u) * (1.0 - t * t) * (
                root * (1.0 + 3 * 0.044715 * square)
            )

        line_g.arrived()
        save(g, o_g)
        ones = jnp.ones((EXTRA, L), BF)

        def make_down(c):
            cols = slice(c * n_down, (c + 1) * n_down)

            def make(p):
                block = act[:, pl.ds(pl.multiple_of(p * w_ff, w_ff), w_ff)]
                right = g[:, :, cols].reshape(L, n_down)
                reduce_down[c].made[p, 0:w_ff, :] = dot_tn(block, right).astype(BF)
                if c == 0:
                    mine = g[:, :, pl.ds(pl.multiple_of(p * rows_d, rows_d), rows_d)]
                    term = dot(ones, mine.reshape(L, rows_d))
                    reduce_down[c].made[p, w_ff:, :] = term.astype(BF)

            return make

        def make_up(c):
            cols = slice(c * n_up, (c + 1) * n_up)

            def make(p):
                block = normed[:, :, pl.ds(pl.multiple_of(p * rows_d, rows_d), rows_d)]
                made = dot_tn(block.reshape(L, rows_d), gp[:, cols])
                reduce_up[c].made[p, 0:rows_d, :] = made.astype(BF)
                if c == 0:
                    term = dot(ones, gp[:, pl.ds(pl.multiple_of(p * w_ff, w_ff), w_ff)])
                    reduce_up[c].made[p, rows_d:, :] = term.astype(BF)

            return make

        for c in range(CHUNKS):
            reduce_down[c].make(make_down(c), c < 2)
        gathers[1].arrived()

        @pl.loop(0, F)
        def _(p):
            cols = pl.ds(pl.multiple_of(p * w_ff, w_ff), w_ff)
            grad_act = dot_nt(g[...].reshape(L, D), w_down[p])
            gp[:, cols] = (grad_act * slope[:, cols]).astype(BF)


        def end_down(c):
            total = reduce_down[c].total()
            pieces[c] = total[0:w_ff, :]
            if c == 0:
                o_vec[...] = total[w_ff:, :]
            lines[c].start()

        def end_up(c):
            total = reduce_up[c].total()
            if c:
                o_piece[c - 1] = total
            else:
                reduce_up[0].made[f] = total
                lines[CHUNKS].start()

        def serve(c, d):
            lines[c].near(d)
            lines[c].far(d)

        def feed_out(i):
            cols = slice(i * rows_d, (i + 1) * rows_d)
            made = dot(act[:, 0:w_ff], w_down[0, :, cols])
            for p in range(1, F):
                made = made + dot(act[:, p * w_ff : (p + 1) * w_ff], w_down[p, :, cols])
            part_out[:, :, cols] = made.astype(BF).reshape(S, tok, rows_d)

        def feed_gn(i):
            made = dot_nt(gp[...], w_up[i])
            cols = slice(i * rows_d, (i + 1) * rows_d)
            part_gn[:, :, cols] = made.astype(BF).reshape(S, tok, rows_d)

        for c in (0, 1):
            reduce_down[c].middle()
        for c in (2, 3):
            reduce_down[c].send()
        for c in (0, 1):
            reduce_up[c].make(make_up(c), False)
        for c in (0, 1):
            end_down(c)
        for c in (2, 3):
            reduce_up[c].make(make_up(c), False)
        serve(0, 1)
        for c in (2, 3):
            reduce_down[c].middle()
        for c in (0, 1):
            reduce_up[c].send()
        serve(1, 1)
        feed_out(0)
        feed_out(1)
        for c in (2, 3):
            end_down(c)
        feed_out(2)
        serve(0, 2)
        for c in (0, 1):
            reduce_up[c].middle()
        for c in (2, 3):
            reduce_up[c].send()
        gathers[2].start()
        serve(1, 2)
        feed_out(3)
        save(part_out, o_out)
        serve(2, 1)
        for c in (0, 1):
            end_up(c)
        feed_gn(0)
        serve(3, 1)
        feed_gn(1)
        for d in range(3, Q):
            serve(0, d)
            serve(1, d)
        for c in (2, 3):
            reduce_up[c].middle()
        feed_gn(2)
        serve(2, 2)
        feed_gn(3)
        save(part_gn, o_gn)
        serve(3, 2)
        serve(CHUNKS, 1)
        gathers[2].relay()
        for c in (2, 3):
            end_up(c)
        for d in range(3, Q):
            serve(2, d)
            serve(3, d)
        for d in range(2, Q):
            serve(CHUNKS, d)
        o_small[...] = small_all[...]
        for copy, _ in smalls:
            copy.wait_send()
        for gather in gathers[2:]:
            gather.arrived()
        for line in lines:
            line.arrived()
        for item in [line_n, line_g] + lines + gathers + reduce_down + reduce_up:
            item.finish()
        for copy in saves:
            copy.wait()

    vmem = pl.BlockSpec(memory_space=pltpu.VMEM)
    anywhere = pl.BlockSpec(memory_space=pl.ANY)
    out = lambda shape, dtype=BF: jax.ShapeDtypeStruct(shape, dtype)
    scratch = [
        pltpu.VMEM(shape, dtype)
        for shape, dtype in (
            ((tok, D), BF), ((tok, D), BF), ((tok, D), BF), ((rows_d, cols_up), BF),
            ((w_ff, D), BF), ((dense_rows, D), BF), ((6 * pairs, rows_d, LANES), BF),
            ((rows_d, wide), BF),
            ((S, tok, D), BF), ((S, tok, D), BF), ((F, rows_d, cols_up), BF), ((F, w_ff, D), BF),
            ((L, cols_up), BF), ((L, cols_up), BF), ((L, cols_up), F32),
            ((S, tok, D), BF), ((S, tok, D), BF),
            ((F, SMALL, 128), F32), ((CHUNKS, w_ff, n_down), BF),
        )
    ]
    scratch += [
        pltpu.SemaphoreType.DMA((F + 4 + 6 * pairs,)), pltpu.SemaphoreType.DMA((6,)),
        pltpu.SemaphoreType.DMA((F - 1,)), pltpu.SemaphoreType.DMA((F - 1,)),
    ]
    for _ in range(4):
        scratch += ShardGather.scratch(F)
    for _ in range(2):
        scratch += TokenGather.scratch(S)
    for c in range(CHUNKS):
        scratch += CornerReduce.scratch(w_ff + (0 if c else EXTRA), n_down)
    for c in range(CHUNKS):
        scratch += CornerReduce.scratch(rows_d + (0 if c else EXTRA), n_up)
    for _ in range(CHUNKS + 1):
        scratch += TokenGather.scratch(S)
    return pl.pallas_call(
        kernel,
        out_shape=(
            out((S, tok, D)), out((S, tok, D)), out((S, tok, D)), out((S, tok, D)),
            out((F, rows_d, wide)), out((F, dense_rows, D)),
            out((CHUNKS, S, w_ff, n_down)), out((1, S, rows_d + EXTRA, n_up)),
            out((CHUNKS - 1, rows_d, n_up)),
            out((EXTRA, n_down)), out((F, SMALL, 128), F32),
        ),
        in_specs=[vmem] + [anywhere] * 6,
        out_specs=(anywhere,) * 8 + (vmem,) * 3,
        scratch_shapes=scratch,
        compiler_params=pltpu.CompilerParams(
            collective_id=collective_id, has_side_effects=True, vmem_limit_bytes=67_000_000
        ),
        cost_estimate=pl.CostEstimate(
            flops=8 * L * D * cols_up, bytes_accessed=200 * L * D, transcendentals=L * cols_up
        ),
    )(small, tokens, cotangent, fc1_weight, fc2_weight, qkv_weight, dense_weight)


def half_lanes(first, second, odd):
    lane = lax.broadcasted_iota(jnp.int32, first.shape, 1)
    if odd:
        first = pltpu.roll(first, HEAD, 1)
    else:
        second = pltpu.roll(second, HEAD, 1)
    return jnp.where(lane < HEAD, first, second)


def pick_qkv(weight, j, F, S, pairs):
    rows = weight.shape[0]
    per_shard = S // 2

    def kernel(j_ref, first, second, out):
        a, b = first[...].astype(F32), second[...].astype(F32)

        @pl.when(j_ref[0] % 2 == 0)
        def _():
            out[...] = half_lanes(a, b, 0).astype(BF)

        @pl.when(j_ref[0] % 2 == 1)
        def _():
            out[...] = half_lanes(a, b, 1).astype(BF)

    def column(which):
        return lambda i, j_ref: (
            0, (i % 3) * F * per_shard + (2 * (i // 3) + which) * per_shard + j_ref[0] // 2
        )

    return pl.pallas_call(
        kernel,
        grid_spec=pltpu.PrefetchScalarGridSpec(
            num_scalar_prefetch=1,
            grid=(3 * pairs,),
            in_specs=[pl.BlockSpec((rows, LANES), column(0)), pl.BlockSpec((rows, LANES), column(1))],
            out_specs=pl.BlockSpec((rows, LANES), lambda i, j_ref: (0, i)),
        ),
        out_shape=jax.ShapeDtypeStruct((rows, 3 * pairs * LANES), BF),
    )(j[None].astype(jnp.int32), weight, weight)


def pick_up(weight, j, F, S):
    rows, ff = weight.shape
    w = ff // (F * S)
    if w % LANES:
        split = weight.reshape(rows, F, S, w)
        return lax.dynamic_index_in_dim(split, j, 2, keepdims=False).reshape(rows, F * w)

    def kernel(j_ref, src, out):
        out[...] = src[...]

    return pl.pallas_call(
        kernel,
        grid_spec=pltpu.PrefetchScalarGridSpec(
            num_scalar_prefetch=1,
            grid=(F,),
            in_specs=[pl.BlockSpec((rows, w), lambda i, j_ref: (0, i * S + j_ref[0]))],
            out_specs=pl.BlockSpec((rows, w), lambda i, j_ref: (0, i)),
        ),
        out_shape=jax.ShapeDtypeStruct((rows, F * w), BF),
    )(j[None].astype(jnp.int32), weight)


def unpack_qkv(gathered, rows, S):
    width = S * HEAD
    pairs = len(gathered)

    def kernel(*refs):
        out = refs[pairs]
        for p in range(pairs):

            @pl.when(pl.program_id(0) % pairs == p)
            def _():
                src = refs[p]
                for half in range(2):
                    for z in range(S // 2):
                        a, b = src[2 * z].astype(F32), src[2 * z + 1].astype(F32)
                        at = half * width + z * LANES
                        out[:, at : at + LANES] = half_lanes(a, b, half)

    return pl.pallas_call(
        kernel,
        grid=(3 * pairs,),
        in_specs=[pl.BlockSpec((S, rows, LANES), lambda i: (0, 0, i // pairs))] * pairs,
        out_specs=pl.BlockSpec((rows, 2 * width), lambda i: (0, i)),
        out_shape=jax.ShapeDtypeStruct((rows, HEADS * HEAD * 3), F32),
    )(*gathered)


def unpack_groups(*stacks, rows):
    S, w = stacks[0].shape[1], stacks[0].shape[3]
    groups = [stack.shape[0] for stack in stacks]
    starts = [sum(groups[:i]) for i in range(len(groups))]

    def kernel(*refs):
        i = pl.program_id(0)
        for src, start, count in zip(refs, starts, groups):

            @pl.when((i >= start) & (i < start + count))
            def _():
                for s in range(S):
                    refs[-1][:, s * w : (s + 1) * w] = src[0, s].astype(F32)

    def block(start, count):
        return pl.BlockSpec(
            (1, S, rows, w), lambda i: (jnp.clip(i - start, 0, count - 1), 0, 0, 0)
        )

    return pl.pallas_call(
        kernel,
        grid=(sum(groups),),
        in_specs=[block(start, count) for start, count in zip(starts, groups)],
        out_specs=pl.BlockSpec((rows, S * w), lambda i: (0, i)),
        out_shape=jax.ShapeDtypeStruct((rows, sum(groups) * S * w), F32),
    )(*stacks)


def unpack_cols(gathered, rows, F):
    S, _, cols = gathered.shape
    w = cols // F
    if w % LANES:
        split = gathered[:, :rows].reshape(S, rows, F, w)
        return split.transpose(1, 2, 0, 3).reshape(rows, F * S * w).astype(F32)

    def kernel(src, out):
        for s in range(S):
            out[:, s * w : (s + 1) * w] = src[s].astype(F32)

    return pl.pallas_call(
        kernel,
        grid=(F,),
        in_specs=[pl.BlockSpec((S, rows, w), lambda i: (0, 0, i))],
        out_specs=pl.BlockSpec((rows, S * w), lambda i: (0, i)),
        out_shape=jax.ShapeDtypeStruct((rows, F * S * w), F32),
    )(gathered)


def unpack_chunks(gathered):
    C, S, rows, n = gathered.shape

    def kernel(src, out):
        for c in range(C):
            out[:, c * n : (c + 1) * n] = src[c, 0].astype(F32)

    return pl.pallas_call(
        kernel,
        grid=(S,),
        in_specs=[pl.BlockSpec((C, 1, rows, n), lambda i: (0, i, 0, 0))],
        out_specs=pl.BlockSpec((rows, C * n), lambda i: (i, 0)),
        out_shape=jax.ShapeDtypeStruct((S * rows, C * n), F32),
    )(gathered)


def unpack_rows(gathered, rows):
    S, _, n = gathered.shape

    def kernel(src, out):
        out[...] = src[0].astype(F32)

    return pl.pallas_call(
        kernel,
        grid=(S,),
        in_specs=[pl.BlockSpec((1, rows, n), lambda i: (i, 0, 0))],
        out_specs=pl.BlockSpec((rows, n), lambda i: (i, 0)),
        out_shape=jax.ShapeDtypeStruct((S * rows, n), F32),
    )(gathered)


def body(
    tokens,
    ln_gain,
    ln_bias,
    qkv_weight,
    qkv_bias,
    dense_weight,
    dense_bias,
    fc1_weight,
    fc1_bias,
    fc2_weight,
    fc2_bias,
    segments,
    positions,
    cotangent,
):
    S, F = lax.axis_size("seq"), lax.axis_size("fsdp")
    j, f = lax.axis_index("seq"), lax.axis_index("fsdp")
    tok, D = tokens.shape[1], tokens.shape[2]
    length = tok * S
    rows_d = D // F
    ff = fc1_weight.shape[1]
    cols_up = ff // S
    block_up = cols_up // F
    hp = HEADS // S
    pairs = hp // 2
    per_shard = HEADS // F
    spread = per_shard % S == 0
    slots = per_shard // S if spread else 0

    qkv_width = pairs * 3 * LANES

    def heads_of(array, lead):
        shape = array.shape
        if spread:
            split = array.reshape(shape[:lead] + (F, S, slots) + shape[lead + 1 :])
            mine = lax.dynamic_index_in_dim(split, j, lead + 1, keepdims=False)
            return mine.reshape(shape[:lead] + (hp,) + shape[lead + 1 :])
        return lax.dynamic_slice_in_dim(array, j * hp, hp, lead)

    def qkv_cols(array):
        n = array.shape[0]
        mine = heads_of(array.reshape(n, 3, HEADS, HEAD), 2)
        return mine.reshape(n, 3, pairs, 2, HEAD).transpose(0, 2, 1, 3, 4).reshape(n, -1)

    def from_qkv_cols(gathered):
        n = gathered.shape[1]
        split = gathered.reshape(S, n, pairs, 3, 2, HEAD).transpose(0, 1, 3, 2, 4, 5)
        split = split.reshape(S, n, 3, hp, HEAD)
        if spread:
            moved = jnp.moveaxis(split.reshape(S, n, 3, F, slots, HEAD), 0, 3)
        else:
            moved = jnp.moveaxis(split, 0, 2)
        return moved.reshape(n, -1)

    inputs = tokens[0].astype(F32)
    centre = jnp.mean(inputs, axis=-1, keepdims=True)
    variance = jnp.mean((inputs - centre) ** 2, axis=-1, keepdims=True)
    inv_std = lax.rsqrt(variance + EPS)
    standard = (inputs - centre) * inv_std
    upstream_own = cotangent[0]
    seg_row = segments[0]
    block_dense = slots * HEAD

    def rider(values, width):
        return jnp.pad(values[:, None], ((0, 0), (0, EXTRA - 1), (0, width - values.shape[1])))

    def split_small(small):
        cuts, at = [], 0
        for piece in smalls:
            cuts.append(small[:, at : at + piece.shape[0]].reshape(-1).astype(F32))
            at += piece.shape[0]
        return cuts

    smalls = (ln_gain, ln_bias, qkv_bias, dense_bias, fc1_bias, fc2_bias)
    fused = F == 4 and spread and slots == 1 and block_up % 128 == 0
    if fused:
        rows = [piece.astype(F32).reshape(-1, 128) for piece in smalls]
        small = jnp.concatenate(rows, axis=0)
        small = jnp.pad(small, ((0, SMALL - small.shape[0]), (0, 0)))
        (normed, feed_out, feed_gn, upstream, w_qkv, w_dense, all_down, first_up, rest_up,
         out_mine, small) = opening(
            S, 1, tok, small, tokens[0], upstream_own, fc1_weight, fc2_weight, qkv_weight,
            dense_weight,
        )
        gain, shift, b_qkv, b_dense, b_up, b_down = split_small(small.reshape(F, -1))
        w_dense = [w_dense]
        out_mine = out_mine[0, :rows_d].astype(F32)
    else:
        small = jnp.concatenate(smalls)
        small = lax.all_gather(small, "fsdp", axis=0)
        gain, shift, b_qkv, b_dense, b_up, b_down = split_small(small)

        normed_own = (standard * gain + shift).astype(BF)

        up_own = pick_up(fc1_weight, j, F, S)
        down_own = lax.dynamic_slice_in_dim(fc2_weight, j * block_up, block_up, 0)
        if spread and slots == 1:
            qkv_own = pick_qkv(qkv_weight, j, F, S, pairs)
        else:
            qkv_own = qkv_cols(qkv_weight)
        w_up, w_down, normed, upstream = exchange(
            S, F, 1, shards=(up_own, down_own), tokens=(normed_own, upstream_own)
        )
        w_up, w_down = w_up.reshape(D, cols_up), w_down.reshape(cols_up, D)
        normed, upstream = normed.reshape(length, D), upstream.reshape(length, D)

        bias_up = lax.dynamic_index_in_dim(b_up.reshape(F, S, block_up), j, 1, keepdims=False)
        bias_up = bias_up.reshape(-1)

        pre_act = dot(normed, w_up) + bias_up
        activated = gelu_tanh(pre_act).astype(BF)
        out_term = jnp.sum(upstream.astype(F32), axis=0).reshape(F, rows_d)
        piece_down, out_mine = exchange(
            S, F, 2, grads=((activated, upstream, rider(out_term, D)),), split=True
        )
        out_mine = out_mine[0, :rows_d].astype(F32)

        grad_act = dot_nt(upstream, w_down)
        grad_pre = jax.vjp(gelu_tanh, pre_act)[1](grad_act)[0].astype(BF)
        up_term = jnp.sum(grad_pre.astype(F32), axis=0).reshape(F, block_up)
        shards = (qkv_own,)
        if spread:
            shards += (lax.dynamic_slice_in_dim(dense_weight, j * block_dense, block_dense, 0),)
        piece_up, w_qkv, *w_dense, all_down = exchange(
            S, F, 3, grads=((normed, grad_pre, rider(up_term, cols_up)),), shards=shards,
            tokens=(piece_down,),
        )
    bias_qkv = qkv_cols(b_qkv[None])[0]
    w_qkv = w_qkv.reshape(D, qkv_width)
    if spread:
        w_dense = w_dense[0].reshape(hp * HEAD, D)
    else:
        w_dense = lax.dynamic_slice_in_dim(
            lax.all_gather(dense_weight, "fsdp", axis=0, tiled=True), j * hp * HEAD, hp * HEAD, 0
        )
    if fused:
        branches, grad_normed, ln_mine, late_up, *gathered = attend_and_close(
            S, F, 5, tok, normed, upstream, feed_out, feed_gn, w_dense, w_qkv, rest_up,
            angle_tables(seg_row),
            seg_row[:, None], seg_row[None, :], bias_qkv[None], standard,
        )
    else:
        all_up = lax.all_gather(piece_up, "seq", axis=0)
        projected = dot(normed, w_qkv) + bias_qkv
        grad_att = dot_nt(upstream, w_dense).astype(BF)
        attended, grad_mixed = attention(projected, grad_att, angle_tables(seg_row), seg_row)
        qkv_term = jnp.sum(grad_mixed.astype(F32), axis=0)
        qkv_term = jnp.broadcast_to(qkv_term[None], (F, qkv_width))
        branches, grad_normed, ln_mine, *gathered = closing(
            S, F, 5, tok, normed, upstream, grad_mixed, attended, activated, grad_pre,
            w_dense, w_down, w_qkv, w_up, rider(qkv_term, qkv_width), standard, spread,
        )
    all_qkv = gathered[:pairs]
    result = (inputs + branches + (b_dense + b_down)).astype(BF)
    scaled = grad_normed * gain
    grad_inputs = upstream_own.astype(F32) + inv_std * (
        scaled
        - jnp.mean(scaled, axis=-1, keepdims=True)
        - standard * jnp.mean(scaled * standard, axis=-1, keepdims=True)
    )

    if fused:
        grad_down = unpack_chunks(all_down)
        grad_up = unpack_groups(first_up, late_up, rows=rows_d)
        up_mine = first_up[0, :, rows_d].astype(F32).reshape(-1)
    else:
        grad_down = unpack_rows(all_down, block_up)
        grad_up = unpack_cols(all_up, rows_d, F)
        up_mine = all_up[:, rows_d, :block_up].astype(F32).reshape(-1)
    qkv_sums = jnp.concatenate([piece[:, rows_d] for piece in all_qkv], axis=1)
    qkv_sums = from_qkv_cols(qkv_sums[:, None]).reshape(F, -1)
    qkv_mine = lax.dynamic_index_in_dim(qkv_sums, f, 0, keepdims=False).astype(F32)
    if spread and slots == 1:
        grad_qkv = unpack_qkv(all_qkv, rows_d, S)
    else:
        joined = jnp.concatenate([piece[:, :rows_d] for piece in all_qkv], axis=2)
        grad_qkv = from_qkv_cols(joined).astype(F32)
    if spread:
        grad_dense = gathered[pairs].reshape(rows_d, D).astype(F32)
    else:
        part = lax.all_gather(dot_tn(attended, upstream).astype(BF), "seq", axis=0, tiled=True)
        grad_dense = lax.psum_scatter(part, "fsdp", scatter_dimension=0, tiled=True).astype(F32)
    return (
        result[None],
        grad_inputs[None],
        ln_mine[0],
        ln_mine[1],
        grad_qkv,
        qkv_mine,
        grad_dense,
        out_mine,
        grad_up,
        up_mine,
        grad_down,
        out_mine,
    )


def solution(mesh):
    row, mat = P("fsdp"), P("fsdp", None)
    act = P("fsdp", "seq", None)
    return jax.shard_map(
        body,
        mesh=mesh,
        in_specs=(
            act, row, row, mat, row, mat, row, mat, row, mat, row, mat, P("fsdp", "seq"), act,
        ),
        out_specs=(act, act, row, row, mat, row, mat, row, mat, row, mat, row),
        check_vma=False,
    )
```

```python
import functools

import jax
import jax.numpy as jnp
from jax import lax
from jax.experimental import pallas as pl
from jax.experimental.pallas import tpu as pltpu
from jax.sharding import PartitionSpec as P


HEADS = 32
HEAD = 64
ROT = 32
EPS = 1e-05
DOC_SHIFT = 1023
LANES = 2 * HEAD
BF = jnp.bfloat16
F32 = jnp.float32


def dot(left, right):
    return lax.dot_general(left, right, (((1,), (0,)), ((), ())), preferred_element_type=F32)


def dot_nt(left, right):
    return lax.dot_general(left, right, (((1,), (1,)), ((), ())), preferred_element_type=F32)


def dot_tn(left, right):
    return lax.dot_general(left, right, (((0,), (0,)), ((), ())), preferred_element_type=F32)


def columns(ref, cols):
    if len(ref.shape) == 2:
        return ref[:, cols]
    block = ref[:, :, cols]
    return block.reshape(-1, block.shape[-1])


def gelu_tanh(values_in):
    return jax.nn.gelu(values_in, approximate=True)


def turn(values, cos, sin_low, sin_high):
    half = ROT // 2
    return (
        values * cos
        - pltpu.roll(values, LANES - half, 1) * sin_low
        + pltpu.roll(values, half, 1) * sin_high
    )


def attention_kernel(
    rows, proj, grad_out, cos, sin_low, sin_high, seg_col, seg_row,
    out, grad_proj, qs, ks, vs, dk, dv, pause=None,
):
    length = proj.shape[0]
    blocks = length // rows
    scale = HEAD**-0.5
    for i in range(blocks):
        r = slice(i * rows, (i + 1) * rows)
        c, lo, hi = cos[r, :], sin_low[r, :], sin_high[r, :]
        qs[r, :] = turn(proj[r, 0:LANES], c, lo, hi).astype(BF) * jnp.asarray(scale, BF)
        ks[r, :] = turn(proj[r, LANES : 2 * LANES], c, lo, hi).astype(BF)
        vs[r, :] = proj[r, 2 * LANES : 3 * LANES].astype(BF)
    lane = lax.broadcasted_iota(jnp.int32, (rows, LANES), 1)
    first = lane < HEAD
    zero = jnp.zeros((rows, LANES), BF)
    for i in reversed(range(blocks)):
        r = slice(i * rows, (i + 1) * rows)
        n = (i + 1) * rows
        place_q = i * rows + lax.broadcasted_iota(jnp.int32, (rows, n), 0)
        place_k = lax.broadcasted_iota(jnp.int32, (rows, n), 1)
        allowed = (place_k <= place_q) & (seg_col[r, :] == seg_row[:, 0:n])
        q2, g2 = qs[r, :], grad_out[r, :]
        k, v = ks[0:n, :], vs[0:n, :]
        o_parts, dq_parts = [], []
        for h in range(2):
            mine = first if h == 0 else ~first
            q = jnp.where(mine, q2, zero)
            g = jnp.where(mine, g2, zero)
            s = jnp.where(allowed, dot_nt(q, k), -1e30)
            e = jnp.exp(s - jnp.max(s, axis=-1, keepdims=True))
            p = e * (1.0 / jnp.sum(e, axis=-1, keepdims=True))
            pb = p.astype(BF)
            o_parts.append(dot(pb, v))
            dp = dot_nt(g, v)
            inner = jnp.sum(p * dp, axis=-1, keepdims=True)
            ds = (p * (dp - inner)).astype(BF)
            dq_parts.append(dot(ds, k))
            dk_new, dv_new = dot_tn(ds, q), dot_tn(pb, g)
            if i == blocks - 1 and h == 0:
                dk[...] = dk_new
                dv[...] = dv_new
            else:
                dk[0:n, :] += dk_new
                dv[0:n, :] += dv_new
        out[r, :] = jnp.where(first, o_parts[0], o_parts[1]).astype(BF)
        dq = (jnp.where(first, dq_parts[0], dq_parts[1]) * scale).astype(BF).astype(F32)
        c, lo, hi = cos[r, :], sin_low[r, :], sin_high[r, :]
        grad_proj[r, 0:LANES] = turn(dq, c, -lo, -hi).astype(BF)
        if pause is not None:
            pause(i)
    for i in range(blocks):
        r = slice(i * rows, (i + 1) * rows)
        c, lo, hi = cos[r, :], sin_low[r, :], sin_high[r, :]
        grad_k = dk[r, :].astype(BF).astype(F32)
        grad_proj[r, LANES : 2 * LANES] = turn(grad_k, c, -lo, -hi).astype(BF)
        grad_proj[r, 2 * LANES : 3 * LANES] = dv[r, :].astype(BF)


def attention(proj, grad_att, tables, segments):
    length = proj.shape[0]
    pairs = grad_att.shape[1] // LANES
    rows = 256
    whole = lambda shape: pl.BlockSpec(shape, lambda p: (0, 0))
    return pl.pallas_call(
        functools.partial(attention_kernel, rows),
        grid=(pairs,),
        out_shape=(
            jax.ShapeDtypeStruct((length, pairs * LANES), BF),
            jax.ShapeDtypeStruct((length, 3 * pairs * LANES), BF),
        ),
        in_specs=[
            pl.BlockSpec((length, 3 * LANES), lambda p: (0, p)),
            pl.BlockSpec((length, LANES), lambda p: (0, p)),
            whole((length, LANES)),
            whole((length, LANES)),
            whole((length, LANES)),
            whole((length, 1)),
            whole((1, length)),
        ],
        out_specs=(
            pl.BlockSpec((length, LANES), lambda p: (0, p)),
            pl.BlockSpec((length, 3 * LANES), lambda p: (0, p)),
        ),
        scratch_shapes=[pltpu.VMEM((length, LANES), BF)] * 3
        + [pltpu.VMEM((length, LANES), F32)] * 2,
        cost_estimate=pl.CostEstimate(
            flops=14 * pairs * length * length * LANES,
            bytes_accessed=pairs * length * LANES * 24,
            transcendentals=pairs * length * length,
        ),
    )(proj, grad_att, *tables, segments[:, None], segments[None, :])


def angle_tables(seg_row):
    length = seg_row.shape[0]
    position = jnp.arange(length, dtype=jnp.int32) + jnp.where(seg_row > 0, DOC_SHIFT, 0)
    inverse = 1.0 / 10000.0 ** (jnp.arange(0, ROT, 2, dtype=F32) / ROT)
    inverse = jnp.tile(inverse, LANES // (ROT // 2))
    angles = position.astype(F32)[:, None] * inverse[None, :]
    cosine, sine = jnp.cos(angles), jnp.sin(angles)
    lane = jnp.arange(LANES)[None, :] % HEAD
    low = lane < ROT // 2
    return (
        jnp.where(lane < ROT, cosine, 1.0),
        jnp.where(low, sine, 0.0),
        jnp.where((lane < ROT) & ~low, sine, 0.0),
    )


MESH = pl.DeviceIdType.MESH


def remote(src, dst, send, recv, device):
    return pltpu.make_async_remote_copy(
        src_ref=src, dst_ref=dst, send_sem=send, recv_sem=recv, device_id=device,
        device_id_type=MESH,
    )


class Place:
    def __init__(self, S, F):
        self.S, self.F, self.Q = S, F, S // 2
        self.j, self.f = lax.axis_index("seq"), lax.axis_index("fsdp")
        self.q, self.c = self.j // 2, lax.rem(self.j, 2)
        self.partner = 2 * self.q + 1 - self.c
        self.low = 1 - self.q // (self.Q // 2)
        self.side = 2 * (2 * self.low - 1)
        self.end = self.low * self.q + (1 - self.low) * (self.Q - 1 - self.q)

    def greet(self, over_fsdp, over_seq):
        barrier = pltpu.get_barrier_semaphore()

        def signal(j, f):
            pl.semaphore_signal(barrier, inc=1, device_id=(j, f), device_id_type=MESH)

        count = 0
        if over_fsdp:
            for k in range(1, self.F):
                signal(self.j, lax.rem(self.f + k, self.F))
            count += self.F - 1
        if over_seq == "all":
            for k in range(1, self.S):
                signal(lax.rem(self.j + k, self.S), self.f)
            count += self.S - 1
        elif over_seq == "line":
            signal(self.partner, self.f)

            @pl.when(self.q > 0)
            def _():
                signal(self.j - 2, self.f)

            @pl.when(self.q < self.Q - 1)
            def _():
                signal(self.j + 2, self.f)

            count += 1 + (self.q + self.Q - 1) // self.Q + (2 * self.Q - 2 - self.q) // self.Q
        pl.semaphore_wait(barrier, count)


class ShardGather:
    @staticmethod
    def scratch(F):
        n = 6 if F == 4 else F - 1
        return [pltpu.SemaphoreType.DMA((n,)), pltpu.SemaphoreType.DMA((n,)),
                pltpu.SemaphoreType.DMA]

    def __init__(self, at, src, dst, send, recv, local):
        self.at, self.src, self.dst = at, src, dst
        f, j = at.f, at.j
        self.own = pltpu.make_async_copy(src, dst.at[f], local)
        self.first, self.later, self.arrivals = [], [], []
        if at.F == 4:
            nx = f + 1 - 2 * lax.rem(f, 2)
            ny = lax.rem(f + 2, 4)
            nd = lax.rem(nx + 2, 4)
            half = src.shape[0] // 2
            a, b = pl.ds(0, half), pl.ds(half, half)
            table = ((nx, a), (nx, b), (ny, a), (ny, b))
            for i, (to, rows) in enumerate(table):
                self.first.append(
                    remote(src.at[rows], dst.at[f, rows], send.at[i], recv.at[i], (j, to))
                )
                self.arrivals.append(
                    remote(src.at[rows], dst.at[to, rows], send.at[i], recv.at[i], (j, to))
                )
            for i, (of, rows, to) in ((4, (nx, a, ny)), (5, (ny, b, nx))):
                self.later.append(
                    remote(dst.at[of, rows], dst.at[of, rows], send.at[i], recv.at[i], (j, to))
                )
                self.arrivals.append(
                    remote(dst.at[nd, rows], dst.at[nd, rows], send.at[i], recv.at[i], (j, to))
                )
        else:
            for k in range(1, at.F):
                to, of = lax.rem(f + k, at.F), lax.rem(f + at.F - k, at.F)
                self.first.append(
                    remote(src, dst.at[f], send.at[k - 1], recv.at[k - 1], (j, to))
                )
                self.arrivals.append(
                    remote(src, dst.at[of], send.at[k - 1], recv.at[k - 1], (j, to))
                )

    def start(self):
        self.own.start()
        for copy in self.first:
            copy.start()

    def relay(self):
        if self.later:
            self.arrivals[0].wait_recv()
            self.later[0].start()
            self.arrivals[3].wait_recv()
            self.later[1].start()

    def arrived(self):
        for i, copy in enumerate(self.arrivals):
            if not (self.later and i in (0, 3)):
                copy.wait_recv()
        self.own.wait()

    def finish(self):
        for copy in self.first + self.later:
            copy.wait_send()


class TokenGather:
    @staticmethod
    def scratch(S):
        Q = S // 2
        return [pltpu.SemaphoreType.DMA((2 * Q,)), pltpu.SemaphoreType.DMA((2 * Q,)),
                pltpu.SemaphoreType.DMA((S,)), pltpu.SemaphoreType.DMA]

    def __init__(self, at, src, dst, send, share, recv, local, rows=None):
        self.at, self.src, self.dst, self.rows = at, src, dst, rows
        self.send, self.share, self.recv = send, share, recv
        self.own = pltpu.make_async_copy(src, self.place(at.j), local)

    def place(self, slot):
        return self.dst.at[slot] if self.rows is None else self.dst.at[slot, self.rows]

    def onward(self, slot, source, i, by):
        to = self.place(slot)
        return remote(
            source, to, self.send.at[i], self.recv.at[slot], (self.at.j + by, self.at.f)
        )

    def given(self, slot, source, i):
        to = self.place(slot)
        return remote(
            source, to, self.share.at[i], self.recv.at[slot], (self.at.partner, self.at.f)
        )

    def own_copies(self):
        at, j = self.at, self.at.j
        return (
            self.onward(j, self.src, 0, at.side), self.onward(j, self.src, at.Q, -at.side),
            self.given(j, self.src, 0),
        )

    def start(self):
        self.own.start()
        far, near, part = self.own_copies()
        far.start()

        @pl.when(self.at.end > 0)
        def _():
            near.start()

        part.start()

    def from_near(self, d):
        at = self.at
        slot = at.j - at.side * d
        here = self.place(slot)
        return self.onward(slot, here, d, at.side), self.given(slot, here, d)

    def from_far(self, d):
        at = self.at
        slot = at.j + at.side * d
        here = self.place(slot)
        return self.onward(slot, here, at.Q + d, -at.side), self.given(slot, here, at.Q + d)

    def near(self, d):
        if d > self.at.Q // 2 - 1:
            return

        @pl.when(self.at.end >= d)
        def _():
            onward, part = self.from_near(d)
            onward.wait_recv()
            onward.start()
            part.start()

    def far(self, d):
        @pl.when(self.at.end + d <= self.at.Q - 1)
        def _():
            onward, part = self.from_far(d)
            part.wait_recv()

            @pl.when(self.at.end > 0)
            def _():
                onward.start()

            part.start()

    def arrived(self):
        for q in range(self.at.Q):
            slot = 2 * q + 1 - self.at.c
            self.given(slot, self.place(slot), 0).wait_recv()
        self.own.wait()

    def finish(self):
        at, Q = self.at, self.at.Q
        far, near, part = self.own_copies()
        far.wait_send()

        @pl.when(at.end > 0)
        def _():
            near.wait_send()

        part.wait_send()
        for d in range(1, Q):
            if d <= Q // 2 - 1:

                @pl.when(at.end >= d)
                def _():
                    onward, part = self.from_near(d)
                    onward.wait_send()
                    part.wait_send()

            @pl.when(at.end + d <= Q - 1)
            def _():
                onward, part = self.from_far(d)

                @pl.when(at.end > 0)
                def _():
                    onward.wait_send()

                part.wait_send()


class GradReduce:
    @staticmethod
    def scratch(F, rows, n):
        return [pltpu.VMEM((F, rows, n), BF), pltpu.VMEM((F - 1, rows, n), BF),
                pltpu.SemaphoreType.DMA((F - 1,)), pltpu.SemaphoreType.DMA((F - 1,))]

    def __init__(self, at, left, right, extra, made, got, send, recv):
        self.at, self.left, self.right, self.extra = at, left, right, extra
        self.made, self.got, self.send, self.recv = made, got, send, recv
        self.n = right.shape[-1]
        self.rows = left.shape[-1] // at.F
        self.tile = next(t for t in (512, 384, 256, 128) if self.n % t == 0)

    def copy(self, k):
        at = self.at
        to = lax.rem(at.f + k, at.F)
        return remote(
            self.made.at[to], self.got.at[k - 1], self.send.at[k - 1], self.recv.at[k - 1],
            (at.j, to),
        )

    def start(self):
        at, rows = self.at, self.rows
        aligned = rows % 128 == 0
        for t in range(0, self.n, self.tile) if not aligned else ():
            cols = slice(t, t + self.tile)
            full = dot_tn(self.left[...], columns(self.right, cols)).astype(BF)
            for p in range(at.F):
                self.made[p, 0:rows, cols] = full[p * rows : (p + 1) * rows, :]
        for k in list(range(1, at.F)) + [0]:
            p = lax.rem(at.f + k, at.F)
            if aligned:
                block = columns(self.left, pl.ds(pl.multiple_of(p * rows, 128), rows))
                for t in range(0, self.n, self.tile):
                    cols = slice(t, t + self.tile)
                    made = dot_tn(block, columns(self.right, cols))
                    self.made[p, 0:rows, cols] = made.astype(BF)
            if callable(self.extra):
                self.made[p, rows:, :] = self.extra()
            elif self.extra is not None:
                self.made[p, rows : rows + self.extra.shape[1], :] = self.extra[p].astype(BF)
            if k:
                self.copy(k).start()

    def finish(self, store):
        at = self.at
        for k in range(1, at.F):
            self.copy(k).wait_recv()
        for t in range(0, self.n, self.tile):
            cols = slice(t, t + self.tile)
            total = self.made[at.f, :, cols].astype(F32)
            for k in range(1, at.F):
                total += self.got[k - 1, :, cols].astype(F32)
            store(t, self.tile, total.astype(BF))
        for k in range(1, at.F):
            self.copy(k).wait_send()


EXTRA = 16


def exchange(S, F, collective_id, grads=(), shards=(), tokens=(), split=False):
    operands, in_specs = [], []
    vmem = pl.BlockSpec(memory_space=pltpu.VMEM)
    outs, out_specs, scratch = [], [], []
    shapes = []
    for left, right, extra in grads:
        rows, n = left.shape[1] // F + (0 if extra is None else EXTRA), right.shape[1]
        operands += [left, right] + ([] if extra is None else [extra])
        scratch += GradReduce.scratch(F, rows, n)
        shapes.append((rows, n))
        if split:
            outs.append(jax.ShapeDtypeStruct((rows - EXTRA, n), BF))
            outs.append(jax.ShapeDtypeStruct((EXTRA, n), BF))
        else:
            outs.append(jax.ShapeDtypeStruct((rows, n), BF))
    out_specs += [vmem] * len(outs)
    for array in shards:
        operands.append(array)
        outs.append(jax.ShapeDtypeStruct((F,) + array.shape, BF))
        out_specs.append(pl.BlockSpec(memory_space=pl.ANY))
        scratch += ShardGather.scratch(F)
    for array in tokens:
        operands.append(array)
        outs.append(jax.ShapeDtypeStruct((S,) + array.shape, BF))
        out_specs.append(pl.BlockSpec(memory_space=pl.ANY))
        scratch += TokenGather.scratch(S)
    in_specs = [vmem] * len(operands)
    n_in, n_out = len(operands), len(outs)

    def kernel(*refs):
        ins, results, rest = list(refs[:n_in]), list(refs[n_in : n_in + n_out]), list(
            refs[n_in + n_out :]
        )
        take = lambda items, n: [items.pop(0) for _ in range(n)]
        at = Place(S, F)
        jobs, stores = [], []
        for (_, _, extra), (rows, n) in zip(grads, shapes):
            left, right = take(ins, 2)
            extra_ref = None if extra is None else take(ins, 1)[0]
            jobs.append(GradReduce(at, left, right, extra_ref, *take(rest, 4)))
            target = take(results, 1)[0]
            rider_ref = take(results, 1)[0] if split else None

            def store(t, width, value, target=target, rows=rows, rider_ref=rider_ref):
                if split:
                    target[:, t : t + width] = value[: rows - EXTRA]
                    rider_ref[:, t : t + width] = value[rows - EXTRA :]
                else:
                    target[:, t : t + width] = value

            stores.append(store)
        spreads = [
            ShardGather(at, take(ins, 1)[0], take(results, 1)[0], *take(rest, 3)) for _ in shards
        ]
        lines = [
            TokenGather(at, take(ins, 1)[0], take(results, 1)[0], *take(rest, 4)) for _ in tokens
        ]
        at.greet(bool(jobs or spreads), "line" if lines else "")
        for item in lines + spreads:
            item.start()
        for job in jobs:
            job.start()
        waiting = list(spreads)
        for d in range(1, at.Q) if lines else ():
            for item in lines:
                item.near(d)
                item.far(d)
            if waiting:
                waiting.pop(0).relay()
        for item in waiting:
            item.relay()
        for job, store in zip(jobs, stores):
            job.finish(store)
        for item in spreads + lines:
            item.arrived()
            item.finish()

    flops = sum(2 * l.shape[0] * l.shape[1] * r.shape[1] for l, r, _ in grads)
    moved = sum(o.size * 2 for o in outs)
    return pl.pallas_call(
        kernel,
        out_shape=tuple(outs),
        in_specs=in_specs,
        out_specs=tuple(out_specs),
        scratch_shapes=scratch,
        compiler_params=pltpu.CompilerParams(
            collective_id=collective_id, has_side_effects=True
        ),
        cost_estimate=pl.CostEstimate(
            flops=flops, bytes_accessed=20 * moved, transcendentals=0
        ),
    )(*operands)


LN_ROWS = 8


class Loads:
    def __init__(self, sources, buffers, sems):
        self.copies = [
            pltpu.make_async_copy(src, buf, sems.at[i])
            for i, (src, buf) in enumerate(zip(sources, buffers))
        ]
        self.buffers = buffers

    def start(self):
        for copy in self.copies:
            copy.start()

    def ready(self, *which):
        for i in which:
            self.copies[i].wait()


class LineSum:
    @staticmethod
    def scratch(S, t, d):
        Q = S // 2
        return [pltpu.VMEM((Q, t, d), BF), pltpu.VMEM((Q + 1, t, d), BF),
                pltpu.SemaphoreType.DMA((2 * Q,)), pltpu.SemaphoreType.DMA((2 * Q,)),
                pltpu.SemaphoreType.DMA((Q,)), pltpu.SemaphoreType.DMA((Q,))]

    def __init__(self, at, part, result, pair, got, s_line, r_line, s_pair, r_pair):
        self.at, self.part, self.result, self.pair, self.got = at, part, result, pair, got
        self.s_line, self.r_line, self.s_pair, self.r_pair = s_line, r_line, s_pair, r_pair

    def share(self, slot):
        at = self.at
        return remote(
            self.part.at[2 * slot + 1 - at.c], self.pair.at[slot], self.s_pair.at[slot],
            self.r_pair.at[slot], (at.partner, at.f),
        )

    def hop(self, slot, up, last):
        at = self.at
        i = slot + (1 - up) * at.Q
        into = slot + last * (at.Q - slot)
        return remote(
            self.pair.at[slot], self.got.at[into], self.s_line.at[i], self.r_line.at[i],
            (at.j + 4 * up - 2, at.f),
        )

    def last(self, slot, up):
        at = self.at
        return (1 - up) * (1 - (at.q - 1 - slot + at.Q - 1) // at.Q)

    def start(self):
        order = []
        for i in range(self.at.Q):
            for slot in (self.at.Q - 1 - i, i):
                if slot not in order:
                    order.append(slot)
        for slot in order:
            self.share(slot).start()

    def base(self, slot):
        self.share(slot).wait_recv()
        return self.part[2 * slot + self.at.c].astype(F32) + self.pair[slot].astype(F32)

    def pass_on(self, slot, up):
        at = self.at

        @pl.when((2 * up - 1) * (slot - at.q) > 0)
        def _():
            value = self.base(slot)
            self.hop(slot, up, 0).wait_recv()
            self.pair[slot] = (value + self.got[slot].astype(F32)).astype(BF)
            self.hop(slot, up, self.last(slot, up)).start()

    def ends(self, steps):
        at = self.at

        @pl.when(at.end == 0)
        def _():
            for i in steps:
                slot = at.low * (at.Q - 1 - i) + (1 - at.low) * i
                self.pair[slot] = self.base(slot).astype(BF)
                self.hop(slot, at.low, self.last(slot, at.low)).start()

    def near(self, i):
        at = self.at

        @pl.when(at.end > 0)
        def _():
            self.pass_on(at.low * (at.Q - 1 - i) + (1 - at.low) * i, at.low)

    def far(self, i):
        at = self.at
        self.pass_on((1 - at.low) * (at.Q - 1 - i) + at.low * i, 1 - at.low)

    def total(self):
        at = self.at
        self.result[...] = self.base(at.q)

        @pl.when(at.q > 0)
        def _():
            self.hop(at.q, 1, 0).wait_recv()
            self.result[...] += self.got[at.q].astype(F32)

        @pl.when(at.q < at.Q - 1)
        def _():
            self.hop(at.q, 0, 1).wait_recv()
            self.result[...] += self.got[at.Q].astype(F32)

    def finish(self):
        q = self.at.q
        for slot in range(self.at.Q):
            self.share(slot).wait_send()

            @pl.when(q < slot)
            def _():
                self.hop(slot, 1, 0).wait_send()

            @pl.when(q > slot)
            def _():
                self.hop(slot, 0, 0).wait_send()


class VectorSum:
    @staticmethod
    def scratch(S, F, w):
        return [
            pltpu.VMEM((F, LN_ROWS, w), F32),
            pltpu.VMEM((F, LN_ROWS, w), F32),
            pltpu.VMEM((S, LN_ROWS, w), F32),
            pltpu.SemaphoreType.DMA((F - 1,)),
            pltpu.SemaphoreType.DMA((F,)),
            pltpu.SemaphoreType.DMA((S - 1,)),
            pltpu.SemaphoreType.DMA((S,)),
        ]

    def __init__(self, at, made, by_shard, by_seq, s_f, r_f, s_s, r_s):
        self.at, self.made, self.by_shard, self.by_seq = at, made, by_shard, by_seq
        j, f, S, F = at.j, at.f, at.S, at.F
        self.over_f, self.over_s = [], []
        for k in range(1, F):
            to, of = lax.rem(f + k, F), lax.rem(f + F - k, F)
            self.over_f.append(
                (remote(made.at[to], by_shard.at[f], s_f.at[k - 1], r_f.at[f], (j, to)),
                 remote(made.at[to], by_shard.at[of], s_f.at[k - 1], r_f.at[of], (j, to)))
            )
        for k in range(1, S):
            to, of = lax.rem(j + k, S), lax.rem(j + S - k, S)
            self.over_s.append(
                (remote(by_seq.at[j], by_seq.at[j], s_s.at[k - 1], r_s.at[j], (to, f)),
                 remote(by_seq.at[j], by_seq.at[of], s_s.at[k - 1], r_s.at[of], (to, f)))
            )

    def start(self):
        for copy, _ in self.over_f:
            copy.start()
        self.by_shard[self.at.f] = self.made[self.at.f]

    def turn_to_seq(self):
        for _, arrival in self.over_f:
            arrival.wait_recv()
        total = self.by_shard[0]
        for p in range(1, self.at.F):
            total += self.by_shard[p]
        self.by_seq[self.at.j] = total
        for copy, _ in self.over_s:
            copy.start()

    def finish(self, result):
        for _, arrival in self.over_s:
            arrival.wait_recv()
        total = self.by_seq[0]
        for p in range(1, self.at.S):
            total += self.by_seq[p]
        result[...] = total
        for copy, _ in self.over_f + self.over_s:
            copy.wait_send()


def closing(
    S, F, collective_id, tok, normed, upstream, grad_mixed, attended, activated, grad_pre,
    w_dense, w_down, w_qkv, w_up, extra, standard, with_dense,
):
    L, D = normed.shape
    w = D // F
    chunk = 3 * LANES
    pairs = grad_mixed.shape[1] // chunk
    grads = [(D // F + EXTRA, chunk)] * pairs
    if with_dense:
        grads.append((attended.shape[1] // F, D))
    big = [normed, grad_mixed, attended, activated, w_dense, w_down, grad_pre, w_qkv, w_up]
    if with_dense:
        big.append(upstream)
    tile = 512
    m = len(grads)

    def kernel(*refs):
        refs = list(refs)
        take = lambda n: [refs.pop(0) for _ in range(n)]
        at = Place(S, F)
        sources = take(len(big))
        extra_ref, standard_ref = take(2)
        branches, normed_sum, ln_out = take(3)
        gathered = take(m)
        loads = Loads(sources, take(len(big)), take(1)[0])
        x, gm, att, act, wd, wdn, gp, wq, wu = loads.buffers[:9]
        jobs, packed, lines = [], [], []
        for i in range(pairs):
            cols = slice(i * chunk, (i + 1) * chunk)
            jobs.append(GradReduce(at, x, gm.at[:, cols], extra_ref.at[:, :, cols], *take(4)))
        if with_dense:
            jobs.append(GradReduce(at, att, loads.buffers[9], None, *take(4)))
        for i in range(m):
            packed.append(take(1)[0])
            lines.append(TokenGather(at, packed[i], gathered[i], *take(4)))
        parts = take(2)
        sums = [
            LineSum(at, part, res, *take(6)) for part, res in zip(parts, (branches, normed_sum))
        ]
        vectors = VectorSum(at, *take(7))
        loads.start()
        at.greet(True, "all")
        loads.ready(0, 1)
        for job in jobs[:pairs]:
            job.start()
        loads.ready(2)
        if with_dense:
            loads.ready(9)
            jobs[-1].start()
        loads.ready(3, 4, 5)

        @pl.loop(0, D // tile)
        def _(i):
            cols = pl.ds(pl.multiple_of(i * tile, tile), tile)
            made = dot(att[...], wd[:, cols]) + dot(act[...], wdn[:, cols])
            parts[0][:, :, cols] = made.astype(BF).reshape(S, tok, tile)

        sums[0].start()
        sums[0].ends([0])
        loads.ready(6, 7, 8)

        @pl.loop(0, D // tile)
        def _(i):
            rows = pl.ds(pl.multiple_of(i * tile, tile), tile)
            made = dot_nt(gm[...], wq[rows, :]) + dot_nt(gp[...], wu[rows, :])
            parts[1][:, :, rows] = made.astype(BF).reshape(S, tok, tile)

        sums[1].start()
        sums[1].ends([0])

        def reduced(i):
            def store(t, wide, value):
                packed[i][:, t : t + wide] = value

            jobs[i].finish(store)
            lines[i].start()

        for i in range(m):
            reduced(i)
            if i < 2:
                sums[i].near(0)
            lines[i].far(1)
        for i in range(m, 2):
            sums[i].near(0)
        for item in sums:
            item.ends(range(1, at.Q - 1))
        for i in range(max(m, 2)):
            if i < 2:
                sums[i].far(0)
            if i < m:
                lines[i].near(1)
        for step in range(1, at.Q - 1):
            for line in lines:
                line.far(step + 1)
            for item in sums:
                item.near(step)
            for item in sums:
                item.far(step)
            for line in lines:
                line.near(step + 1)
        for item in sums:
            item.total()
        grad_normed = normed_sum[...]
        both = jnp.concatenate(
            [
                jnp.sum(grad_normed * standard_ref[...], axis=0, keepdims=True),
                jnp.sum(grad_normed, axis=0, keepdims=True),
                jnp.zeros((LN_ROWS - 2, D), F32),
            ],
            axis=0,
        )
        for p in range(F):
            vectors.made[p] = both[:, p * w : (p + 1) * w]
        vectors.start()
        vectors.turn_to_seq()
        for line in lines:
            line.arrived()
            line.finish()
        vectors.finish(ln_out)
        for item in sums:
            item.finish()

    vmem = pl.BlockSpec(memory_space=pltpu.VMEM)
    anywhere = pl.BlockSpec(memory_space=pl.ANY)
    scratch = [pltpu.VMEM(a.shape, a.dtype) for a in big]
    scratch.append(pltpu.SemaphoreType.DMA((len(big),)))
    for rows, n in grads:
        scratch += GradReduce.scratch(F, rows, n)
    for rows, n in grads:
        scratch.append(pltpu.VMEM((rows, n), BF))
        scratch += TokenGather.scratch(S)
    scratch += [pltpu.VMEM((S, tok, D), BF)] * 2
    scratch += LineSum.scratch(S, tok, D) * 2
    scratch += VectorSum.scratch(S, F, w)
    full = jax.ShapeDtypeStruct((tok, D), F32)
    return pl.pallas_call(
        kernel,
        out_shape=(full, full, jax.ShapeDtypeStruct((LN_ROWS, w), F32))
        + tuple(jax.ShapeDtypeStruct((S, rows, n), BF) for rows, n in grads),
        in_specs=[anywhere] * len(big) + [vmem] * 2,
        out_specs=(vmem,) * 3 + (anywhere,) * m,
        scratch_shapes=scratch,
        compiler_params=pltpu.CompilerParams(
            collective_id=collective_id, has_side_effects=True,
            vmem_limit_bytes=67_000_000 if L > 1024 else None,
        ),
        cost_estimate=pl.CostEstimate(
            flops=6 * L * D * (grad_mixed.shape[1] + activated.shape[1]),
            bytes_accessed=80 * L * D,
            transcendentals=0,
        ),
    )(*big, extra, standard)


def attend_and_close(
    S, F, collective_id, tok, normed, upstream, feed_out, feed_gn, w_dense, w_qkv, rest_up, tables,
    seg_col, seg_row, bias, standard, inv_std, tokens, cotangent, gain, out_bias,
):
    L, D = S * tok, normed.shape[2]
    w = D // F
    chunk = 3 * LANES
    pairs = w_qkv.shape[1] // chunk
    rows_att = 256
    grads = [(D // F + EXTRA, chunk)] * pairs + [(pairs * LANES // F, D)]
    m = len(grads)
    big = [normed, upstream, w_qkv, w_dense, feed_out, feed_gn]
    small = [*tables, seg_col, seg_row, bias, standard, inv_std, tokens, cotangent, gain, out_bias, rest_up]
    tile = 512
    late = rest_up.shape[0]

    def kernel(*refs):
        refs = list(refs)
        take = lambda n: [refs.pop(0) for _ in range(n)]
        at = Place(S, F)
        sources = take(len(big))
        cos, low, high, seg_c, seg_r, bias_ref, standard_ref, inv_ref = take(8)
        tok_ref, cot_ref, gain_ref, out_bias_ref, up_ref = take(5)
        out_ref, grad_ref, ln_out, all_up = take(4)
        gathered = take(m)
        branches, normed_sum = take(2)
        loads = Loads(sources, take(len(big)), take(1)[0])
        x, g, wq, wd, out_part, gn_part = loads.buffers
        gm, att, proj, gatt, qs, ks, vs, dk, dv = take(9)
        ones = jnp.ones((16, L), BF)
        jobs, lines = [], []
        for i in range(pairs):
            cols = slice(i * chunk, (i + 1) * chunk)
            total_row = lambda cols=cols: dot(ones, gm[:, cols]).astype(BF)
            jobs.append(GradReduce(at, x, gm.at[:, cols], total_row, *take(4)))
        jobs.append(GradReduce(at, att, g, None, *take(4)))
        for i in range(m):
            lines.append(TokenGather(at, jobs[i].made.at[at.f], gathered[i], *take(4)))
        ups = [
            TokenGather(at, up_ref.at[i], all_up.at[i], *take(4)) for i in range(late)
        ]
        parts = [gn_part, out_part]
        sums = [
            LineSum(at, part, res, *take(6)) for part, res in zip(parts, (normed_sum, branches))
        ]
        vectors = VectorSum(at, *take(7))
        loads.start()
        at.greet(True, "all")
        for up in ups:
            up.start()
        loads.ready(0, 1, 2, 3)

        @pl.loop(0, pairs)
        def _(p):
            cols = pl.ds(pl.multiple_of(p * chunk, LANES), chunk)
            lanes = pl.ds(pl.multiple_of(p * LANES, LANES), LANES)

            @pl.loop(0, L // rows_att)
            def _(i):
                slots = pl.ds(i * (rows_att // tok), rows_att // tok)
                rows = pl.ds(pl.multiple_of(i * rows_att, rows_att), rows_att)
                block = x[slots].reshape(rows_att, D)
                proj[rows, :] = dot(block, wq[:, cols]) + bias_ref[:, cols]
                block = g[slots].reshape(rows_att, D)
                gatt[rows, :] = dot_nt(block, wd[lanes, :]).astype(BF)

            def during(pair, *steps):
                @pl.when(p == pair)
                def _():
                    for step in steps:
                        step()

            def serve(i, d):
                return lambda: (ups[i].near(d), ups[i].far(d))

            during(0, serve(0, 1))
            during(1, serve(0, 2))

            def pause(i):
                if i == 3:
                    during(0, serve(1, 1))
                    during(1, serve(1, 2))
                if i == 2:
                    during(0, *(serve(k, 1) for k in range(2, late)))
                    during(1, *(serve(k, 2) for k in range(2, late)))

            attention_kernel(
                rows_att, proj, gatt, cos, low, high, seg_c, seg_r, att.at[:, lanes],
                gm.at[:, cols], qs, ks, vs, dk, dv, pause,
            )
            during(0, jobs[0].start)

        loads.ready(5)

        @pl.loop(0, D // tile)
        def _(i):
            rows = pl.ds(pl.multiple_of(i * tile, tile), tile)
            made = columns(gn_part, rows).astype(F32) + dot_nt(gm[...], wq[rows, :])
            gn_part[:, :, rows] = made.astype(BF).reshape(S, tok, tile)

        sums[0].start()
        sums[0].ends([0])
        loads.ready(4)

        @pl.loop(0, D // tile)
        def _(i):
            cols = pl.ds(pl.multiple_of(i * tile, tile), tile)
            made = columns(out_part, cols).astype(F32) + dot(att[...], wd[:, cols])
            out_part[:, :, cols] = made.astype(BF).reshape(S, tok, tile)

        sums[1].start()
        sums[1].ends([0])
        jobs[1].start()

        def reduced(i):
            def store(t, wide, value):
                jobs[i].made[at.f, :, t : t + wide] = value

            jobs[i].finish(store)
            lines[i].start()

        reduced(0)
        for job in jobs[2:]:
            job.start()
        for d in range(3, at.Q):
            for up in ups:
                up.near(d)
                up.far(d)
        lines[0].far(1)

        for item in sums:
            item.ends([1])
        for i in range(m):
            if i:
                reduced(i)
            if i < 2:
                sums[i].near(0)
            if i:
                lines[i].far(1)
        for item in sums:
            item.ends(range(2, at.Q - 1))
        for i in range(m):
            if i < 2:
                sums[i].far(0)
            lines[i].near(1)
        for step in range(1, at.Q - 1):
            for line in lines:
                line.far(step + 1)
            for item in sums:
                item.near(step)
            for item in sums:
                item.far(step)
            for line in lines:
                line.near(step + 1)
        sums[0].total()
        grad_normed, standard = normed_sum[...], standard_ref[...]
        both = jnp.concatenate(
            [
                jnp.sum(grad_normed * standard, axis=0, keepdims=True),
                jnp.sum(grad_normed, axis=0, keepdims=True),
                jnp.zeros((LN_ROWS - 2, D), F32),
            ],
            axis=0,
        )
        for p in range(F):
            vectors.made[p] = both[:, p * w : (p + 1) * w]
        vectors.start()
        scaled = grad_normed * gain_ref[...]
        turned = (
            scaled
            - jnp.mean(scaled, axis=-1, keepdims=True)
            - standard * jnp.mean(scaled * standard, axis=-1, keepdims=True)
        )
        grad_ref[...] = cot_ref[...].astype(F32) + inv_ref[:, 0:1] * turned
        vectors.turn_to_seq()
        sums[1].total()
        out_ref[...] = (tok_ref[...].astype(F32) + branches[...] + out_bias_ref[...]).astype(BF)
        for line in ups + lines:
            line.arrived()
            line.finish()
        vectors.finish(ln_out)
        for item in sums:
            item.finish()

    vmem = pl.BlockSpec(memory_space=pltpu.VMEM)
    anywhere = pl.BlockSpec(memory_space=pl.ANY)
    scratch = [pltpu.VMEM((tok, D), F32)] * 2
    scratch += [pltpu.VMEM(a.shape, a.dtype) for a in big]
    scratch.append(pltpu.SemaphoreType.DMA((len(big),)))
    scratch += [
        pltpu.VMEM((L, pairs * chunk), BF),
        pltpu.VMEM((L, pairs * LANES), BF),
        pltpu.VMEM((L, chunk), F32),
    ]
    scratch += [pltpu.VMEM((L, LANES), BF)] * 4 + [pltpu.VMEM((L, LANES), F32)] * 2
    for rows, n in grads:
        scratch += GradReduce.scratch(F, rows, n)
    scratch += TokenGather.scratch(S) * m
    scratch += TokenGather.scratch(S) * late
    scratch += LineSum.scratch(S, tok, D) * 2
    scratch += VectorSum.scratch(S, F, w)
    full = jax.ShapeDtypeStruct((tok, D), F32)
    return pl.pallas_call(
        kernel,
        out_shape=(
            jax.ShapeDtypeStruct((tok, D), BF), full, jax.ShapeDtypeStruct((LN_ROWS, w), F32),
            jax.ShapeDtypeStruct((late, S) + rest_up.shape[1:], BF),
        )
        + tuple(jax.ShapeDtypeStruct((S, rows, n), BF) for rows, n in grads),
        in_specs=[anywhere] * len(big) + [vmem] * len(small),
        out_specs=(vmem,) * 3 + (anywhere,) * (1 + m),
        scratch_shapes=scratch,
        compiler_params=pltpu.CompilerParams(
            collective_id=collective_id, has_side_effects=True, vmem_limit_bytes=67_000_000
        ),
        cost_estimate=pl.CostEstimate(
            flops=10 * L * D * pairs * chunk,
            bytes_accessed=100 * L * D,
            transcendentals=pairs * L * L,
        ),
    )(*big, *small)


class CornerReduce:
    @staticmethod
    def scratch(rows, n):
        return [pltpu.VMEM((4, rows, n), BF), pltpu.VMEM((3, rows, n), BF),
                pltpu.SemaphoreType.DMA((3,)), pltpu.SemaphoreType.DMA((3,))]

    def __init__(self, at, axis, made, got, send, recv):
        f = at.f
        nx, ny = f + 1 - 2 * lax.rem(f, 2), lax.rem(f + 2, 4)
        self.at, self.made, self.got = at, made, got
        self.one, self.two = (nx, ny) if axis == 0 else (ny, nx)
        self.far = lax.rem(nx + 2, 4)
        self.copies = [
            remote(made.at[block], got.at[i], send.at[i], recv.at[i], (at.j, to))
            for i, (block, to) in enumerate(
                ((self.far, self.one), (self.one, self.one), (self.two, self.two))
            )
        ]

    def send(self):
        self.copies[0].start()
        self.copies[1].start()

    def make(self, make, send):
        for p in (self.far, self.one, self.two, self.at.f):
            make(p)
            if send and p is self.one:
                self.send()

    def middle(self):
        self.copies[0].wait_recv()
        block = self.made[self.two].astype(F32) + self.got[0].astype(F32)
        self.made[self.two] = block.astype(BF)
        self.copies[2].start()

    def total(self):
        self.copies[1].wait_recv()
        self.copies[2].wait_recv()
        total = self.made[self.at.f].astype(F32) + self.got[1].astype(F32)
        return (total + self.got[2].astype(F32)).astype(BF)

    def finish(self):
        for copy in self.copies:
            copy.wait_send()


SMALL = 48
CHUNKS = 4


def opening(
    S, collective_id, tok, small, tokens, cotangent, fc1_weight, fc2_weight, qkv_weight,
    dense_weight,
):
    F, Q, L = 4, S // 2, tok * S
    D, ff = tokens.shape[1], fc1_weight.shape[1]
    rows_d, cols_up = D // F, ff // S
    w_ff = cols_up // F
    pairs = HEADS // S // 2
    wide = 3 * pairs * LANES
    dense_rows = HEAD * HEADS // (F * S)
    half = S // 2
    n_down, n_up = D // CHUNKS, cols_up // CHUNKS
    lead = {}
    at_row = 0
    for name, n in (
        ("gain", rows_d), ("bias", rows_d), ("qkv", 3 * rows_d), ("dense", rows_d),
        ("up", ff // F), ("down", rows_d),
    ):
        lead[name] = (at_row, n // 128)
        at_row += n // 128

    def kernel(*refs):
        refs = list(refs)
        take = lambda n: [refs.pop(0) for _ in range(n)]
        (small_in, tok_in, cot_in, up_in, down_in, qkv_in, dense_in) = take(7)
        (o_normed, o_out, o_gn, o_g, o_qkv, o_dense, o_alldown, o_allup, o_piece,
         o_vec, o_small, o_std, o_inv) = take(13)
        at = Place(S, F)
        j, f = at.j, at.f
        x_own, g_own, n_own, up_own, down_own, dense_own, qkv_raw, qkv_own = take(8)
        normed, g, w_up, w_down, act, gp, slope, part_out, part_gn = take(9)
        small_all, pieces = take(2)
        load_sem, save_sem, s_small, r_small = take(4)
        copies = []

        def load(src, dst):
            copy = pltpu.make_async_copy(src, dst, load_sem.at[len(copies)])
            copies.append(copy)
            copy.start()
            return copy

        for p in range(F):
            load(up_in.at[:, pl.ds(pl.multiple_of((p * S + j) * w_ff, w_ff), w_ff)],
                 up_own.at[:, p * w_ff : (p + 1) * w_ff])
        load(tok_in, x_own)
        load(cot_in, g_own)
        load(down_in.at[pl.ds(pl.multiple_of(j * w_ff, w_ff), w_ff)], down_own)
        load(dense_in.at[pl.ds(pl.multiple_of(j * dense_rows, dense_rows), dense_rows)],
             dense_own)
        for i in range(3 * pairs):
            for which in range(2):
                block = (i % 3) * F * half + (2 * (i // 3) + which) * half + j // 2
                load(qkv_in.at[:, pl.ds(pl.multiple_of(block * LANES, LANES), LANES)],
                     qkv_raw.at[2 * i + which])

        gathers = [
            ShardGather(at, src, dst, *take(3))
            for src, dst in (
                (up_own, w_up), (down_own, w_down), (qkv_own, o_qkv), (dense_own, o_dense),
            )
        ]
        line_n = TokenGather(at, n_own, normed, *take(4))
        line_g = TokenGather(at, g_own, g, *take(4))
        reduce_down = [CornerReduce(at, i % 2, *take(4)) for i in range(CHUNKS)]
        reduce_up = [CornerReduce(at, i % 2, *take(4)) for i in range(CHUNKS)]
        lines = [
            TokenGather(at, pieces.at[i], o_alldown.at[i], *take(4)) for i in range(CHUNKS)
        ]
        lines.append(TokenGather(at, reduce_up[0].made.at[f], o_allup.at[0], *take(4)))
        at.greet(True, "line")
        smalls = []
        for k in range(1, F):
            to, of = lax.rem(f + k, F), lax.rem(f + F - k, F)
            smalls.append(
                (remote(small_in, small_all.at[f], s_small.at[k - 1], r_small.at[k - 1], (j, to)),
                 remote(small_in, small_all.at[of], s_small.at[k - 1], r_small.at[k - 1], (j, to)))
            )
        for copy, _ in smalls:
            copy.start()
        small_all[f] = small_in[...]
        for p in range(F):
            copies[p].wait()
        gathers[0].start()
        copies[F + 2].wait()
        gathers[1].start()
        copies[F + 3].wait()
        copies[F + 1].wait()
        line_g.start()

        def row_of(name):
            first, n = lead[name]
            return jnp.concatenate(
                [small_all[p, first + r : first + r + 1, :] for p in range(F) for r in range(n)],
                axis=1,
            )

        copies[F].wait()
        values = x_own[...].astype(F32)
        centre = jnp.mean(values, axis=-1, keepdims=True)
        values = values - centre
        inv_std = lax.rsqrt(jnp.mean(values * values, axis=-1, keepdims=True) + EPS)
        values = values * inv_std
        o_std[...] = values
        o_inv[...] = jnp.broadcast_to(inv_std, (tok, 128))
        for _, arrival in smalls:
            arrival.wait_recv()
        n_own[...] = (values * row_of("gain") + row_of("bias")).astype(BF)
        line_n.start()

        for d in range(1, Q - 1):
            line_g.near(d)
            line_g.far(d)
            if d == 1:
                gathers[0].relay()
            line_n.near(d)
            line_n.far(d)
            if d == 1:
                gathers[1].relay()
                gathers[3].start()
        odd = lax.rem(j, 2) == 1
        lane = lax.broadcasted_iota(jnp.int32, (rows_d, LANES), 1)
        for copy in copies[F + 4 :]:
            copy.wait()
        for i in range(3 * pairs):
            first, second = qkv_raw[2 * i].astype(F32), qkv_raw[2 * i + 1].astype(F32)
            first = jnp.where(odd, pltpu.roll(first, HEAD, 1), first)
            second = jnp.where(odd, second, pltpu.roll(second, HEAD, 1))
            qkv_own[:, i * LANES : (i + 1) * LANES] = jnp.where(
                lane < HEAD, first, second
            ).astype(BF)
        line_g.far(Q - 1)
        gathers[3].relay()
        line_n.far(Q - 1)
        line_n.arrived()
        gathers[0].arrived()
        saves = []

        def save(src, dst):
            copy = pltpu.make_async_copy(src, dst, save_sem.at[len(saves)])
            saves.append(copy)
            copy.start()

        save(normed, o_normed)
        up_first = lead["up"][0]

        @pl.loop(0, F)
        def _(p):
            cols = pl.ds(pl.multiple_of(p * w_ff, w_ff), w_ff)
            u = jnp.concatenate(
                [
                    small_all[p, pl.ds(up_first + j * (w_ff // 128) + r, 1), :]
                    for r in range(w_ff // 128)
                ],
                axis=1,
            )
            for s in range(F):
                part = normed[:, :, s * rows_d : (s + 1) * rows_d].reshape(L, rows_d)
                u = u + dot(part, w_up[s, :, cols])
            square = u * u
            root = 0.7978845608028654
            t = jnp.tanh(root * (u + 0.044715 * (square * u)))
            act[:, cols] = ((0.5 * u) * (1.0 + t)).astype(BF)
            slope[:, cols] = 0.5 * (1.0 + t) + (0.5 * u) * (1.0 - t * t) * (
                root * (1.0 + 3 * 0.044715 * square)
            )

        line_g.arrived()
        save(g, o_g)
        ones = jnp.ones((EXTRA, L), BF)

        def make_down(c):
            cols = slice(c * n_down, (c + 1) * n_down)

            def make(p):
                block = act[:, pl.ds(pl.multiple_of(p * w_ff, w_ff), w_ff)]
                right = g[:, :, cols].reshape(L, n_down)
                reduce_down[c].made[p, 0:w_ff, :] = dot_tn(block, right).astype(BF)
                if c == 0:
                    mine = g[:, :, pl.ds(pl.multiple_of(p * rows_d, rows_d), rows_d)]
                    term = dot(ones, mine.reshape(L, rows_d))
                    reduce_down[c].made[p, w_ff:, :] = term.astype(BF)

            return make

        def make_up(c):
            cols = slice(c * n_up, (c + 1) * n_up)

            def make(p):
                block = normed[:, :, pl.ds(pl.multiple_of(p * rows_d, rows_d), rows_d)]
                made = dot_tn(block.reshape(L, rows_d), gp[:, cols])
                reduce_up[c].made[p, 0:rows_d, :] = made.astype(BF)
                if c == 0:
                    term = dot(ones, gp[:, pl.ds(pl.multiple_of(p * w_ff, w_ff), w_ff)])
                    reduce_up[c].made[p, rows_d:, :] = term.astype(BF)

            return make

        for c in range(CHUNKS):
            reduce_down[c].make(make_down(c), c < 2)
        gathers[1].arrived()

        @pl.loop(0, F)
        def _(p):
            cols = pl.ds(pl.multiple_of(p * w_ff, w_ff), w_ff)
            grad_act = dot_nt(g[...].reshape(L, D), w_down[p])
            gp[:, cols] = (grad_act * slope[:, cols]).astype(BF)


        def end_down(c):
            total = reduce_down[c].total()
            pieces[c] = total[0:w_ff, :]
            if c == 0:
                o_vec[...] = total[w_ff:, :]
            lines[c].start()

        def end_up(c):
            total = reduce_up[c].total()
            if c:
                o_piece[c - 1] = total
            else:
                reduce_up[0].made[f] = total
                lines[CHUNKS].start()

        def serve(c, d):
            lines[c].near(d)
            lines[c].far(d)

        def feed_out(i):
            cols = slice(i * rows_d, (i + 1) * rows_d)
            made = dot(act[:, 0:w_ff], w_down[0, :, cols])
            for p in range(1, F):
                made = made + dot(act[:, p * w_ff : (p + 1) * w_ff], w_down[p, :, cols])
            part_out[:, :, cols] = made.astype(BF).reshape(S, tok, rows_d)

        def feed_gn(i):
            made = dot_nt(gp[...], w_up[i])
            cols = slice(i * rows_d, (i + 1) * rows_d)
            part_gn[:, :, cols] = made.astype(BF).reshape(S, tok, rows_d)

        for c in (0, 1):
            reduce_down[c].middle()
        for c in (2, 3):
            reduce_down[c].send()
        for c in (0, 1):
            reduce_up[c].make(make_up(c), False)
        for c in (0, 1):
            end_down(c)
        for c in (2, 3):
            reduce_up[c].make(make_up(c), False)
        serve(0, 1)
        for c in (2, 3):
            reduce_down[c].middle()
        for c in (0, 1):
            reduce_up[c].send()
        serve(1, 1)
        feed_out(0)
        feed_out(1)
        for c in (2, 3):
            end_down(c)
        feed_out(2)
        serve(0, 2)
        for c in (0, 1):
            reduce_up[c].middle()
        for c in (2, 3):
            reduce_up[c].send()
        gathers[2].start()
        serve(1, 2)
        feed_out(3)
        save(part_out, o_out)
        serve(2, 1)
        for c in (0, 1):
            end_up(c)
        feed_gn(0)
        serve(3, 1)
        feed_gn(1)
        for d in range(3, Q):
            serve(0, d)
            serve(1, d)
        for c in (2, 3):
            reduce_up[c].middle()
        feed_gn(2)
        serve(2, 2)
        feed_gn(3)
        save(part_gn, o_gn)
        serve(3, 2)
        serve(CHUNKS, 1)
        gathers[2].relay()
        for c in (2, 3):
            end_up(c)
        for d in range(3, Q):
            serve(2, d)
            serve(3, d)
        for d in range(2, Q):
            serve(CHUNKS, d)
        o_small[...] = small_all[...]
        for copy, _ in smalls:
            copy.wait_send()
        for gather in gathers[2:]:
            gather.arrived()
        for line in lines:
            line.arrived()
        for item in [line_n, line_g] + lines + gathers + reduce_down + reduce_up:
            item.finish()
        for copy in saves:
            copy.wait()

    vmem = pl.BlockSpec(memory_space=pltpu.VMEM)
    anywhere = pl.BlockSpec(memory_space=pl.ANY)
    out = lambda shape, dtype=BF: jax.ShapeDtypeStruct(shape, dtype)
    scratch = [
        pltpu.VMEM(shape, dtype)
        for shape, dtype in (
            ((tok, D), BF), ((tok, D), BF), ((tok, D), BF), ((rows_d, cols_up), BF),
            ((w_ff, D), BF), ((dense_rows, D), BF), ((6 * pairs, rows_d, LANES), BF),
            ((rows_d, wide), BF),
            ((S, tok, D), BF), ((S, tok, D), BF), ((F, rows_d, cols_up), BF), ((F, w_ff, D), BF),
            ((L, cols_up), BF), ((L, cols_up), BF), ((L, cols_up), F32),
            ((S, tok, D), BF), ((S, tok, D), BF),
            ((F, SMALL, 128), F32), ((CHUNKS, w_ff, n_down), BF),
        )
    ]
    scratch += [
        pltpu.SemaphoreType.DMA((F + 4 + 6 * pairs,)), pltpu.SemaphoreType.DMA((6,)),
        pltpu.SemaphoreType.DMA((F - 1,)), pltpu.SemaphoreType.DMA((F - 1,)),
    ]
    for _ in range(4):
        scratch += ShardGather.scratch(F)
    for _ in range(2):
        scratch += TokenGather.scratch(S)
    for c in range(CHUNKS):
        scratch += CornerReduce.scratch(w_ff + (0 if c else EXTRA), n_down)
    for c in range(CHUNKS):
        scratch += CornerReduce.scratch(rows_d + (0 if c else EXTRA), n_up)
    for _ in range(CHUNKS + 1):
        scratch += TokenGather.scratch(S)
    return pl.pallas_call(
        kernel,
        out_shape=(
            out((S, tok, D)), out((S, tok, D)), out((S, tok, D)), out((S, tok, D)),
            out((F, rows_d, wide)), out((F, dense_rows, D)),
            out((CHUNKS, S, w_ff, n_down)), out((1, S, rows_d + EXTRA, n_up)),
            out((CHUNKS - 1, rows_d, n_up)),
            out((EXTRA, n_down)), out((F, SMALL, 128), F32),
            out((tok, D), F32), out((tok, 128), F32),
        ),
        in_specs=[vmem] + [anywhere] * 6,
        out_specs=(anywhere,) * 8 + (vmem,) * 5,
        scratch_shapes=scratch,
        compiler_params=pltpu.CompilerParams(
            collective_id=collective_id, has_side_effects=True, vmem_limit_bytes=67_000_000
        ),
        cost_estimate=pl.CostEstimate(
            flops=8 * L * D * cols_up, bytes_accessed=200 * L * D, transcendentals=L * cols_up
        ),
    )(small, tokens, cotangent, fc1_weight, fc2_weight, qkv_weight, dense_weight)


def half_lanes(first, second, odd):
    lane = lax.broadcasted_iota(jnp.int32, first.shape, 1)
    if odd:
        first = pltpu.roll(first, HEAD, 1)
    else:
        second = pltpu.roll(second, HEAD, 1)
    return jnp.where(lane < HEAD, first, second)


def pick_qkv(weight, j, F, S, pairs):
    rows = weight.shape[0]
    per_shard = S // 2

    def kernel(j_ref, first, second, out):
        a, b = first[...].astype(F32), second[...].astype(F32)

        @pl.when(j_ref[0] % 2 == 0)
        def _():
            out[...] = half_lanes(a, b, 0).astype(BF)

        @pl.when(j_ref[0] % 2 == 1)
        def _():
            out[...] = half_lanes(a, b, 1).astype(BF)

    def column(which):
        return lambda i, j_ref: (
            0, (i % 3) * F * per_shard + (2 * (i // 3) + which) * per_shard + j_ref[0] // 2
        )

    return pl.pallas_call(
        kernel,
        grid_spec=pltpu.PrefetchScalarGridSpec(
            num_scalar_prefetch=1,
            grid=(3 * pairs,),
            in_specs=[pl.BlockSpec((rows, LANES), column(0)), pl.BlockSpec((rows, LANES), column(1))],
            out_specs=pl.BlockSpec((rows, LANES), lambda i, j_ref: (0, i)),
        ),
        out_shape=jax.ShapeDtypeStruct((rows, 3 * pairs * LANES), BF),
    )(j[None].astype(jnp.int32), weight, weight)


def pick_up(weight, j, F, S):
    rows, ff = weight.shape
    w = ff // (F * S)
    if w % LANES:
        split = weight.reshape(rows, F, S, w)
        return lax.dynamic_index_in_dim(split, j, 2, keepdims=False).reshape(rows, F * w)

    def kernel(j_ref, src, out):
        out[...] = src[...]

    return pl.pallas_call(
        kernel,
        grid_spec=pltpu.PrefetchScalarGridSpec(
            num_scalar_prefetch=1,
            grid=(F,),
            in_specs=[pl.BlockSpec((rows, w), lambda i, j_ref: (0, i * S + j_ref[0]))],
            out_specs=pl.BlockSpec((rows, w), lambda i, j_ref: (0, i)),
        ),
        out_shape=jax.ShapeDtypeStruct((rows, F * w), BF),
    )(j[None].astype(jnp.int32), weight)


def unpack_qkv(gathered, rows, S):
    width = S * HEAD
    pairs = len(gathered)

    def kernel(*refs):
        out = refs[pairs]
        for p in range(pairs):

            @pl.when(pl.program_id(0) % pairs == p)
            def _():
                src = refs[p]
                for half in range(2):
                    for z in range(S // 2):
                        a, b = src[2 * z].astype(F32), src[2 * z + 1].astype(F32)
                        at = half * width + z * LANES
                        out[:, at : at + LANES] = half_lanes(a, b, half)

    return pl.pallas_call(
        kernel,
        grid=(3 * pairs,),
        in_specs=[pl.BlockSpec((S, rows, LANES), lambda i: (0, 0, i // pairs))] * pairs,
        out_specs=pl.BlockSpec((rows, 2 * width), lambda i: (0, i)),
        out_shape=jax.ShapeDtypeStruct((rows, HEADS * HEAD * 3), F32),
    )(*gathered)


def unpack_groups(*stacks, rows):
    S, w = stacks[0].shape[1], stacks[0].shape[3]
    groups = [stack.shape[0] for stack in stacks]
    starts = [sum(groups[:i]) for i in range(len(groups))]

    def kernel(*refs):
        i = pl.program_id(0)
        for src, start, count in zip(refs, starts, groups):

            @pl.when((i >= start) & (i < start + count))
            def _():
                for s in range(S):
                    refs[-1][:, s * w : (s + 1) * w] = src[0, s].astype(F32)

    def block(start, count):
        return pl.BlockSpec(
            (1, S, rows, w), lambda i: (jnp.clip(i - start, 0, count - 1), 0, 0, 0)
        )

    return pl.pallas_call(
        kernel,
        grid=(sum(groups),),
        in_specs=[block(start, count) for start, count in zip(starts, groups)],
        out_specs=pl.BlockSpec((rows, S * w), lambda i: (0, i)),
        out_shape=jax.ShapeDtypeStruct((rows, sum(groups) * S * w), F32),
    )(*stacks)


def unpack_cols(gathered, rows, F):
    S, _, cols = gathered.shape
    w = cols // F
    if w % LANES:
        split = gathered[:, :rows].reshape(S, rows, F, w)
        return split.transpose(1, 2, 0, 3).reshape(rows, F * S * w).astype(F32)

    def kernel(src, out):
        for s in range(S):
            out[:, s * w : (s + 1) * w] = src[s].astype(F32)

    return pl.pallas_call(
        kernel,
        grid=(F,),
        in_specs=[pl.BlockSpec((S, rows, w), lambda i: (0, 0, i))],
        out_specs=pl.BlockSpec((rows, S * w), lambda i: (0, i)),
        out_shape=jax.ShapeDtypeStruct((rows, F * S * w), F32),
    )(gathered)


def unpack_chunks(gathered):
    C, S, rows, n = gathered.shape

    def kernel(src, out):
        for c in range(C):
            out[:, c * n : (c + 1) * n] = src[c, 0].astype(F32)

    return pl.pallas_call(
        kernel,
        grid=(S,),
        in_specs=[pl.BlockSpec((C, 1, rows, n), lambda i: (0, i, 0, 0))],
        out_specs=pl.BlockSpec((rows, C * n), lambda i: (i, 0)),
        out_shape=jax.ShapeDtypeStruct((S * rows, C * n), F32),
    )(gathered)


def unpack_rows(gathered, rows):
    S, _, n = gathered.shape

    def kernel(src, out):
        out[...] = src[0].astype(F32)

    return pl.pallas_call(
        kernel,
        grid=(S,),
        in_specs=[pl.BlockSpec((1, rows, n), lambda i: (i, 0, 0))],
        out_specs=pl.BlockSpec((rows, n), lambda i: (i, 0)),
        out_shape=jax.ShapeDtypeStruct((S * rows, n), F32),
    )(gathered)


def body(
    tokens,
    ln_gain,
    ln_bias,
    qkv_weight,
    qkv_bias,
    dense_weight,
    dense_bias,
    fc1_weight,
    fc1_bias,
    fc2_weight,
    fc2_bias,
    segments,
    positions,
    cotangent,
):
    S, F = lax.axis_size("seq"), lax.axis_size("fsdp")
    j, f = lax.axis_index("seq"), lax.axis_index("fsdp")
    tok, D = tokens.shape[1], tokens.shape[2]
    length = tok * S
    rows_d = D // F
    ff = fc1_weight.shape[1]
    cols_up = ff // S
    block_up = cols_up // F
    hp = HEADS // S
    pairs = hp // 2
    per_shard = HEADS // F
    spread = per_shard % S == 0
    slots = per_shard // S if spread else 0

    qkv_width = pairs * 3 * LANES

    def heads_of(array, lead):
        shape = array.shape
        if spread:
            split = array.reshape(shape[:lead] + (F, S, slots) + shape[lead + 1 :])
            mine = lax.dynamic_index_in_dim(split, j, lead + 1, keepdims=False)
            return mine.reshape(shape[:lead] + (hp,) + shape[lead + 1 :])
        return lax.dynamic_slice_in_dim(array, j * hp, hp, lead)

    def qkv_cols(array):
        n = array.shape[0]
        mine = heads_of(array.reshape(n, 3, HEADS, HEAD), 2)
        return mine.reshape(n, 3, pairs, 2, HEAD).transpose(0, 2, 1, 3, 4).reshape(n, -1)

    def from_qkv_cols(gathered):
        n = gathered.shape[1]
        split = gathered.reshape(S, n, pairs, 3, 2, HEAD).transpose(0, 1, 3, 2, 4, 5)
        split = split.reshape(S, n, 3, hp, HEAD)
        if spread:
            moved = jnp.moveaxis(split.reshape(S, n, 3, F, slots, HEAD), 0, 3)
        else:
            moved = jnp.moveaxis(split, 0, 2)
        return moved.reshape(n, -1)

    upstream_own = cotangent[0]
    seg_row = segments[0]
    block_dense = slots * HEAD

    def rider(values, width):
        return jnp.pad(values[:, None], ((0, 0), (0, EXTRA - 1), (0, width - values.shape[1])))

    def split_small(small):
        cuts, at = [], 0
        for piece in smalls:
            cuts.append(small[:, at : at + piece.shape[0]].reshape(-1).astype(F32))
            at += piece.shape[0]
        return cuts

    smalls = (ln_gain, ln_bias, qkv_bias, dense_bias, fc1_bias, fc2_bias)
    fused = F == 4 and spread and slots == 1 and block_up % 128 == 0
    if fused:
        rows = [piece.astype(F32).reshape(-1, 128) for piece in smalls]
        small = jnp.concatenate(rows, axis=0)
        small = jnp.pad(small, ((0, SMALL - small.shape[0]), (0, 0)))
        (normed, feed_out, feed_gn, upstream, w_qkv, w_dense, all_down, first_up, rest_up,
         out_mine, small, standard, inv_std) = opening(
            S, 1, tok, small, tokens[0], upstream_own, fc1_weight, fc2_weight, qkv_weight,
            dense_weight,
        )
        gain, shift, b_qkv, b_dense, b_up, b_down = split_small(small.reshape(F, -1))
        w_dense = [w_dense]
        out_mine = out_mine[0, :rows_d].astype(F32)
    else:
        inputs = tokens[0].astype(F32)
        centre = jnp.mean(inputs, axis=-1, keepdims=True)
        variance = jnp.mean((inputs - centre) ** 2, axis=-1, keepdims=True)
        inv_std = lax.rsqrt(variance + EPS)
        standard = (inputs - centre) * inv_std
        small = jnp.concatenate(smalls)
        small = lax.all_gather(small, "fsdp", axis=0)
        gain, shift, b_qkv, b_dense, b_up, b_down = split_small(small)

        normed_own = (standard * gain + shift).astype(BF)

        up_own = pick_up(fc1_weight, j, F, S)
        down_own = lax.dynamic_slice_in_dim(fc2_weight, j * block_up, block_up, 0)
        if spread and slots == 1:
            qkv_own = pick_qkv(qkv_weight, j, F, S, pairs)
        else:
            qkv_own = qkv_cols(qkv_weight)
        w_up, w_down, normed, upstream = exchange(
            S, F, 1, shards=(up_own, down_own), tokens=(normed_own, upstream_own)
        )
        w_up, w_down = w_up.reshape(D, cols_up), w_down.reshape(cols_up, D)
        normed, upstream = normed.reshape(length, D), upstream.reshape(length, D)

        bias_up = lax.dynamic_index_in_dim(b_up.reshape(F, S, block_up), j, 1, keepdims=False)
        bias_up = bias_up.reshape(-1)

        pre_act = dot(normed, w_up) + bias_up
        activated = gelu_tanh(pre_act).astype(BF)
        out_term = jnp.sum(upstream.astype(F32), axis=0).reshape(F, rows_d)
        piece_down, out_mine = exchange(
            S, F, 2, grads=((activated, upstream, rider(out_term, D)),), split=True
        )
        out_mine = out_mine[0, :rows_d].astype(F32)

        grad_act = dot_nt(upstream, w_down)
        grad_pre = jax.vjp(gelu_tanh, pre_act)[1](grad_act)[0].astype(BF)
        up_term = jnp.sum(grad_pre.astype(F32), axis=0).reshape(F, block_up)
        shards = (qkv_own,)
        if spread:
            shards += (lax.dynamic_slice_in_dim(dense_weight, j * block_dense, block_dense, 0),)
        piece_up, w_qkv, *w_dense, all_down = exchange(
            S, F, 3, grads=((normed, grad_pre, rider(up_term, cols_up)),), shards=shards,
            tokens=(piece_down,),
        )
    bias_qkv = qkv_cols(b_qkv[None])[0]
    w_qkv = w_qkv.reshape(D, qkv_width)
    if spread:
        w_dense = w_dense[0].reshape(hp * HEAD, D)
    else:
        w_dense = lax.dynamic_slice_in_dim(
            lax.all_gather(dense_weight, "fsdp", axis=0, tiled=True), j * hp * HEAD, hp * HEAD, 0
        )
    if fused:
        result, grad_inputs, ln_mine, late_up, *gathered = attend_and_close(
            S, F, 5, tok, normed, upstream, feed_out, feed_gn, w_dense, w_qkv, rest_up,
            angle_tables(seg_row),
            seg_row[:, None], seg_row[None, :], bias_qkv[None], standard, inv_std, tokens[0],
            upstream_own, gain[None], (b_dense + b_down)[None],
        )
    else:
        all_up = lax.all_gather(piece_up, "seq", axis=0)
        projected = dot(normed, w_qkv) + bias_qkv
        grad_att = dot_nt(upstream, w_dense).astype(BF)
        attended, grad_mixed = attention(projected, grad_att, angle_tables(seg_row), seg_row)
        qkv_term = jnp.sum(grad_mixed.astype(F32), axis=0)
        qkv_term = jnp.broadcast_to(qkv_term[None], (F, qkv_width))
        branches, grad_normed, ln_mine, *gathered = closing(
            S, F, 5, tok, normed, upstream, grad_mixed, attended, activated, grad_pre,
            w_dense, w_down, w_qkv, w_up, rider(qkv_term, qkv_width), standard, spread,
        )
    all_qkv = gathered[:pairs]
    if not fused:
        result = (inputs + branches + (b_dense + b_down)).astype(BF)
        scaled = grad_normed * gain
        grad_inputs = upstream_own.astype(F32) + inv_std * (
            scaled
            - jnp.mean(scaled, axis=-1, keepdims=True)
            - standard * jnp.mean(scaled * standard, axis=-1, keepdims=True)
        )

    if fused:
        grad_down = unpack_chunks(all_down)
        grad_up = unpack_groups(first_up, late_up, rows=rows_d)
        up_mine = first_up[0, :, rows_d].astype(F32).reshape(-1)
    else:
        grad_down = unpack_rows(all_down, block_up)
        grad_up = unpack_cols(all_up, rows_d, F)
        up_mine = all_up[:, rows_d, :block_up].astype(F32).reshape(-1)
    qkv_sums = jnp.concatenate([piece[:, rows_d] for piece in all_qkv], axis=1)
    qkv_sums = from_qkv_cols(qkv_sums[:, None]).reshape(F, -1)
    qkv_mine = lax.dynamic_index_in_dim(qkv_sums, f, 0, keepdims=False).astype(F32)
    if spread and slots == 1:
        grad_qkv = unpack_qkv(all_qkv, rows_d, S)
    else:
        joined = jnp.concatenate([piece[:, :rows_d] for piece in all_qkv], axis=2)
        grad_qkv = from_qkv_cols(joined).astype(F32)
    if spread:
        grad_dense = gathered[pairs].reshape(rows_d, D).astype(F32)
    else:
        part = lax.all_gather(dot_tn(attended, upstream).astype(BF), "seq", axis=0, tiled=True)
        grad_dense = lax.psum_scatter(part, "fsdp", scatter_dimension=0, tiled=True).astype(F32)
    return (
        result[None],
        grad_inputs[None],
        ln_mine[0],
        ln_mine[1],
        grad_qkv,
        qkv_mine,
        grad_dense,
        out_mine,
        grad_up,
        up_mine,
        grad_down,
        out_mine,
    )


def solution(mesh):
    row, mat = P("fsdp"), P("fsdp", None)
    act = P("fsdp", "seq", None)
    return jax.shard_map(
        body,
        mesh=mesh,
        in_specs=(
            act, row, row, mat, row, mat, row, mat, row, mat, row, mat, P("fsdp", "seq"), act,
        ),
        out_specs=(act, act, row, row, mat, row, mat, row, mat, row, mat, row),
        check_vma=False,
    )
```

```python
import functools

import jax
import jax.numpy as jnp
from jax import lax
from jax.experimental import pallas as pl
from jax.experimental.pallas import tpu as pltpu
from jax.sharding import PartitionSpec as P


HEADS = 32
HEAD = 64
ROT = 32
EPS = 1e-05
DOC_SHIFT = 1023
LANES = 2 * HEAD
BF = jnp.bfloat16
F32 = jnp.float32


def dot(left, right):
    return lax.dot_general(left, right, (((1,), (0,)), ((), ())), preferred_element_type=F32)


def dot_nt(left, right):
    return lax.dot_general(left, right, (((1,), (1,)), ((), ())), preferred_element_type=F32)


def dot_tn(left, right):
    return lax.dot_general(left, right, (((0,), (0,)), ((), ())), preferred_element_type=F32)


def columns(ref, cols):
    if len(ref.shape) == 2:
        return ref[:, cols]
    block = ref[:, :, cols]
    return block.reshape(-1, block.shape[-1])


def gelu_tanh(values_in):
    return jax.nn.gelu(values_in, approximate=True)


def turn(values, cos, sin_low, sin_high):
    half = ROT // 2
    return (
        values * cos
        - pltpu.roll(values, LANES - half, 1) * sin_low
        + pltpu.roll(values, half, 1) * sin_high
    )


def attention_kernel(
    rows, proj, grad_out, cos, sin_low, sin_high, seg_col, seg_row,
    out, grad_proj, qs, ks, vs, dk, dv, pause=None,
):
    length = proj.shape[0]
    blocks = length // rows
    scale = HEAD**-0.5
    for i in range(blocks):
        r = slice(i * rows, (i + 1) * rows)
        c, lo, hi = cos[r, :], sin_low[r, :], sin_high[r, :]
        qs[r, :] = turn(proj[r, 0:LANES], c, lo, hi).astype(BF) * jnp.asarray(scale, BF)
        ks[r, :] = turn(proj[r, LANES : 2 * LANES], c, lo, hi).astype(BF)
        vs[r, :] = proj[r, 2 * LANES : 3 * LANES].astype(BF)
    lane = lax.broadcasted_iota(jnp.int32, (rows, LANES), 1)
    first = lane < HEAD
    zero = jnp.zeros((rows, LANES), BF)
    for i in reversed(range(blocks)):
        r = slice(i * rows, (i + 1) * rows)
        n = (i + 1) * rows
        place_q = i * rows + lax.broadcasted_iota(jnp.int32, (rows, n), 0)
        place_k = lax.broadcasted_iota(jnp.int32, (rows, n), 1)
        allowed = (place_k <= place_q) & (seg_col[r, :] == seg_row[:, 0:n])
        q2, g2 = qs[r, :], grad_out[r, :]
        k, v = ks[0:n, :], vs[0:n, :]
        o_parts, dq_parts = [], []
        for h in range(2):
            mine = first if h == 0 else ~first
            q = jnp.where(mine, q2, zero)
            g = jnp.where(mine, g2, zero)
            s = jnp.where(allowed, dot_nt(q, k), -1e30)
            e = jnp.exp(s - jnp.max(s, axis=-1, keepdims=True))
            p = e * (1.0 / jnp.sum(e, axis=-1, keepdims=True))
            pb = p.astype(BF)
            o_parts.append(dot(pb, v))
            dp = dot_nt(g, v)
            inner = jnp.sum(p * dp, axis=-1, keepdims=True)
            ds = (p * (dp - inner)).astype(BF)
            dq_parts.append(dot(ds, k))
            dk_new, dv_new = dot_tn(ds, q), dot_tn(pb, g)
            if i == blocks - 1 and h == 0:
                dk[...] = dk_new
                dv[...] = dv_new
            else:
                dk[0:n, :] += dk_new
                dv[0:n, :] += dv_new
        out[r, :] = jnp.where(first, o_parts[0], o_parts[1]).astype(BF)
        dq = (jnp.where(first, dq_parts[0], dq_parts[1]) * scale).astype(BF).astype(F32)
        c, lo, hi = cos[r, :], sin_low[r, :], sin_high[r, :]
        grad_proj[r, 0:LANES] = turn(dq, c, -lo, -hi).astype(BF)
        if pause is not None:
            pause(i)
    for i in range(blocks):
        r = slice(i * rows, (i + 1) * rows)
        c, lo, hi = cos[r, :], sin_low[r, :], sin_high[r, :]
        grad_k = dk[r, :].astype(BF).astype(F32)
        grad_proj[r, LANES : 2 * LANES] = turn(grad_k, c, -lo, -hi).astype(BF)
        grad_proj[r, 2 * LANES : 3 * LANES] = dv[r, :].astype(BF)


def attention(proj, grad_att, tables, segments):
    length = proj.shape[0]
    pairs = grad_att.shape[1] // LANES
    rows = 256
    whole = lambda shape: pl.BlockSpec(shape, lambda p: (0, 0))
    return pl.pallas_call(
        functools.partial(attention_kernel, rows),
        grid=(pairs,),
        out_shape=(
            jax.ShapeDtypeStruct((length, pairs * LANES), BF),
            jax.ShapeDtypeStruct((length, 3 * pairs * LANES), BF),
        ),
        in_specs=[
            pl.BlockSpec((length, 3 * LANES), lambda p: (0, p)),
            pl.BlockSpec((length, LANES), lambda p: (0, p)),
            whole((length, LANES)),
            whole((length, LANES)),
            whole((length, LANES)),
            whole((length, 1)),
            whole((1, length)),
        ],
        out_specs=(
            pl.BlockSpec((length, LANES), lambda p: (0, p)),
            pl.BlockSpec((length, 3 * LANES), lambda p: (0, p)),
        ),
        scratch_shapes=[pltpu.VMEM((length, LANES), BF)] * 3
        + [pltpu.VMEM((length, LANES), F32)] * 2,
        cost_estimate=pl.CostEstimate(
            flops=14 * pairs * length * length * LANES,
            bytes_accessed=pairs * length * LANES * 24,
            transcendentals=pairs * length * length,
        ),
    )(proj, grad_att, *tables, segments[:, None], segments[None, :])


def angle_tables(seg_row):
    length = seg_row.shape[0]
    position = jnp.arange(length, dtype=jnp.int32) + jnp.where(seg_row > 0, DOC_SHIFT, 0)
    inverse = 1.0 / 10000.0 ** (jnp.arange(0, ROT, 2, dtype=F32) / ROT)
    inverse = jnp.tile(inverse, LANES // (ROT // 2))
    angles = position.astype(F32)[:, None] * inverse[None, :]
    cosine, sine = jnp.cos(angles), jnp.sin(angles)
    lane = jnp.arange(LANES)[None, :] % HEAD
    low = lane < ROT // 2
    return (
        jnp.where(lane < ROT, cosine, 1.0),
        jnp.where(low, sine, 0.0),
        jnp.where((lane < ROT) & ~low, sine, 0.0),
    )


MESH = pl.DeviceIdType.MESH


def remote(src, dst, send, recv, device):
    return pltpu.make_async_remote_copy(
        src_ref=src, dst_ref=dst, send_sem=send, recv_sem=recv, device_id=device,
        device_id_type=MESH,
    )


class Place:
    def __init__(self, S, F):
        self.S, self.F, self.Q = S, F, S // 2
        self.j, self.f = lax.axis_index("seq"), lax.axis_index("fsdp")
        self.q, self.c = self.j // 2, lax.rem(self.j, 2)
        self.partner = 2 * self.q + 1 - self.c
        self.low = 1 - self.q // (self.Q // 2)
        self.side = 2 * (2 * self.low - 1)
        self.end = self.low * self.q + (1 - self.low) * (self.Q - 1 - self.q)

    def greet(self, over_fsdp, over_seq):
        barrier = pltpu.get_barrier_semaphore()

        def signal(j, f):
            pl.semaphore_signal(barrier, inc=1, device_id=(j, f), device_id_type=MESH)

        count = 0
        if over_fsdp:
            for k in range(1, self.F):
                signal(self.j, lax.rem(self.f + k, self.F))
            count += self.F - 1
        if over_seq == "all":
            for k in range(1, self.S):
                signal(lax.rem(self.j + k, self.S), self.f)
            count += self.S - 1
        elif over_seq == "line":
            signal(self.partner, self.f)

            @pl.when(self.q > 0)
            def _():
                signal(self.j - 2, self.f)

            @pl.when(self.q < self.Q - 1)
            def _():
                signal(self.j + 2, self.f)

            count += 1 + (self.q + self.Q - 1) // self.Q + (2 * self.Q - 2 - self.q) // self.Q
        pl.semaphore_wait(barrier, count)


class ShardGather:
    @staticmethod
    def scratch(F):
        n = 6 if F == 4 else F - 1
        return [pltpu.SemaphoreType.DMA((n,)), pltpu.SemaphoreType.DMA((n,)),
                pltpu.SemaphoreType.DMA]

    def __init__(self, at, src, dst, send, recv, local):
        self.at, self.src, self.dst = at, src, dst
        f, j = at.f, at.j
        self.own = pltpu.make_async_copy(src, dst.at[f], local)
        self.first, self.later, self.arrivals = [], [], []
        if at.F == 4:
            nx = f + 1 - 2 * lax.rem(f, 2)
            ny = lax.rem(f + 2, 4)
            nd = lax.rem(nx + 2, 4)
            half = src.shape[0] // 2
            a, b = pl.ds(0, half), pl.ds(half, half)
            table = ((nx, a), (nx, b), (ny, a), (ny, b))
            for i, (to, rows) in enumerate(table):
                self.first.append(
                    remote(src.at[rows], dst.at[f, rows], send.at[i], recv.at[i], (j, to))
                )
                self.arrivals.append(
                    remote(src.at[rows], dst.at[to, rows], send.at[i], recv.at[i], (j, to))
                )
            for i, (of, rows, to) in ((4, (nx, a, ny)), (5, (ny, b, nx))):
                self.later.append(
                    remote(dst.at[of, rows], dst.at[of, rows], send.at[i], recv.at[i], (j, to))
                )
                self.arrivals.append(
                    remote(dst.at[nd, rows], dst.at[nd, rows], send.at[i], recv.at[i], (j, to))
                )
        else:
            for k in range(1, at.F):
                to, of = lax.rem(f + k, at.F), lax.rem(f + at.F - k, at.F)
                self.first.append(
                    remote(src, dst.at[f], send.at[k - 1], recv.at[k - 1], (j, to))
                )
                self.arrivals.append(
                    remote(src, dst.at[of], send.at[k - 1], recv.at[k - 1], (j, to))
                )

    def start(self):
        self.own.start()
        for copy in self.first:
            copy.start()

    def relay(self):
        if self.later:
            self.arrivals[0].wait_recv()
            self.later[0].start()
            self.arrivals[3].wait_recv()
            self.later[1].start()

    def arrived(self):
        for i, copy in enumerate(self.arrivals):
            if not (self.later and i in (0, 3)):
                copy.wait_recv()
        self.own.wait()

    def finish(self):
        for copy in self.first + self.later:
            copy.wait_send()


class TokenGather:
    @staticmethod
    def scratch(S):
        Q = S // 2
        return [pltpu.SemaphoreType.DMA((2 * Q,)), pltpu.SemaphoreType.DMA((2 * Q,)),
                pltpu.SemaphoreType.DMA((S,)), pltpu.SemaphoreType.DMA]

    def __init__(self, at, src, dst, send, share, recv, local, rows=None):
        self.at, self.src, self.dst, self.rows = at, src, dst, rows
        self.send, self.share, self.recv = send, share, recv
        self.own = pltpu.make_async_copy(src, self.place(at.j), local)

    def place(self, slot):
        return self.dst.at[slot] if self.rows is None else self.dst.at[slot, self.rows]

    def onward(self, slot, source, i, by):
        to = self.place(slot)
        return remote(
            source, to, self.send.at[i], self.recv.at[slot], (self.at.j + by, self.at.f)
        )

    def given(self, slot, source, i):
        to = self.place(slot)
        return remote(
            source, to, self.share.at[i], self.recv.at[slot], (self.at.partner, self.at.f)
        )

    def own_copies(self):
        at, j = self.at, self.at.j
        return (
            self.onward(j, self.src, 0, at.side), self.onward(j, self.src, at.Q, -at.side),
            self.given(j, self.src, 0),
        )

    def start(self):
        self.own.start()
        far, near, part = self.own_copies()
        far.start()

        @pl.when(self.at.end > 0)
        def _():
            near.start()

        part.start()

    def from_near(self, d):
        at = self.at
        slot = at.j - at.side * d
        here = self.place(slot)
        return self.onward(slot, here, d, at.side), self.given(slot, here, d)

    def from_far(self, d):
        at = self.at
        slot = at.j + at.side * d
        here = self.place(slot)
        return self.onward(slot, here, at.Q + d, -at.side), self.given(slot, here, at.Q + d)

    def near(self, d):
        if d > self.at.Q // 2 - 1:
            return

        @pl.when(self.at.end >= d)
        def _():
            onward, part = self.from_near(d)
            onward.wait_recv()
            onward.start()
            part.start()

    def far(self, d):
        @pl.when(self.at.end + d <= self.at.Q - 1)
        def _():
            onward, part = self.from_far(d)
            part.wait_recv()

            @pl.when(self.at.end > 0)
            def _():
                onward.start()

            part.start()

    def arrived(self):
        for q in range(self.at.Q):
            slot = 2 * q + 1 - self.at.c
            self.given(slot, self.place(slot), 0).wait_recv()
        self.own.wait()

    def finish(self):
        at, Q = self.at, self.at.Q
        far, near, part = self.own_copies()
        far.wait_send()

        @pl.when(at.end > 0)
        def _():
            near.wait_send()

        part.wait_send()
        for d in range(1, Q):
            if d <= Q // 2 - 1:

                @pl.when(at.end >= d)
                def _():
                    onward, part = self.from_near(d)
                    onward.wait_send()
                    part.wait_send()

            @pl.when(at.end + d <= Q - 1)
            def _():
                onward, part = self.from_far(d)

                @pl.when(at.end > 0)
                def _():
                    onward.wait_send()

                part.wait_send()


class GradReduce:
    @staticmethod
    def scratch(F, rows, n):
        return [pltpu.VMEM((F, rows, n), BF), pltpu.VMEM((F - 1, rows, n), BF),
                pltpu.SemaphoreType.DMA((F - 1,)), pltpu.SemaphoreType.DMA((F - 1,))]

    def __init__(self, at, left, right, extra, made, got, send, recv):
        self.at, self.left, self.right, self.extra = at, left, right, extra
        self.made, self.got, self.send, self.recv = made, got, send, recv
        self.n = right.shape[-1]
        self.rows = left.shape[-1] // at.F
        self.tile = next(t for t in (512, 384, 256, 128) if self.n % t == 0)

    def copy(self, k):
        at = self.at
        to = lax.rem(at.f + k, at.F)
        return remote(
            self.made.at[to], self.got.at[k - 1], self.send.at[k - 1], self.recv.at[k - 1],
            (at.j, to),
        )

    def start(self):
        at, rows = self.at, self.rows
        aligned = rows % 128 == 0
        for t in range(0, self.n, self.tile) if not aligned else ():
            cols = slice(t, t + self.tile)
            full = dot_tn(self.left[...], columns(self.right, cols)).astype(BF)
            for p in range(at.F):
                self.made[p, 0:rows, cols] = full[p * rows : (p + 1) * rows, :]
        for k in list(range(1, at.F)) + [0]:
            p = lax.rem(at.f + k, at.F)
            if aligned:
                block = columns(self.left, pl.ds(pl.multiple_of(p * rows, 128), rows))
                for t in range(0, self.n, self.tile):
                    cols = slice(t, t + self.tile)
                    made = dot_tn(block, columns(self.right, cols))
                    self.made[p, 0:rows, cols] = made.astype(BF)
            if callable(self.extra):
                self.made[p, rows:, :] = self.extra()
            elif self.extra is not None:
                self.made[p, rows : rows + self.extra.shape[1], :] = self.extra[p].astype(BF)
            if k:
                self.copy(k).start()

    def finish(self, store):
        at = self.at
        for k in range(1, at.F):
            self.copy(k).wait_recv()
        for t in range(0, self.n, self.tile):
            cols = slice(t, t + self.tile)
            total = self.made[at.f, :, cols].astype(F32)
            for k in range(1, at.F):
                total += self.got[k - 1, :, cols].astype(F32)
            store(t, self.tile, total.astype(BF))
        for k in range(1, at.F):
            self.copy(k).wait_send()


EXTRA = 16


def exchange(S, F, collective_id, grads=(), shards=(), tokens=(), split=False):
    operands, in_specs = [], []
    vmem = pl.BlockSpec(memory_space=pltpu.VMEM)
    outs, out_specs, scratch = [], [], []
    shapes = []
    for left, right, extra in grads:
        rows, n = left.shape[1] // F + (0 if extra is None else EXTRA), right.shape[1]
        operands += [left, right] + ([] if extra is None else [extra])
        scratch += GradReduce.scratch(F, rows, n)
        shapes.append((rows, n))
        if split:
            outs.append(jax.ShapeDtypeStruct((rows - EXTRA, n), BF))
            outs.append(jax.ShapeDtypeStruct((EXTRA, n), BF))
        else:
            outs.append(jax.ShapeDtypeStruct((rows, n), BF))
    out_specs += [vmem] * len(outs)
    for array in shards:
        operands.append(array)
        outs.append(jax.ShapeDtypeStruct((F,) + array.shape, BF))
        out_specs.append(pl.BlockSpec(memory_space=pl.ANY))
        scratch += ShardGather.scratch(F)
    for array in tokens:
        operands.append(array)
        outs.append(jax.ShapeDtypeStruct((S,) + array.shape, BF))
        out_specs.append(pl.BlockSpec(memory_space=pl.ANY))
        scratch += TokenGather.scratch(S)
    in_specs = [vmem] * len(operands)
    n_in, n_out = len(operands), len(outs)

    def kernel(*refs):
        ins, results, rest = list(refs[:n_in]), list(refs[n_in : n_in + n_out]), list(
            refs[n_in + n_out :]
        )
        take = lambda items, n: [items.pop(0) for _ in range(n)]
        at = Place(S, F)
        jobs, stores = [], []
        for (_, _, extra), (rows, n) in zip(grads, shapes):
            left, right = take(ins, 2)
            extra_ref = None if extra is None else take(ins, 1)[0]
            jobs.append(GradReduce(at, left, right, extra_ref, *take(rest, 4)))
            target = take(results, 1)[0]
            rider_ref = take(results, 1)[0] if split else None

            def store(t, width, value, target=target, rows=rows, rider_ref=rider_ref):
                if split:
                    target[:, t : t + width] = value[: rows - EXTRA]
                    rider_ref[:, t : t + width] = value[rows - EXTRA :]
                else:
                    target[:, t : t + width] = value

            stores.append(store)
        spreads = [
            ShardGather(at, take(ins, 1)[0], take(results, 1)[0], *take(rest, 3)) for _ in shards
        ]
        lines = [
            TokenGather(at, take(ins, 1)[0], take(results, 1)[0], *take(rest, 4)) for _ in tokens
        ]
        at.greet(bool(jobs or spreads), "line" if lines else "")
        for item in lines + spreads:
            item.start()
        for job in jobs:
            job.start()
        waiting = list(spreads)
        for d in range(1, at.Q) if lines else ():
            for item in lines:
                item.near(d)
                item.far(d)
            if waiting:
                waiting.pop(0).relay()
        for item in waiting:
            item.relay()
        for job, store in zip(jobs, stores):
            job.finish(store)
        for item in spreads + lines:
            item.arrived()
            item.finish()

    flops = sum(2 * l.shape[0] * l.shape[1] * r.shape[1] for l, r, _ in grads)
    moved = sum(o.size * 2 for o in outs)
    return pl.pallas_call(
        kernel,
        out_shape=tuple(outs),
        in_specs=in_specs,
        out_specs=tuple(out_specs),
        scratch_shapes=scratch,
        compiler_params=pltpu.CompilerParams(
            collective_id=collective_id, has_side_effects=True
        ),
        cost_estimate=pl.CostEstimate(
            flops=flops, bytes_accessed=20 * moved, transcendentals=0
        ),
    )(*operands)


LN_ROWS = 8


class Loads:
    def __init__(self, sources, buffers, sems):
        self.copies = [
            pltpu.make_async_copy(src, buf, sems.at[i])
            for i, (src, buf) in enumerate(zip(sources, buffers))
        ]
        self.buffers = buffers

    def start(self):
        for copy in self.copies:
            copy.start()

    def ready(self, *which):
        for i in which:
            self.copies[i].wait()


class LineSum:
    @staticmethod
    def scratch(S, t, d):
        Q = S // 2
        return [pltpu.VMEM((Q, t, d), BF), pltpu.VMEM((Q + 1, t, d), BF),
                pltpu.SemaphoreType.DMA((2 * Q,)), pltpu.SemaphoreType.DMA((2 * Q,)),
                pltpu.SemaphoreType.DMA((Q,)), pltpu.SemaphoreType.DMA((Q,))]

    def __init__(self, at, part, result, pair, got, s_line, r_line, s_pair, r_pair):
        self.at, self.part, self.result, self.pair, self.got = at, part, result, pair, got
        self.s_line, self.r_line, self.s_pair, self.r_pair = s_line, r_line, s_pair, r_pair

    def share(self, slot):
        at = self.at
        return remote(
            self.part.at[2 * slot + 1 - at.c], self.pair.at[slot], self.s_pair.at[slot],
            self.r_pair.at[slot], (at.partner, at.f),
        )

    def hop(self, slot, up, last):
        at = self.at
        i = slot + (1 - up) * at.Q
        into = slot + last * (at.Q - slot)
        return remote(
            self.pair.at[slot], self.got.at[into], self.s_line.at[i], self.r_line.at[i],
            (at.j + 4 * up - 2, at.f),
        )

    def last(self, slot, up):
        at = self.at
        return (1 - up) * (1 - (at.q - 1 - slot + at.Q - 1) // at.Q)

    def start(self):
        order = []
        for i in range(self.at.Q):
            for slot in (self.at.Q - 1 - i, i):
                if slot not in order:
                    order.append(slot)
        for slot in order:
            self.share(slot).start()

    def base(self, slot):
        self.share(slot).wait_recv()
        return self.part[2 * slot + self.at.c].astype(F32) + self.pair[slot].astype(F32)

    def pass_on(self, slot, up):
        at = self.at

        @pl.when((2 * up - 1) * (slot - at.q) > 0)
        def _():
            value = self.base(slot)
            self.hop(slot, up, 0).wait_recv()
            self.pair[slot] = (value + self.got[slot].astype(F32)).astype(BF)
            self.hop(slot, up, self.last(slot, up)).start()

    def ends(self, steps):
        at = self.at

        @pl.when(at.end == 0)
        def _():
            for i in steps:
                slot = at.low * (at.Q - 1 - i) + (1 - at.low) * i
                self.pair[slot] = self.base(slot).astype(BF)
                self.hop(slot, at.low, self.last(slot, at.low)).start()

    def near(self, i):
        at = self.at

        @pl.when(at.end > 0)
        def _():
            self.pass_on(at.low * (at.Q - 1 - i) + (1 - at.low) * i, at.low)

    def far(self, i):
        at = self.at
        self.pass_on((1 - at.low) * (at.Q - 1 - i) + at.low * i, 1 - at.low)

    def total(self):
        at = self.at
        self.result[...] = self.base(at.q)

        @pl.when(at.q > 0)
        def _():
            self.hop(at.q, 1, 0).wait_recv()
            self.result[...] += self.got[at.q].astype(F32)

        @pl.when(at.q < at.Q - 1)
        def _():
            self.hop(at.q, 0, 1).wait_recv()
            self.result[...] += self.got[at.Q].astype(F32)

    def finish(self):
        q = self.at.q
        for slot in range(self.at.Q):
            self.share(slot).wait_send()

            @pl.when(q < slot)
            def _():
                self.hop(slot, 1, 0).wait_send()

            @pl.when(q > slot)
            def _():
                self.hop(slot, 0, 0).wait_send()


class VectorSum:
    @staticmethod
    def scratch(S, F, w):
        return [
            pltpu.VMEM((F, LN_ROWS, w), F32),
            pltpu.VMEM((F, LN_ROWS, w), F32),
            pltpu.VMEM((S, LN_ROWS, w), F32),
            pltpu.SemaphoreType.DMA((F - 1,)),
            pltpu.SemaphoreType.DMA((F,)),
            pltpu.SemaphoreType.DMA((S - 1,)),
            pltpu.SemaphoreType.DMA((S,)),
        ]

    def __init__(self, at, made, by_shard, by_seq, s_f, r_f, s_s, r_s):
        self.at, self.made, self.by_shard, self.by_seq = at, made, by_shard, by_seq
        j, f, S, F = at.j, at.f, at.S, at.F
        self.over_f, self.over_s = [], []
        for k in range(1, F):
            to, of = lax.rem(f + k, F), lax.rem(f + F - k, F)
            self.over_f.append(
                (remote(made.at[to], by_shard.at[f], s_f.at[k - 1], r_f.at[f], (j, to)),
                 remote(made.at[to], by_shard.at[of], s_f.at[k - 1], r_f.at[of], (j, to)))
            )
        for k in range(1, S):
            to, of = lax.rem(j + k, S), lax.rem(j + S - k, S)
            self.over_s.append(
                (remote(by_seq.at[j], by_seq.at[j], s_s.at[k - 1], r_s.at[j], (to, f)),
                 remote(by_seq.at[j], by_seq.at[of], s_s.at[k - 1], r_s.at[of], (to, f)))
            )

    def start(self):
        for copy, _ in self.over_f:
            copy.start()
        self.by_shard[self.at.f] = self.made[self.at.f]

    def turn_to_seq(self):
        for _, arrival in self.over_f:
            arrival.wait_recv()
        total = self.by_shard[0]
        for p in range(1, self.at.F):
            total += self.by_shard[p]
        self.by_seq[self.at.j] = total
        for copy, _ in self.over_s:
            copy.start()

    def finish(self, result):
        for _, arrival in self.over_s:
            arrival.wait_recv()
        total = self.by_seq[0]
        for p in range(1, self.at.S):
            total += self.by_seq[p]
        result[...] = total
        for copy, _ in self.over_f + self.over_s:
            copy.wait_send()


def closing(
    S, F, collective_id, tok, normed, upstream, grad_mixed, attended, activated, grad_pre,
    w_dense, w_down, w_qkv, w_up, extra, standard, with_dense,
):
    L, D = normed.shape
    w = D // F
    chunk = 3 * LANES
    pairs = grad_mixed.shape[1] // chunk
    grads = [(D // F + EXTRA, chunk)] * pairs
    if with_dense:
        grads.append((attended.shape[1] // F, D))
    big = [normed, grad_mixed, attended, activated, w_dense, w_down, grad_pre, w_qkv, w_up]
    if with_dense:
        big.append(upstream)
    tile = 512
    m = len(grads)

    def kernel(*refs):
        refs = list(refs)
        take = lambda n: [refs.pop(0) for _ in range(n)]
        at = Place(S, F)
        sources = take(len(big))
        extra_ref, standard_ref = take(2)
        branches, normed_sum, ln_out = take(3)
        gathered = take(m)
        loads = Loads(sources, take(len(big)), take(1)[0])
        x, gm, att, act, wd, wdn, gp, wq, wu = loads.buffers[:9]
        jobs, packed, lines = [], [], []
        for i in range(pairs):
            cols = slice(i * chunk, (i + 1) * chunk)
            jobs.append(GradReduce(at, x, gm.at[:, cols], extra_ref.at[:, :, cols], *take(4)))
        if with_dense:
            jobs.append(GradReduce(at, att, loads.buffers[9], None, *take(4)))
        for i in range(m):
            packed.append(take(1)[0])
            lines.append(TokenGather(at, packed[i], gathered[i], *take(4)))
        parts = take(2)
        sums = [
            LineSum(at, part, res, *take(6)) for part, res in zip(parts, (branches, normed_sum))
        ]
        vectors = VectorSum(at, *take(7))
        loads.start()
        at.greet(True, "all")
        loads.ready(0, 1)
        for job in jobs[:pairs]:
            job.start()
        loads.ready(2)
        if with_dense:
            loads.ready(9)
            jobs[-1].start()
        loads.ready(3, 4, 5)

        @pl.loop(0, D // tile)
        def _(i):
            cols = pl.ds(pl.multiple_of(i * tile, tile), tile)
            made = dot(att[...], wd[:, cols]) + dot(act[...], wdn[:, cols])
            parts[0][:, :, cols] = made.astype(BF).reshape(S, tok, tile)

        sums[0].start()
        sums[0].ends([0])
        loads.ready(6, 7, 8)

        @pl.loop(0, D // tile)
        def _(i):
            rows = pl.ds(pl.multiple_of(i * tile, tile), tile)
            made = dot_nt(gm[...], wq[rows, :]) + dot_nt(gp[...], wu[rows, :])
            parts[1][:, :, rows] = made.astype(BF).reshape(S, tok, tile)

        sums[1].start()
        sums[1].ends([0])

        def reduced(i):
            def store(t, wide, value):
                packed[i][:, t : t + wide] = value

            jobs[i].finish(store)
            lines[i].start()

        for i in range(m):
            reduced(i)
            if i < 2:
                sums[i].near(0)
            lines[i].far(1)
        for i in range(m, 2):
            sums[i].near(0)
        for item in sums:
            item.ends(range(1, at.Q - 1))
        for i in range(max(m, 2)):
            if i < 2:
                sums[i].far(0)
            if i < m:
                lines[i].near(1)
        for step in range(1, at.Q - 1):
            for line in lines:
                line.far(step + 1)
            for item in sums:
                item.near(step)
            for item in sums:
                item.far(step)
            for line in lines:
                line.near(step + 1)
        for item in sums:
            item.total()
        grad_normed = normed_sum[...]
        both = jnp.concatenate(
            [
                jnp.sum(grad_normed * standard_ref[...], axis=0, keepdims=True),
                jnp.sum(grad_normed, axis=0, keepdims=True),
                jnp.zeros((LN_ROWS - 2, D), F32),
            ],
            axis=0,
        )
        for p in range(F):
            vectors.made[p] = both[:, p * w : (p + 1) * w]
        vectors.start()
        vectors.turn_to_seq()
        for line in lines:
            line.arrived()
            line.finish()
        vectors.finish(ln_out)
        for item in sums:
            item.finish()

    vmem = pl.BlockSpec(memory_space=pltpu.VMEM)
    anywhere = pl.BlockSpec(memory_space=pl.ANY)
    scratch = [pltpu.VMEM(a.shape, a.dtype) for a in big]
    scratch.append(pltpu.SemaphoreType.DMA((len(big),)))
    for rows, n in grads:
        scratch += GradReduce.scratch(F, rows, n)
    for rows, n in grads:
        scratch.append(pltpu.VMEM((rows, n), BF))
        scratch += TokenGather.scratch(S)
    scratch += [pltpu.VMEM((S, tok, D), BF)] * 2
    scratch += LineSum.scratch(S, tok, D) * 2
    scratch += VectorSum.scratch(S, F, w)
    full = jax.ShapeDtypeStruct((tok, D), F32)
    return pl.pallas_call(
        kernel,
        out_shape=(full, full, jax.ShapeDtypeStruct((LN_ROWS, w), F32))
        + tuple(jax.ShapeDtypeStruct((S, rows, n), BF) for rows, n in grads),
        in_specs=[anywhere] * len(big) + [vmem] * 2,
        out_specs=(vmem,) * 3 + (anywhere,) * m,
        scratch_shapes=scratch,
        compiler_params=pltpu.CompilerParams(
            collective_id=collective_id, has_side_effects=True,
            vmem_limit_bytes=67_000_000 if L > 1024 else None,
        ),
        cost_estimate=pl.CostEstimate(
            flops=6 * L * D * (grad_mixed.shape[1] + activated.shape[1]),
            bytes_accessed=80 * L * D,
            transcendentals=0,
        ),
    )(*big, extra, standard)


def attend_and_close(
    S, F, collective_id, tok, normed, upstream, feed_out, feed_gn, w_dense, w_qkv, rest_up, tables,
    seg_col, seg_row, bias, standard, inv_std, tokens, cotangent, gain, out_bias,
):
    L, D = S * tok, normed.shape[2]
    w = D // F
    chunk = 3 * LANES
    pairs = w_qkv.shape[1] // chunk
    rows_att = 256
    grads = [(D // F + EXTRA, chunk)] * pairs + [(pairs * LANES // F, D)]
    m = len(grads)
    big = [normed, upstream, w_qkv, w_dense, feed_out, feed_gn]
    small = [*tables, seg_col, seg_row, bias, standard, inv_std, tokens, cotangent, gain, out_bias, rest_up]
    tile = 512
    late = rest_up.shape[0]

    def kernel(*refs):
        refs = list(refs)
        take = lambda n: [refs.pop(0) for _ in range(n)]
        at = Place(S, F)
        sources = take(len(big))
        cos, low, high, seg_c, seg_r, bias_ref, standard_ref, inv_ref = take(8)
        tok_ref, cot_ref, gain_ref, out_bias_ref, up_ref = take(5)
        out_ref, grad_ref, ln_out, all_up = take(4)
        gathered = take(m)
        branches, normed_sum = take(2)
        loads = Loads(sources, take(len(big)), take(1)[0])
        x, g, wq, wd, out_part, gn_part = loads.buffers
        gm, att, proj, gatt, qs, ks, vs, dk, dv = take(9)
        ones = jnp.ones((16, L), BF)
        jobs, lines = [], []
        for i in range(pairs):
            cols = slice(i * chunk, (i + 1) * chunk)
            total_row = lambda cols=cols: dot(ones, gm[:, cols]).astype(BF)
            jobs.append(GradReduce(at, x, gm.at[:, cols], total_row, *take(4)))
        jobs.append(GradReduce(at, att, g, None, *take(4)))
        for i in range(m):
            lines.append(TokenGather(at, jobs[i].made.at[at.f], gathered[i], *take(4)))
        ups = [
            TokenGather(at, up_ref.at[i], all_up.at[i], *take(4)) for i in range(late)
        ]
        parts = [gn_part, out_part]
        sums = [
            LineSum(at, part, res, *take(6)) for part, res in zip(parts, (normed_sum, branches))
        ]
        vectors = VectorSum(at, *take(7))
        loads.start()
        at.greet(True, "all")
        for up in ups:
            up.start()
        loads.ready(0, 1, 2, 3)

        @pl.loop(0, pairs)
        def _(p):
            cols = pl.ds(pl.multiple_of(p * chunk, LANES), chunk)
            lanes = pl.ds(pl.multiple_of(p * LANES, LANES), LANES)

            @pl.loop(0, L // rows_att)
            def _(i):
                slots = pl.ds(i * (rows_att // tok), rows_att // tok)
                rows = pl.ds(pl.multiple_of(i * rows_att, rows_att), rows_att)
                block = x[slots].reshape(rows_att, D)
                proj[rows, :] = dot(block, wq[:, cols]) + bias_ref[:, cols]
                block = g[slots].reshape(rows_att, D)
                gatt[rows, :] = dot_nt(block, wd[lanes, :]).astype(BF)

            def during(pair, *steps):
                @pl.when(p == pair)
                def _():
                    for step in steps:
                        step()

            def serve(i, d):
                return lambda: (ups[i].near(d), ups[i].far(d))

            during(0, serve(0, 1))
            during(1, serve(0, 2))

            def pause(i):
                if i == 3:
                    during(0, serve(1, 1))
                    during(1, serve(1, 2))
                if i == 2:
                    during(0, *(serve(k, 1) for k in range(2, late)))
                    during(1, *(serve(k, 2) for k in range(2, late)))

            attention_kernel(
                rows_att, proj, gatt, cos, low, high, seg_c, seg_r, att.at[:, lanes],
                gm.at[:, cols], qs, ks, vs, dk, dv, pause,
            )
            during(0, jobs[0].start)

        loads.ready(5)

        @pl.loop(0, D // tile)
        def _(i):
            rows = pl.ds(pl.multiple_of(i * tile, tile), tile)
            made = columns(gn_part, rows).astype(F32) + dot_nt(gm[...], wq[rows, :])
            gn_part[:, :, rows] = made.astype(BF).reshape(S, tok, tile)

        sums[0].start()
        sums[0].ends([0])
        loads.ready(4)

        @pl.loop(0, D // tile)
        def _(i):
            cols = pl.ds(pl.multiple_of(i * tile, tile), tile)
            made = columns(out_part, cols).astype(F32) + dot(att[...], wd[:, cols])
            out_part[:, :, cols] = made.astype(BF).reshape(S, tok, tile)

        sums[1].start()
        sums[1].ends([0])
        jobs[1].start()

        def reduced(i):
            def store(t, wide, value):
                jobs[i].made[at.f, :, t : t + wide] = value

            jobs[i].finish(store)
            lines[i].start()

        for job in jobs[2:]:
            job.start()
        reduced(0)
        for d in range(3, at.Q):
            for up in ups:
                up.near(d)
                up.far(d)
        lines[0].far(1)

        for item in sums:
            item.ends([1])
        for i in range(m):
            if i:
                reduced(i)
            if i < 2:
                sums[i].near(0)
            if i:
                lines[i].far(1)
        for item in sums:
            item.ends(range(2, at.Q - 1))
        for i in range(m):
            if i < 2:
                sums[i].far(0)
            lines[i].near(1)
        for step in range(1, at.Q - 1):
            for line in lines:
                line.far(step + 1)
            for item in sums:
                item.near(step)
            for item in sums:
                item.far(step)
            for line in lines:
                line.near(step + 1)
        sums[0].total()
        grad_normed, standard = normed_sum[...], standard_ref[...]
        both = jnp.concatenate(
            [
                jnp.sum(grad_normed * standard, axis=0, keepdims=True),
                jnp.sum(grad_normed, axis=0, keepdims=True),
                jnp.zeros((LN_ROWS - 2, D), F32),
            ],
            axis=0,
        )
        for p in range(F):
            vectors.made[p] = both[:, p * w : (p + 1) * w]
        vectors.start()
        scaled = grad_normed * gain_ref[...]
        turned = (
            scaled
            - jnp.mean(scaled, axis=-1, keepdims=True)
            - standard * jnp.mean(scaled * standard, axis=-1, keepdims=True)
        )
        grad_ref[...] = cot_ref[...].astype(F32) + inv_ref[:, 0:1] * turned
        vectors.turn_to_seq()
        sums[1].total()
        out_ref[...] = (tok_ref[...].astype(F32) + branches[...] + out_bias_ref[...]).astype(BF)
        for line in ups + lines:
            line.arrived()
            line.finish()
        vectors.finish(ln_out)
        for item in sums:
            item.finish()

    vmem = pl.BlockSpec(memory_space=pltpu.VMEM)
    anywhere = pl.BlockSpec(memory_space=pl.ANY)
    scratch = [pltpu.VMEM((tok, D), F32)] * 2
    scratch += [pltpu.VMEM(a.shape, a.dtype) for a in big]
    scratch.append(pltpu.SemaphoreType.DMA((len(big),)))
    scratch += [
        pltpu.VMEM((L, pairs * chunk), BF),
        pltpu.VMEM((L, pairs * LANES), BF),
        pltpu.VMEM((L, chunk), F32),
    ]
    scratch += [pltpu.VMEM((L, LANES), BF)] * 4 + [pltpu.VMEM((L, LANES), F32)] * 2
    for rows, n in grads:
        scratch += GradReduce.scratch(F, rows, n)
    scratch += TokenGather.scratch(S) * m
    scratch += TokenGather.scratch(S) * late
    scratch += LineSum.scratch(S, tok, D) * 2
    scratch += VectorSum.scratch(S, F, w)
    full = jax.ShapeDtypeStruct((tok, D), F32)
    return pl.pallas_call(
        kernel,
        out_shape=(
            jax.ShapeDtypeStruct((tok, D), BF), full, jax.ShapeDtypeStruct((LN_ROWS, w), F32),
            jax.ShapeDtypeStruct((late, S) + rest_up.shape[1:], BF),
        )
        + tuple(jax.ShapeDtypeStruct((S, rows, n), BF) for rows, n in grads),
        in_specs=[anywhere] * len(big) + [vmem] * len(small),
        out_specs=(vmem,) * 3 + (anywhere,) * (1 + m),
        scratch_shapes=scratch,
        compiler_params=pltpu.CompilerParams(
            collective_id=collective_id, has_side_effects=True, vmem_limit_bytes=67_000_000
        ),
        cost_estimate=pl.CostEstimate(
            flops=10 * L * D * pairs * chunk,
            bytes_accessed=100 * L * D,
            transcendentals=pairs * L * L,
        ),
    )(*big, *small)


class CornerReduce:
    @staticmethod
    def scratch(rows, n):
        return [pltpu.VMEM((4, rows, n), BF), pltpu.VMEM((3, rows, n), BF),
                pltpu.SemaphoreType.DMA((3,)), pltpu.SemaphoreType.DMA((3,))]

    def __init__(self, at, axis, made, got, send, recv):
        f = at.f
        nx, ny = f + 1 - 2 * lax.rem(f, 2), lax.rem(f + 2, 4)
        self.at, self.made, self.got = at, made, got
        self.one, self.two = (nx, ny) if axis == 0 else (ny, nx)
        self.far = lax.rem(nx + 2, 4)
        self.copies = [
            remote(made.at[block], got.at[i], send.at[i], recv.at[i], (at.j, to))
            for i, (block, to) in enumerate(
                ((self.far, self.one), (self.one, self.one), (self.two, self.two))
            )
        ]

    def send(self):
        self.copies[0].start()
        self.copies[1].start()

    def make(self, make, send):
        for p in (self.far, self.one, self.two, self.at.f):
            make(p)
            if send and p is self.one:
                self.send()

    def middle(self):
        self.copies[0].wait_recv()
        block = self.made[self.two].astype(F32) + self.got[0].astype(F32)
        self.made[self.two] = block.astype(BF)
        self.copies[2].start()

    def total(self):
        self.copies[1].wait_recv()
        self.copies[2].wait_recv()
        total = self.made[self.at.f].astype(F32) + self.got[1].astype(F32)
        return (total + self.got[2].astype(F32)).astype(BF)

    def finish(self):
        for copy in self.copies:
            copy.wait_send()


SMALL = 48
CHUNKS = 4


def opening(
    S, collective_id, tok, small, tokens, cotangent, fc1_weight, fc2_weight, qkv_weight,
    dense_weight,
):
    F, Q, L = 4, S // 2, tok * S
    D, ff = tokens.shape[1], fc1_weight.shape[1]
    rows_d, cols_up = D // F, ff // S
    w_ff = cols_up // F
    pairs = HEADS // S // 2
    wide = 3 * pairs * LANES
    dense_rows = HEAD * HEADS // (F * S)
    half = S // 2
    n_down, n_up = D // CHUNKS, cols_up // CHUNKS
    lead = {}
    at_row = 0
    for name, n in (
        ("gain", rows_d), ("bias", rows_d), ("qkv", 3 * rows_d), ("dense", rows_d),
        ("up", ff // F), ("down", rows_d),
    ):
        lead[name] = (at_row, n // 128)
        at_row += n // 128

    def kernel(*refs):
        refs = list(refs)
        take = lambda n: [refs.pop(0) for _ in range(n)]
        (small_in, tok_in, cot_in, up_in, down_in, qkv_in, dense_in) = take(7)
        (o_normed, o_out, o_gn, o_g, o_qkv, o_dense, o_alldown, o_allup, o_piece,
         o_vec, o_small, o_std, o_inv) = take(13)
        at = Place(S, F)
        j, f = at.j, at.f
        x_own, g_own, n_own, up_own, down_own, dense_own, qkv_raw, qkv_own = take(8)
        normed, g, w_up, w_down, act, gp, slope, part_out, part_gn = take(9)
        small_all, pieces = take(2)
        load_sem, save_sem, s_small, r_small = take(4)
        copies = []

        def load(src, dst):
            copy = pltpu.make_async_copy(src, dst, load_sem.at[len(copies)])
            copies.append(copy)
            copy.start()
            return copy

        for p in range(F):
            load(up_in.at[:, pl.ds(pl.multiple_of((p * S + j) * w_ff, w_ff), w_ff)],
                 up_own.at[:, p * w_ff : (p + 1) * w_ff])
        load(tok_in, x_own)
        load(cot_in, g_own)
        load(down_in.at[pl.ds(pl.multiple_of(j * w_ff, w_ff), w_ff)], down_own)
        load(dense_in.at[pl.ds(pl.multiple_of(j * dense_rows, dense_rows), dense_rows)],
             dense_own)
        for i in range(3 * pairs):
            for which in range(2):
                block = (i % 3) * F * half + (2 * (i // 3) + which) * half + j // 2
                load(qkv_in.at[:, pl.ds(pl.multiple_of(block * LANES, LANES), LANES)],
                     qkv_raw.at[2 * i + which])

        gathers = [
            ShardGather(at, src, dst, *take(3))
            for src, dst in (
                (up_own, w_up), (down_own, w_down), (qkv_own, o_qkv), (dense_own, o_dense),
            )
        ]
        line_n = TokenGather(at, n_own, normed, *take(4))
        line_g = TokenGather(at, g_own, g, *take(4))
        reduce_down = [CornerReduce(at, i % 2, *take(4)) for i in range(CHUNKS)]
        reduce_up = [CornerReduce(at, i % 2, *take(4)) for i in range(CHUNKS)]
        lines = [
            TokenGather(at, pieces.at[i], o_alldown.at[i], *take(4)) for i in range(CHUNKS)
        ]
        lines.append(TokenGather(at, reduce_up[0].made.at[f], o_allup.at[0], *take(4)))
        at.greet(True, "line")
        smalls = []
        for k in range(1, F):
            to, of = lax.rem(f + k, F), lax.rem(f + F - k, F)
            smalls.append(
                (remote(small_in, small_all.at[f], s_small.at[k - 1], r_small.at[k - 1], (j, to)),
                 remote(small_in, small_all.at[of], s_small.at[k - 1], r_small.at[k - 1], (j, to)))
            )
        for copy, _ in smalls:
            copy.start()
        small_all[f] = small_in[...]
        for p in range(F):
            copies[p].wait()
        gathers[0].start()
        copies[F + 2].wait()
        gathers[1].start()
        copies[F + 3].wait()
        copies[F + 1].wait()
        line_g.start()

        def row_of(name):
            first, n = lead[name]
            return jnp.concatenate(
                [small_all[p, first + r : first + r + 1, :] for p in range(F) for r in range(n)],
                axis=1,
            )

        copies[F].wait()
        values = x_own[...].astype(F32)
        centre = jnp.mean(values, axis=-1, keepdims=True)
        values = values - centre
        inv_std = lax.rsqrt(jnp.mean(values * values, axis=-1, keepdims=True) + EPS)
        values = values * inv_std
        o_std[...] = values
        o_inv[...] = jnp.broadcast_to(inv_std, (tok, 128))
        for _, arrival in smalls:
            arrival.wait_recv()
        n_own[...] = (values * row_of("gain") + row_of("bias")).astype(BF)
        line_n.start()

        for d in range(1, Q - 1):
            line_g.near(d)
            line_g.far(d)
            if d == 1:
                gathers[0].relay()
            line_n.near(d)
            line_n.far(d)
            if d == 1:
                gathers[1].relay()
                gathers[3].start()
        odd = lax.rem(j, 2) == 1
        lane = lax.broadcasted_iota(jnp.int32, (rows_d, LANES), 1)
        for copy in copies[F + 4 :]:
            copy.wait()
        for i in range(3 * pairs):
            first, second = qkv_raw[2 * i].astype(F32), qkv_raw[2 * i + 1].astype(F32)
            first = jnp.where(odd, pltpu.roll(first, HEAD, 1), first)
            second = jnp.where(odd, second, pltpu.roll(second, HEAD, 1))
            qkv_own[:, i * LANES : (i + 1) * LANES] = jnp.where(
                lane < HEAD, first, second
            ).astype(BF)
        line_g.far(Q - 1)
        gathers[3].relay()
        line_n.far(Q - 1)
        line_n.arrived()
        gathers[0].arrived()
        saves = []

        def save(src, dst):
            copy = pltpu.make_async_copy(src, dst, save_sem.at[len(saves)])
            saves.append(copy)
            copy.start()

        save(normed, o_normed)
        up_first = lead["up"][0]

        @pl.loop(0, F)
        def _(p):
            cols = pl.ds(pl.multiple_of(p * w_ff, w_ff), w_ff)
            u = jnp.concatenate(
                [
                    small_all[p, pl.ds(up_first + j * (w_ff // 128) + r, 1), :]
                    for r in range(w_ff // 128)
                ],
                axis=1,
            )
            for s in range(F):
                part = normed[:, :, s * rows_d : (s + 1) * rows_d].reshape(L, rows_d)
                u = u + dot(part, w_up[s, :, cols])
            square = u * u
            root = 0.7978845608028654
            t = jnp.tanh(root * (u + 0.044715 * (square * u)))
            act[:, cols] = ((0.5 * u) * (1.0 + t)).astype(BF)
            slope[:, cols] = 0.5 * (1.0 + t) + (0.5 * u) * (1.0 - t * t) * (
                root * (1.0 + 3 * 0.044715 * square)
            )

        line_g.arrived()
        save(g, o_g)
        ones = jnp.ones((EXTRA, L), BF)

        def make_down(c):
            cols = slice(c * n_down, (c + 1) * n_down)

            def make(p):
                block = act[:, pl.ds(pl.multiple_of(p * w_ff, w_ff), w_ff)]
                right = g[:, :, cols].reshape(L, n_down)
                reduce_down[c].made[p, 0:w_ff, :] = dot_tn(block, right).astype(BF)
                if c == 0:
                    mine = g[:, :, pl.ds(pl.multiple_of(p * rows_d, rows_d), rows_d)]
                    term = dot(ones, mine.reshape(L, rows_d))
                    reduce_down[c].made[p, w_ff:, :] = term.astype(BF)

            return make

        def make_up(c):
            cols = slice(c * n_up, (c + 1) * n_up)

            def make(p):
                block = normed[:, :, pl.ds(pl.multiple_of(p * rows_d, rows_d), rows_d)]
                made = dot_tn(block.reshape(L, rows_d), gp[:, cols])
                reduce_up[c].made[p, 0:rows_d, :] = made.astype(BF)
                if c == 0:
                    term = dot(ones, gp[:, pl.ds(pl.multiple_of(p * w_ff, w_ff), w_ff)])
                    reduce_up[c].made[p, rows_d:, :] = term.astype(BF)

            return make

        for c in range(CHUNKS):
            reduce_down[c].make(make_down(c), c < 2)
        gathers[1].arrived()

        @pl.loop(0, F)
        def _(p):
            cols = pl.ds(pl.multiple_of(p * w_ff, w_ff), w_ff)
            grad_act = dot_nt(g[...].reshape(L, D), w_down[p])
            gp[:, cols] = (grad_act * slope[:, cols]).astype(BF)


        def end_down(c):
            total = reduce_down[c].total()
            pieces[c] = total[0:w_ff, :]
            if c == 0:
                o_vec[...] = total[w_ff:, :]
            lines[c].start()

        def end_up(c):
            total = reduce_up[c].total()
            if c:
                o_piece[c - 1] = total
            else:
                reduce_up[0].made[f] = total
                lines[CHUNKS].start()

        def serve(c, d):
            lines[c].near(d)
            lines[c].far(d)

        def feed_out(i):
            cols = slice(i * rows_d, (i + 1) * rows_d)
            made = dot(act[:, 0:w_ff], w_down[0, :, cols])
            for p in range(1, F):
                made = made + dot(act[:, p * w_ff : (p + 1) * w_ff], w_down[p, :, cols])
            part_out[:, :, cols] = made.astype(BF).reshape(S, tok, rows_d)

        def feed_gn(i):
            made = dot_nt(gp[...], w_up[i])
            cols = slice(i * rows_d, (i + 1) * rows_d)
            part_gn[:, :, cols] = made.astype(BF).reshape(S, tok, rows_d)

        for c in (0, 1):
            reduce_down[c].middle()
        for c in (2, 3):
            reduce_down[c].send()
        for c in (0, 1):
            reduce_up[c].make(make_up(c), False)
        for c in (0, 1):
            end_down(c)
        for c in (2, 3):
            reduce_up[c].make(make_up(c), False)
        serve(0, 1)
        for c in (2, 3):
            reduce_down[c].middle()
        for c in (0, 1):
            reduce_up[c].send()
        serve(1, 1)
        feed_out(0)
        feed_out(1)
        for c in (2, 3):
            end_down(c)
        feed_out(2)
        serve(0, 2)
        for c in (0, 1):
            reduce_up[c].middle()
        for c in (2, 3):
            reduce_up[c].send()
        gathers[2].start()
        serve(1, 2)
        feed_out(3)
        save(part_out, o_out)
        serve(2, 1)
        for c in (0, 1):
            end_up(c)
        feed_gn(0)
        serve(3, 1)
        feed_gn(1)
        for d in range(3, Q):
            serve(0, d)
            serve(1, d)
        for c in (2, 3):
            reduce_up[c].middle()
        feed_gn(2)
        serve(2, 2)
        feed_gn(3)
        save(part_gn, o_gn)
        serve(3, 2)
        serve(CHUNKS, 1)
        gathers[2].relay()
        for c in (2, 3):
            end_up(c)
        for d in range(3, Q):
            serve(2, d)
            serve(3, d)
        for d in range(2, Q):
            serve(CHUNKS, d)
        o_small[...] = small_all[...]
        for copy, _ in smalls:
            copy.wait_send()
        for gather in gathers[2:]:
            gather.arrived()
        for line in lines:
            line.arrived()
        for item in [line_n, line_g] + lines + gathers + reduce_down + reduce_up:
            item.finish()
        for copy in saves:
            copy.wait()

    vmem = pl.BlockSpec(memory_space=pltpu.VMEM)
    anywhere = pl.BlockSpec(memory_space=pl.ANY)
    out = lambda shape, dtype=BF: jax.ShapeDtypeStruct(shape, dtype)
    scratch = [
        pltpu.VMEM(shape, dtype)
        for shape, dtype in (
            ((tok, D), BF), ((tok, D), BF), ((tok, D), BF), ((rows_d, cols_up), BF),
            ((w_ff, D), BF), ((dense_rows, D), BF), ((6 * pairs, rows_d, LANES), BF),
            ((rows_d, wide), BF),
            ((S, tok, D), BF), ((S, tok, D), BF), ((F, rows_d, cols_up), BF), ((F, w_ff, D), BF),
            ((L, cols_up), BF), ((L, cols_up), BF), ((L, cols_up), F32),
            ((S, tok, D), BF), ((S, tok, D), BF),
            ((F, SMALL, 128), F32), ((CHUNKS, w_ff, n_down), BF),
        )
    ]
    scratch += [
        pltpu.SemaphoreType.DMA((F + 4 + 6 * pairs,)), pltpu.SemaphoreType.DMA((6,)),
        pltpu.SemaphoreType.DMA((F - 1,)), pltpu.SemaphoreType.DMA((F - 1,)),
    ]
    for _ in range(4):
        scratch += ShardGather.scratch(F)
    for _ in range(2):
        scratch += TokenGather.scratch(S)
    for c in range(CHUNKS):
        scratch += CornerReduce.scratch(w_ff + (0 if c else EXTRA), n_down)
    for c in range(CHUNKS):
        scratch += CornerReduce.scratch(rows_d + (0 if c else EXTRA), n_up)
    for _ in range(CHUNKS + 1):
        scratch += TokenGather.scratch(S)
    return pl.pallas_call(
        kernel,
        out_shape=(
            out((S, tok, D)), out((S, tok, D)), out((S, tok, D)), out((S, tok, D)),
            out((F, rows_d, wide)), out((F, dense_rows, D)),
            out((CHUNKS, S, w_ff, n_down)), out((1, S, rows_d + EXTRA, n_up)),
            out((CHUNKS - 1, rows_d, n_up)),
            out((EXTRA, n_down)), out((F, SMALL, 128), F32),
            out((tok, D), F32), out((tok, 128), F32),
        ),
        in_specs=[vmem] + [anywhere] * 6,
        out_specs=(anywhere,) * 8 + (vmem,) * 5,
        scratch_shapes=scratch,
        compiler_params=pltpu.CompilerParams(
            collective_id=collective_id, has_side_effects=True, vmem_limit_bytes=67_000_000
        ),
        cost_estimate=pl.CostEstimate(
            flops=8 * L * D * cols_up, bytes_accessed=200 * L * D, transcendentals=L * cols_up
        ),
    )(small, tokens, cotangent, fc1_weight, fc2_weight, qkv_weight, dense_weight)


def half_lanes(first, second, odd):
    lane = lax.broadcasted_iota(jnp.int32, first.shape, 1)
    if odd:
        first = pltpu.roll(first, HEAD, 1)
    else:
        second = pltpu.roll(second, HEAD, 1)
    return jnp.where(lane < HEAD, first, second)


def pick_qkv(weight, j, F, S, pairs):
    rows = weight.shape[0]
    per_shard = S // 2

    def kernel(j_ref, first, second, out):
        a, b = first[...].astype(F32), second[...].astype(F32)

        @pl.when(j_ref[0] % 2 == 0)
        def _():
            out[...] = half_lanes(a, b, 0).astype(BF)

        @pl.when(j_ref[0] % 2 == 1)
        def _():
            out[...] = half_lanes(a, b, 1).astype(BF)

    def column(which):
        return lambda i, j_ref: (
            0, (i % 3) * F * per_shard + (2 * (i // 3) + which) * per_shard + j_ref[0] // 2
        )

    return pl.pallas_call(
        kernel,
        grid_spec=pltpu.PrefetchScalarGridSpec(
            num_scalar_prefetch=1,
            grid=(3 * pairs,),
            in_specs=[pl.BlockSpec((rows, LANES), column(0)), pl.BlockSpec((rows, LANES), column(1))],
            out_specs=pl.BlockSpec((rows, LANES), lambda i, j_ref: (0, i)),
        ),
        out_shape=jax.ShapeDtypeStruct((rows, 3 * pairs * LANES), BF),
    )(j[None].astype(jnp.int32), weight, weight)


def pick_up(weight, j, F, S):
    rows, ff = weight.shape
    w = ff // (F * S)
    if w % LANES:
        split = weight.reshape(rows, F, S, w)
        return lax.dynamic_index_in_dim(split, j, 2, keepdims=False).reshape(rows, F * w)

    def kernel(j_ref, src, out):
        out[...] = src[...]

    return pl.pallas_call(
        kernel,
        grid_spec=pltpu.PrefetchScalarGridSpec(
            num_scalar_prefetch=1,
            grid=(F,),
            in_specs=[pl.BlockSpec((rows, w), lambda i, j_ref: (0, i * S + j_ref[0]))],
            out_specs=pl.BlockSpec((rows, w), lambda i, j_ref: (0, i)),
        ),
        out_shape=jax.ShapeDtypeStruct((rows, F * w), BF),
    )(j[None].astype(jnp.int32), weight)


def unpack_qkv(gathered, rows, S):
    width = S * HEAD
    pairs = len(gathered)

    def kernel(*refs):
        out = refs[pairs]
        for p in range(pairs):
            for half in range(2):
                for z in range(S // 2):
                    a, b = refs[p][2 * z].astype(F32), refs[p][2 * z + 1].astype(F32)
                    at = (2 * p + half) * width + z * LANES
                    out[:, at : at + LANES] = half_lanes(a, b, half)

    return pl.pallas_call(
        kernel,
        grid=(3,),
        in_specs=[pl.BlockSpec((S, rows, LANES), lambda i: (0, 0, i))] * pairs,
        out_specs=pl.BlockSpec((rows, 2 * pairs * width), lambda i: (0, i)),
        out_shape=jax.ShapeDtypeStruct((rows, HEADS * HEAD * 3), F32),
    )(*gathered)


def unpack_groups(*stacks, rows):
    S, w = stacks[0].shape[1], stacks[0].shape[3]
    groups = [stack.shape[0] for stack in stacks]
    starts = [sum(groups[:i]) for i in range(len(groups))]

    def kernel(*refs):
        i = pl.program_id(0)
        for src, start, count in zip(refs, starts, groups):

            @pl.when((i >= start) & (i < start + count))
            def _():
                for s in range(S):
                    refs[-1][:, s * w : (s + 1) * w] = src[0, s].astype(F32)

    def block(start, count):
        return pl.BlockSpec(
            (1, S, rows, w), lambda i: (jnp.clip(i - start, 0, count - 1), 0, 0, 0)
        )

    return pl.pallas_call(
        kernel,
        grid=(sum(groups),),
        in_specs=[block(start, count) for start, count in zip(starts, groups)],
        out_specs=pl.BlockSpec((rows, S * w), lambda i: (0, i)),
        out_shape=jax.ShapeDtypeStruct((rows, sum(groups) * S * w), F32),
    )(*stacks)


def unpack_cols(gathered, rows, F):
    S, _, cols = gathered.shape
    w = cols // F
    if w % LANES:
        split = gathered[:, :rows].reshape(S, rows, F, w)
        return split.transpose(1, 2, 0, 3).reshape(rows, F * S * w).astype(F32)

    def kernel(src, out):
        for s in range(S):
            out[:, s * w : (s + 1) * w] = src[s].astype(F32)

    return pl.pallas_call(
        kernel,
        grid=(F,),
        in_specs=[pl.BlockSpec((S, rows, w), lambda i: (0, 0, i))],
        out_specs=pl.BlockSpec((rows, S * w), lambda i: (0, i)),
        out_shape=jax.ShapeDtypeStruct((rows, F * S * w), F32),
    )(gathered)


def unpack_chunks(gathered):
    C, S, rows, n = gathered.shape
    several = S // 2

    def kernel(src, out):
        for s in range(several):
            for c in range(C):
                out[s * rows : (s + 1) * rows, c * n : (c + 1) * n] = src[c, s].astype(F32)

    return pl.pallas_call(
        kernel,
        grid=(S // several,),
        in_specs=[pl.BlockSpec((C, several, rows, n), lambda i: (0, i, 0, 0))],
        out_specs=pl.BlockSpec((several * rows, C * n), lambda i: (i, 0)),
        out_shape=jax.ShapeDtypeStruct((S * rows, C * n), F32),
    )(gathered)


def unpack_rows(gathered, rows):
    S, _, n = gathered.shape

    def kernel(src, out):
        out[...] = src[0].astype(F32)

    return pl.pallas_call(
        kernel,
        grid=(S,),
        in_specs=[pl.BlockSpec((1, rows, n), lambda i: (i, 0, 0))],
        out_specs=pl.BlockSpec((rows, n), lambda i: (i, 0)),
        out_shape=jax.ShapeDtypeStruct((S * rows, n), F32),
    )(gathered)


def body(
    tokens,
    ln_gain,
    ln_bias,
    qkv_weight,
    qkv_bias,
    dense_weight,
    dense_bias,
    fc1_weight,
    fc1_bias,
    fc2_weight,
    fc2_bias,
    segments,
    positions,
    cotangent,
):
    S, F = lax.axis_size("seq"), lax.axis_size("fsdp")
    j, f = lax.axis_index("seq"), lax.axis_index("fsdp")
    tok, D = tokens.shape[1], tokens.shape[2]
    length = tok * S
    rows_d = D // F
    ff = fc1_weight.shape[1]
    cols_up = ff // S
    block_up = cols_up // F
    hp = HEADS // S
    pairs = hp // 2
    per_shard = HEADS // F
    spread = per_shard % S == 0
    slots = per_shard // S if spread else 0

    qkv_width = pairs * 3 * LANES

    def heads_of(array, lead):
        shape = array.shape
        if spread:
            split = array.reshape(shape[:lead] + (F, S, slots) + shape[lead + 1 :])
            mine = lax.dynamic_index_in_dim(split, j, lead + 1, keepdims=False)
            return mine.reshape(shape[:lead] + (hp,) + shape[lead + 1 :])
        return lax.dynamic_slice_in_dim(array, j * hp, hp, lead)

    def qkv_cols(array):
        n = array.shape[0]
        mine = heads_of(array.reshape(n, 3, HEADS, HEAD), 2)
        return mine.reshape(n, 3, pairs, 2, HEAD).transpose(0, 2, 1, 3, 4).reshape(n, -1)

    def from_qkv_cols(gathered):
        n = gathered.shape[1]
        split = gathered.reshape(S, n, pairs, 3, 2, HEAD).transpose(0, 1, 3, 2, 4, 5)
        split = split.reshape(S, n, 3, hp, HEAD)
        if spread:
            moved = jnp.moveaxis(split.reshape(S, n, 3, F, slots, HEAD), 0, 3)
        else:
            moved = jnp.moveaxis(split, 0, 2)
        return moved.reshape(n, -1)

    upstream_own = cotangent[0]
    seg_row = segments[0]
    block_dense = slots * HEAD

    def rider(values, width):
        return jnp.pad(values[:, None], ((0, 0), (0, EXTRA - 1), (0, width - values.shape[1])))

    def split_small(small):
        cuts, at = [], 0
        for piece in smalls:
            cuts.append(small[:, at : at + piece.shape[0]].reshape(-1).astype(F32))
            at += piece.shape[0]
        return cuts

    smalls = (ln_gain, ln_bias, qkv_bias, dense_bias, fc1_bias, fc2_bias)
    fused = F == 4 and spread and slots == 1 and block_up % 128 == 0
    if fused:
        small, at = 0.0, 0
        for piece in smalls:
            n = piece.shape[0]
            small = small + jnp.pad(piece.astype(F32), (at, SMALL * 128 - at - n))
            at += n
        small = small.reshape(SMALL, 128)
        (normed, feed_out, feed_gn, upstream, w_qkv, w_dense, all_down, first_up, rest_up,
         out_mine, small, standard, inv_std) = opening(
            S, 1, tok, small, tokens[0], upstream_own, fc1_weight, fc2_weight, qkv_weight,
            dense_weight,
        )
        gain, shift, b_qkv, b_dense, b_up, b_down = split_small(small.reshape(F, -1))
        w_dense = [w_dense]
        out_mine = out_mine[0, :rows_d].astype(F32)
    else:
        inputs = tokens[0].astype(F32)
        centre = jnp.mean(inputs, axis=-1, keepdims=True)
        variance = jnp.mean((inputs - centre) ** 2, axis=-1, keepdims=True)
        inv_std = lax.rsqrt(variance + EPS)
        standard = (inputs - centre) * inv_std
        small = jnp.concatenate(smalls)
        small = lax.all_gather(small, "fsdp", axis=0)
        gain, shift, b_qkv, b_dense, b_up, b_down = split_small(small)

        normed_own = (standard * gain + shift).astype(BF)

        up_own = pick_up(fc1_weight, j, F, S)
        down_own = lax.dynamic_slice_in_dim(fc2_weight, j * block_up, block_up, 0)
        if spread and slots == 1:
            qkv_own = pick_qkv(qkv_weight, j, F, S, pairs)
        else:
            qkv_own = qkv_cols(qkv_weight)
        w_up, w_down, normed, upstream = exchange(
            S, F, 1, shards=(up_own, down_own), tokens=(normed_own, upstream_own)
        )
        w_up, w_down = w_up.reshape(D, cols_up), w_down.reshape(cols_up, D)
        normed, upstream = normed.reshape(length, D), upstream.reshape(length, D)

        bias_up = lax.dynamic_index_in_dim(b_up.reshape(F, S, block_up), j, 1, keepdims=False)
        bias_up = bias_up.reshape(-1)

        pre_act = dot(normed, w_up) + bias_up
        activated = gelu_tanh(pre_act).astype(BF)
        out_term = jnp.sum(upstream.astype(F32), axis=0).reshape(F, rows_d)
        piece_down, out_mine = exchange(
            S, F, 2, grads=((activated, upstream, rider(out_term, D)),), split=True
        )
        out_mine = out_mine[0, :rows_d].astype(F32)

        grad_act = dot_nt(upstream, w_down)
        grad_pre = jax.vjp(gelu_tanh, pre_act)[1](grad_act)[0].astype(BF)
        up_term = jnp.sum(grad_pre.astype(F32), axis=0).reshape(F, block_up)
        shards = (qkv_own,)
        if spread:
            shards += (lax.dynamic_slice_in_dim(dense_weight, j * block_dense, block_dense, 0),)
        piece_up, w_qkv, *w_dense, all_down = exchange(
            S, F, 3, grads=((normed, grad_pre, rider(up_term, cols_up)),), shards=shards,
            tokens=(piece_down,),
        )
    bias_qkv = qkv_cols(b_qkv[None])[0]
    w_qkv = w_qkv.reshape(D, qkv_width)
    if spread:
        w_dense = w_dense[0].reshape(hp * HEAD, D)
    else:
        w_dense = lax.dynamic_slice_in_dim(
            lax.all_gather(dense_weight, "fsdp", axis=0, tiled=True), j * hp * HEAD, hp * HEAD, 0
        )
    if fused:
        result, grad_inputs, ln_mine, late_up, *gathered = attend_and_close(
            S, F, 5, tok, normed, upstream, feed_out, feed_gn, w_dense, w_qkv, rest_up,
            angle_tables(seg_row),
            seg_row[:, None], seg_row[None, :], bias_qkv[None], standard, inv_std, tokens[0],
            upstream_own, gain[None], (b_dense + b_down)[None],
        )
    else:
        all_up = lax.all_gather(piece_up, "seq", axis=0)
        projected = dot(normed, w_qkv) + bias_qkv
        grad_att = dot_nt(upstream, w_dense).astype(BF)
        attended, grad_mixed = attention(projected, grad_att, angle_tables(seg_row), seg_row)
        qkv_term = jnp.sum(grad_mixed.astype(F32), axis=0)
        qkv_term = jnp.broadcast_to(qkv_term[None], (F, qkv_width))
        branches, grad_normed, ln_mine, *gathered = closing(
            S, F, 5, tok, normed, upstream, grad_mixed, attended, activated, grad_pre,
            w_dense, w_down, w_qkv, w_up, rider(qkv_term, qkv_width), standard, spread,
        )
    all_qkv = gathered[:pairs]
    if not fused:
        result = (inputs + branches + (b_dense + b_down)).astype(BF)
        scaled = grad_normed * gain
        grad_inputs = upstream_own.astype(F32) + inv_std * (
            scaled
            - jnp.mean(scaled, axis=-1, keepdims=True)
            - standard * jnp.mean(scaled * standard, axis=-1, keepdims=True)
        )

    if fused:
        grad_down = unpack_chunks(all_down)
        grad_up = unpack_groups(first_up, late_up, rows=rows_d)
        up_mine = first_up[0, :, rows_d].astype(F32).reshape(-1)
    else:
        grad_down = unpack_rows(all_down, block_up)
        grad_up = unpack_cols(all_up, rows_d, F)
        up_mine = all_up[:, rows_d, :block_up].astype(F32).reshape(-1)
    qkv_sums = jnp.concatenate([piece[:, rows_d] for piece in all_qkv], axis=1)
    qkv_sums = from_qkv_cols(qkv_sums[:, None]).reshape(F, -1)
    qkv_mine = lax.dynamic_index_in_dim(qkv_sums, f, 0, keepdims=False).astype(F32)
    if spread and slots == 1:
        grad_qkv = unpack_qkv(all_qkv, rows_d, S)
    else:
        joined = jnp.concatenate([piece[:, :rows_d] for piece in all_qkv], axis=2)
        grad_qkv = from_qkv_cols(joined).astype(F32)
    if spread:
        grad_dense = gathered[pairs].reshape(rows_d, D).astype(F32)
    else:
        part = lax.all_gather(dot_tn(attended, upstream).astype(BF), "seq", axis=0, tiled=True)
        grad_dense = lax.psum_scatter(part, "fsdp", scatter_dimension=0, tiled=True).astype(F32)
    return (
        result[None],
        grad_inputs[None],
        ln_mine[0],
        ln_mine[1],
        grad_qkv,
        qkv_mine,
        grad_dense,
        out_mine,
        grad_up,
        up_mine,
        grad_down,
        out_mine,
    )


def solution(mesh):
    row, mat = P("fsdp"), P("fsdp", None)
    act = P("fsdp", "seq", None)
    return jax.shard_map(
        body,
        mesh=mesh,
        in_specs=(
            act, row, row, mat, row, mat, row, mat, row, mat, row, mat, P("fsdp", "seq"), act,
        ),
        out_specs=(act, act, row, row, mat, row, mat, row, mat, row, mat, row),
        check_vma=False,
    )
```
